64 devices in a mesh: dp: 4 (over x, y), cp: 16 (over z, core).
Axes of the slice: x: 2, y: 2, z: 8, core: 2. Of those that a mesh axis runs over, the one named last changes fastest.
The devices are a block of a 4x4x8 slice.
Arguments:
- q_raw: bfloat16 [16384, 64, 128], P(('dp', 'cp')), parts along dimension 0
- k_raw: bfloat16 [16384, 4, 128], P(('dp', 'cp')), parts along dimension 0
- v_proj: bfloat16 [16384, 4, 128], P(('dp', 'cp')), parts along dimension 0
- out_fwd: bfloat16 [16384, 64, 128], P(('dp', 'cp')), parts along dimension 0
- lse_fwd: float32 [16384, 64], P(('dp', 'cp')), parts along dimension 0
- d_out: bfloat16 [16384, 64, 128], P(('dp', 'cp')), parts along dimension 0
- q_norm: float32 [128], replicated
- k_norm: float32 [128], replicated
Outputs:
- output 1: bfloat16 [16384, 64, 128], P(('dp', 'cp')), parts along dimension 0
- output 2: bfloat16 [16384, 4, 128], P(('dp', 'cp')), parts along dimension 0
- output 3: bfloat16 [16384, 4, 128], P(('dp', 'cp')), parts along dimension 0
- output 4: float32 [512], P('dp'), parts along dimension 0
- output 5: float32 [512], P('dp'), parts along dimension 0
There are 4 independent parts. The reference program is written for one: setup_inputs(seed, part) draws one part's arguments, and reference() takes and returns one part's arrays. A program takes and returns all parts, laid end to end along the dimension named above; an argument that names none is the same for every part.
All inputs are finite; a program needn't handle non-finite values.
Results may differ from the reference program's by a relative error of at most 0.00281665.
Values are sent between devices in bfloat16 or wider.
A program may use at most 768 MiB of HBM per device.

```python
import jax
import jax.numpy as jnp
from jax import lax

HEADS = 64
KV_HEADS = 4
HEAD_DIM = 128
CHUNK = 128
CP_RANKS = 16
QUERY_BLOCK = 64
SEQ_LEN = 2 * CP_RANKS * CHUNK
Q_PER_KV = HEADS // KV_HEADS
BLOCK_COUNT = SEQ_LEN // QUERY_BLOCK
ROPE_THETA = 1000000.0
NORM_EPS = 1e-6


def layout_positions():
    row_ids = jnp.arange(SEQ_LEN)
    owner_dev = row_ids // (2 * CHUNK)
    within = row_ids % (2 * CHUNK)
    chunk_id = jnp.where(within < CHUNK, owner_dev, 2 * CP_RANKS - 1 - owner_dev)
    return chunk_id * CHUNK + within % CHUNK


def rope_tables(positions):
    inv_freq = ROPE_THETA ** (-jnp.arange(0, HEAD_DIM, 2).astype(jnp.float32) / HEAD_DIM)
    angles = positions.astype(jnp.float32)[:, None] * inv_freq[None, :]
    angles = jnp.concatenate([angles, angles], axis=-1)
    return jnp.cos(angles)[:, None, :], jnp.sin(angles)[:, None, :]


def norm_rope(raw_in, weight, cos_t, sin_t):
    mean_sq = jnp.mean(raw_in * raw_in, axis=-1, keepdims=True)
    normed = raw_in * lax.rsqrt(mean_sq + NORM_EPS) * weight
    half_dim = raw_in.shape[-1] // 2
    rotated = jnp.concatenate([-normed[..., half_dim:], normed[..., :half_dim]], axis=-1)
    return normed * cos_t + rotated * sin_t


def forward_stats(q_raw, k_raw, v_proj, q_norm, k_norm):
    positions = layout_positions()
    cos_t, sin_t = rope_tables(positions)
    q_b = norm_rope(q_raw.astype(jnp.float32), q_norm, cos_t, sin_t).astype(jnp.bfloat16)
    k_b = norm_rope(k_raw.astype(jnp.float32), k_norm, cos_t, sin_t).astype(jnp.bfloat16)
    q_f = q_b.astype(jnp.float32).reshape(BLOCK_COUNT, QUERY_BLOCK, KV_HEADS, Q_PER_KV, HEAD_DIM)
    k_f = k_b.astype(jnp.float32)
    v_f = v_proj.astype(jnp.float32)
    sm_scale = HEAD_DIM ** -0.5

    def one_block(scan_in):
        q_blk, q_pos = scan_in
        logits = jnp.einsum('qngd,knd->qngk', q_blk, k_f) * sm_scale
        visible = (q_pos[:, None] >= positions[None, :])[:, None, None, :]
        logits = jnp.where(visible, logits, -jnp.inf)
        row_max = jnp.max(logits, axis=-1, keepdims=True)
        weights = jnp.exp(logits - row_max)
        row_sum = jnp.sum(weights, axis=-1, keepdims=True)
        out_blk = jnp.einsum('qngk,knd->qngd', weights / row_sum, v_f)
        lse_blk = (row_max + jnp.log(row_sum))[..., 0]
        return out_blk, lse_blk

    out_blocks, lse_blocks = lax.map(one_block, (q_f, positions.reshape(BLOCK_COUNT, QUERY_BLOCK)))
    out_fwd = out_blocks.reshape(SEQ_LEN, HEADS, HEAD_DIM).astype(jnp.bfloat16)
    return out_fwd, lse_blocks.reshape(SEQ_LEN, HEADS)


def setup_inputs(seed: int = 0, part: int = 0) -> dict:
    base_key = jax.random.key(seed)
    shared_key, part_key = jax.random.split(base_key)
    part_key = jax.random.fold_in(part_key, part)
    part_keys = jax.random.split(part_key, 4)
    shared_keys = jax.random.split(shared_key, 2)
    q_raw = jax.random.normal(part_keys[0], (SEQ_LEN, HEADS, HEAD_DIM), jnp.float32).astype(jnp.bfloat16)
    k_raw = jax.random.normal(part_keys[1], (SEQ_LEN, KV_HEADS, HEAD_DIM), jnp.float32).astype(jnp.bfloat16)
    v_proj = jax.random.normal(part_keys[2], (SEQ_LEN, KV_HEADS, HEAD_DIM), jnp.float32).astype(jnp.bfloat16)
    d_out = jax.random.normal(part_keys[3], (SEQ_LEN, HEADS, HEAD_DIM), jnp.float32).astype(jnp.bfloat16)
    q_norm = jax.random.uniform(shared_keys[0], (HEAD_DIM,), jnp.float32, minval=0.5, maxval=1.6)
    k_norm = jax.random.uniform(shared_keys[1], (HEAD_DIM,), jnp.float32, minval=0.5, maxval=1.6)
    out_fwd, lse_fwd = forward_stats(q_raw, k_raw, v_proj, q_norm, k_norm)
    return {'q_raw': q_raw, 'k_raw': k_raw, 'v_proj': v_proj, 'out_fwd': out_fwd, 'lse_fwd': lse_fwd, 'd_out': d_out, 'q_norm': q_norm, 'k_norm': k_norm}


def reference(q_raw, k_raw, v_proj, out_fwd, lse_fwd, d_out, q_norm, k_norm):
    positions = layout_positions()
    cos_t, sin_t = rope_tables(positions)
    q_full, pull_q = jax.vjp(lambda raw_in, weight: norm_rope(raw_in, weight, cos_t, sin_t), q_raw.astype(jnp.float32), q_norm)
    k_full, pull_k = jax.vjp(lambda raw_in, weight: norm_rope(raw_in, weight, cos_t, sin_t), k_raw.astype(jnp.float32), k_norm)
    q_f = q_full.astype(jnp.bfloat16).astype(jnp.float32)
    k_f = k_full.astype(jnp.bfloat16).astype(jnp.float32)
    v_f = v_proj.astype(jnp.float32)
    do_f = d_out.astype(jnp.float32)
    delta_sum = jnp.sum(do_f * out_fwd.astype(jnp.float32), axis=-1)
    sm_scale = HEAD_DIM ** -0.5
    scan_in = (q_f.reshape(BLOCK_COUNT, QUERY_BLOCK, KV_HEADS, Q_PER_KV, HEAD_DIM),
               do_f.reshape(BLOCK_COUNT, QUERY_BLOCK, KV_HEADS, Q_PER_KV, HEAD_DIM),
               lse_fwd.reshape(BLOCK_COUNT, QUERY_BLOCK, KV_HEADS, Q_PER_KV),
               delta_sum.reshape(BLOCK_COUNT, QUERY_BLOCK, KV_HEADS, Q_PER_KV),
               positions.reshape(BLOCK_COUNT, QUERY_BLOCK))

    def scan_step(loop_state, block_in):
        dk_acc, dv_acc = loop_state
        q_blk, do_blk, lse_blk, delta_blk, q_pos = block_in
        logits = jnp.einsum('qngd,knd->qngk', q_blk, k_f) * sm_scale - lse_blk[..., None]
        visible = (q_pos[:, None] >= positions[None, :])[:, None, None, :]
        attn_prob = jnp.exp(jnp.where(visible, logits, -jnp.inf))
        attn_dprob = jnp.einsum('qngd,knd->qngk', do_blk, v_f)
        score_grad = (attn_prob * (attn_dprob - delta_blk[..., None])).astype(jnp.bfloat16).astype(jnp.float32)
        prob_bf = attn_prob.astype(jnp.bfloat16).astype(jnp.float32)
        dq_blk = sm_scale * jnp.einsum('qngk,knd->qngd', score_grad, k_f)
        dk_acc = dk_acc + sm_scale * jnp.einsum('qngk,qngd->knd', score_grad, q_blk)
        dv_acc = dv_acc + jnp.einsum('qngk,qngd->knd', prob_bf, do_blk)
        return (dk_acc, dv_acc), dq_blk

    zero_kv = jnp.zeros((SEQ_LEN, KV_HEADS, HEAD_DIM), jnp.float32)
    (dk_sum, dv_sum), dq_blocks = lax.scan(scan_step, (zero_kv, zero_kv), scan_in)
    dq_raw, dq_norm = pull_q(dq_blocks.reshape(SEQ_LEN, HEADS, HEAD_DIM))
    dk_raw, dk_norm = pull_k(dk_sum)
    return (dq_raw.astype(jnp.bfloat16), dk_raw.astype(jnp.bfloat16), dv_sum.astype(jnp.bfloat16), dq_norm, dk_norm)
```

```python
import functools

import jax
import jax.numpy as jnp
from jax import lax
from jax.experimental import pallas as pl
from jax.experimental.pallas import tpu as pltpu
from jax.sharding import PartitionSpec as P

HEAD_DIM = 128
ROPE_THETA = 1000000.0
NORM_EPS = 1e-6
SM_SCALE = HEAD_DIM ** -0.5
LOG2E = 1.4426950408889634
EXP_SCALE = SM_SCALE * LOG2E
F32, BF16 = jnp.float32, jnp.bfloat16


def rope_tables(positions):
    inv_freq = ROPE_THETA ** (-jnp.arange(0, HEAD_DIM, 2).astype(F32) / HEAD_DIM)
    angles = positions.astype(F32)[:, None] * inv_freq[None, :]
    cos_h, sin_h = jnp.cos(angles), jnp.sin(angles)
    return jnp.concatenate([cos_h, cos_h], -1), jnp.concatenate([-sin_h, sin_h], -1)


def swap_halves(x):
    half = x.shape[-1] // 2
    return jnp.concatenate([x[..., half:], x[..., :half]], axis=-1)


def norm_rope(raw_in, weight, cos_t, sin_t):
    mean_sq = jnp.mean(raw_in * raw_in, axis=-1, keepdims=True)
    normed = raw_in * lax.rsqrt(mean_sq + NORM_EPS) * weight
    return normed * cos_t + swap_halves(normed) * sin_t


def dot(a, b, ca, cb):
    return lax.dot_general(a, b, (((ca,), (cb,)), ((), ())), preferred_element_type=F32)


def roll_half(x):
    return pltpu.roll(x, HEAD_DIM // 2, axis=x.ndim - 1)


def head_kernel(group, cp_size, chunk, per_kv, q_ref, do_ref, out_ref, lse_ref, cos_ref, sin_ref, w_ref, kv_ref,
                dq_in, dq_out, dkv_ref, dw_ref, qb, dob, aux, dq):
    rank = lax.axis_index('cp')
    rows = chunk * per_kv
    step = 16
    lane = lax.broadcasted_iota(jnp.int32, (step * per_kv, HEAD_DIM), 1)
    lane3 = lax.broadcasted_iota(jnp.int32, (step, per_kv, HEAD_DIM), 2)
    head3 = lax.broadcasted_iota(jnp.int32, (step, per_kv, HEAD_DIM), 1)
    weight = w_ref[...]

    def prepare(i, carry):
        toks = pl.ds(i * step, step)
        dst = pl.ds(pl.multiple_of(i * step * per_kv, step * per_kv), step * per_kv)
        x = q_ref[toks].astype(F32)
        mean_sq = jnp.mean(x * x, axis=-1, keepdims=True)
        y = x * lax.rsqrt(mean_sq + NORM_EPS) * weight
        qr = y * cos_ref[toks] + roll_half(y) * sin_ref[toks]
        qb[dst, :] = qr.reshape(step * per_kv, HEAD_DIM).astype(BF16)
        do = do_ref[toks]
        dob[dst, :] = do.reshape(step * per_kv, HEAD_DIM)
        delta = jnp.sum(do.astype(F32) * out_ref[toks].astype(F32), axis=-1, keepdims=True)
        lse = jnp.sum(jnp.where(lane3 == head3 + group * per_kv, lse_ref[toks], 0.0), axis=-1, keepdims=True)
        r0 = jnp.where(lane3 < 3, lse * (-1.0 / SM_SCALE), -delta).reshape(step * per_kv, HEAD_DIM)
        r1 = r0 - r0.astype(BF16).astype(F32)
        r2 = r1 - r1.astype(BF16).astype(F32)
        val = jnp.where((lane == 0) | (lane == 3), r0, jnp.where((lane == 1) | (lane == 4), r1, r2))
        aux[dst, :] = jnp.where(lane < 6, val, 0.0).astype(BF16)
        return carry

    lax.fori_loop(0, 2 * chunk // step, prepare, 0)
    dkv_ref[...] = jnp.zeros_like(dkv_ref)
    dq[...] = jnp.zeros_like(dq)

    n_early = rank // 2 + 1
    n_units = cp_size + 1
    keys = 2 * chunk
    klane = lax.broadcasted_iota(jnp.int32, (keys, HEAD_DIM), 1)
    ones_k = jnp.where(klane < 3, 1.0, 0.0).astype(BF16)
    ones_v = jnp.where((klane >= 3) & (klane < 6), 1.0, 0.0).astype(BF16)

    def unit(u, carry):
        late = u >= n_early
        kb = jnp.where(late, u - n_early, u)
        q_chunk = jnp.where(late, 2 * cp_size - 1 - rank, rank)
        half = kb >= cp_size // 2
        dev_a = jnp.where(half, 2 * cp_size - 1 - 2 * kb, 2 * kb)
        dev_b = jnp.where(half, 2 * cp_size - 2 - 2 * kb, 2 * kb + 1)
        hf = jnp.where(half, 1, 0)
        r = pl.ds(pl.multiple_of(jnp.where(late, rows, 0), rows), rows)
        k = jnp.concatenate([kv_ref[dev_a, hf, 0], kv_ref[dev_b, hf, 0]], axis=0)
        v = jnp.concatenate([kv_ref[dev_a, hf, 1], kv_ref[dev_b, hf, 1]], axis=0)
        qq, dd, ax = qb[r, :], dob[r, :], aux[r, :]
        s = dot(jnp.concatenate([qq, ax], 1), jnp.concatenate([k, ones_k], 1), 1, 1)
        dp = dot(jnp.concatenate([dd, ax], 1), jnp.concatenate([v, ones_v], 1), 1, 1)
        p = jnp.exp2(s * EXP_SCALE)
        off = (q_chunk - 2 * kb) * chunk
        klan = lax.broadcasted_iota(jnp.int32, (per_kv, keys), 1)
        p = jnp.concatenate([jnp.where(klan <= off + t, p[per_kv * t:per_kv * (t + 1)], 0.0) for t in range(chunk)], 0)
        ds = (p * dp).astype(BF16)
        pb = p.astype(BF16)
        dv = dot(dd, pb, 0, 0)
        dk = dot(qq, ds, 0, 0)
        dkv_ref[dev_a, hf, 0] += dk[:, :chunk]
        dkv_ref[dev_b, hf, 0] += dk[:, chunk:]
        dkv_ref[dev_a, hf, 1] += dv[:, :chunk]
        dkv_ref[dev_b, hf, 1] += dv[:, chunk:]
        dq[r, :] += dot(ds, k, 1, 0)
        return carry

    lax.fori_loop(0, n_units, unit, 0)

    def finish(i, acc):
        toks = pl.ds(i * step, step)
        src = pl.ds(pl.multiple_of(i * step * per_kv, step * per_kv), step * per_kv)
        x = q_ref[toks].astype(F32)
        rstd = lax.rsqrt(jnp.mean(x * x, axis=-1, keepdims=True) + NORM_EPS)
        xhat = x * rstd
        g = (dq[src, :] * SM_SCALE).reshape(step, per_kv, HEAD_DIM)
        dy = g * cos_ref[toks] - roll_half(g) * sin_ref[toks]
        acc = acc + jnp.sum((dy * xhat).reshape(step * per_kv // 8, 8, HEAD_DIM), axis=0)
        dxh = dy * weight
        dx = rstd * (dxh - xhat * jnp.mean(dxh * xhat, axis=-1, keepdims=True))
        dq_out[toks] = dx.astype(BF16)
        return acc

    dw_ref[...] = lax.fori_loop(0, 2 * chunk // step, finish, jnp.zeros((8, HEAD_DIM), F32))


def head_grads(group, cp_size, q_raw, d_out, out_fwd, lse3, cos3, sin3, w3, kv, dq_prev):
    tokens, heads, hd = q_raw.shape
    chunk = tokens // 2
    per_kv = 16
    rows = tokens * per_kv
    grp = pl.BlockSpec((tokens, per_kv, hd), lambda i: (0, group, 0))
    full = lambda a: pl.BlockSpec(a.shape, lambda i: (0,) * a.ndim)
    args = [q_raw, d_out, out_fwd, lse3, cos3, sin3, w3, kv]
    in_specs = [grp, grp, grp] + [full(a) for a in args[3:]]
    aliases = {}
    kern = functools.partial(head_kernel, group, cp_size, chunk, per_kv)
    if dq_prev is not None:
        args.append(dq_prev)
        in_specs.append(pl.BlockSpec(memory_space=pl.ANY))
        aliases = {8: 0}
    else:
        base = kern
        kern = lambda *refs: base(*refs[:8], None, *refs[8:])
    dkv_shape = kv.shape[:3] + (hd, chunk)
    return pl.pallas_call(
        kern,
        grid=(1,),
        in_specs=in_specs,
        out_specs=[grp, pl.BlockSpec(dkv_shape, lambda i: (0,) * 5), pl.BlockSpec((8, hd), lambda i: (0, 0))],
        out_shape=[jax.ShapeDtypeStruct(q_raw.shape, BF16), jax.ShapeDtypeStruct(dkv_shape, F32),
                   jax.ShapeDtypeStruct((8, hd), F32)],
        scratch_shapes=[pltpu.VMEM((rows, hd), BF16), pltpu.VMEM((rows, hd), BF16), pltpu.VMEM((rows, hd), BF16),
                        pltpu.VMEM((rows, hd), F32)],
        input_output_aliases=aliases,
        name='attn_bwd',
        compiler_params=pltpu.CompilerParams(vmem_limit_bytes=50 * 2 ** 20),
        cost_estimate=pl.CostEstimate(flops=11 * 10 ** 9, bytes_accessed=10 * 2 ** 20, transcendentals=10 ** 7),
    )(*args)


def solution(mesh):
    cp_size = mesh.shape['cp']

    def local_grads(q_raw, k_raw, v_proj, out_fwd, lse_fwd, d_out, q_norm, k_norm):
        dev_rank = lax.axis_index('cp')
        tokens, num_heads = q_raw.shape[0], q_raw.shape[1]
        chunk = tokens // 2
        kv_heads = k_raw.shape[1]
        offsets = jnp.arange(chunk)
        positions = jnp.concatenate([dev_rank * chunk + offsets, (2 * cp_size - 1 - dev_rank) * chunk + offsets])
        cos_t, sin_t = rope_tables(positions)
        k_full, pull_k = jax.vjp(lambda a, w: norm_rope(a, w, cos_t[:, None], sin_t[:, None]), k_raw.astype(F32), k_norm)
        kv = jnp.stack([k_full.astype(BF16), v_proj], axis=0)
        kv = kv.reshape(2, 2, chunk, kv_heads, HEAD_DIM).transpose(3, 1, 0, 2, 4)
        lse3 = jnp.pad(lse_fwd, ((0, 0), (0, HEAD_DIM - num_heads)))[:, None, :]
        cos3, sin3 = cos_t[:, None, :], sin_t[:, None, :]
        w3 = q_norm.reshape(1, 1, HEAD_DIM)
        dq_raw, parts, dws = None, [], []
        for g in range(kv_heads):
            kv_all = lax.all_gather(kv[g], 'cp')
            dq_raw, dkv, dw = head_grads(g, cp_size, q_raw, d_out, out_fwd, lse3, cos3, sin3, w3, kv_all, dq_raw)
            parts.append(lax.psum_scatter(dkv, 'cp', scatter_dimension=0))
            dws.append(dw)
        total = jnp.stack(parts)
        total = total.transpose(2, 1, 4, 0, 3).reshape(2, tokens, kv_heads, HEAD_DIM)
        dk_raw, dk_weight = pull_k(total[0] * SM_SCALE)
        dq_weight = jnp.sum(sum(dws), axis=0)
        return (dq_raw, dk_raw.astype(BF16), total[1].astype(BF16),
                lax.psum(dq_weight, 'cp'), lax.psum(dk_weight, 'cp'))

    row_spec = P(('dp', 'cp'))
    in_specs = (row_spec, row_spec, row_spec, row_spec, row_spec, row_spec, P(), P())
    out_specs = (row_spec, row_spec, row_spec, P('dp'), P('dp'))
    return jax.shard_map(local_grads, mesh=mesh, in_specs=in_specs, out_specs=out_specs, check_vma=False)
```

```python
import functools

import jax
import jax.numpy as jnp
from jax import lax
from jax.experimental import pallas as pl
from jax.experimental.pallas import tpu as pltpu
from jax.sharding import PartitionSpec as P

HEAD_DIM = 128
ROPE_THETA = 1000000.0
NORM_EPS = 1e-6
SM_SCALE = HEAD_DIM ** -0.5
EXP_SCALE = SM_SCALE * 1.4426950408889634
F32, BF16 = jnp.float32, jnp.bfloat16
MESH = pl.DeviceIdType.MESH

ORDER_A = (-1, 1, 4, -3, 3, -2, 2)
ORDER_B = (4, -3, 3, -2, 2, -1, 1)
REACH = ((4, 3), (3, 4))
GATHER_AT = (-1, -1, -1, 0, 2, 3, 5, 7, 9, 11, 8, 10, 13, 15, 17, 20, 22, 25, 28, 31)
REDUCE_AT = (17, 18, 25, 26, 34, 37, 41, 45, 49, 53, 54, 56, 60, 64, 68, 71, 75, 79, 200, 201)
PREP_TOKENS = 32
FIN_STEPS = 16


def rope_tables(positions):
    inv_freq = ROPE_THETA ** (-jnp.arange(0, HEAD_DIM, 2).astype(F32) / HEAD_DIM)
    angles = positions.astype(F32)[:, None] * inv_freq[None, :]
    cos_h, sin_h = jnp.cos(angles), jnp.sin(angles)
    return jnp.concatenate([cos_h, cos_h], -1), jnp.concatenate([-sin_h, sin_h], -1)


def swap_halves(x):
    half = x.shape[-1] // 2
    return jnp.concatenate([x[..., half:], x[..., :half]], axis=-1)


def norm_rope(raw_in, weight, cos_t, sin_t):
    mean_sq = jnp.mean(raw_in * raw_in, axis=-1, keepdims=True)
    normed = raw_in * lax.rsqrt(mean_sq + NORM_EPS) * weight
    return normed * cos_t + swap_halves(normed) * sin_t


def dot(a, b, ca, cb):
    return lax.dot_general(a, b, (((ca,), (cb,)), ((), ())), preferred_element_type=F32)


def roll_half(x):
    return pltpu.roll(x, HEAD_DIM // 2, axis=x.ndim - 1)


def row_sum(prod, ones):
    high = prod.astype(BF16)
    low = (prod - high.astype(F32)).astype(BF16)
    return dot(jnp.concatenate([high, low], 1), ones, 1, 0)


def select_const(index, values):
    out = jnp.int32(values[0])
    for i, v in enumerate(values[1:], 1):
        out = jnp.where(index == i, v, out)
    return out


def lookup(step, table):
    out = jnp.int32(0)
    for i, at in enumerate(table):
        out = jnp.where(step == at, i + 1, out)
    return out


def mega_kernel(nz, chunk, per_kv,
                q_hbm, do_hbm, out_hbm, lse_hbm, kv_hbm, cos_hbm, sin_hbm, w_ref,
                dq_hbm, dkv_hbm, dw_ref,
                xq, xdo, xout, qb, aux, dq, kvall, acc, rsb, lse, cos_t, sin_t,
                ld_sem, xs_sem, xr_sem, kl_sem, ks_sem, kr_sem, tab_sem,
                ag_send, ag_recv, rs_send, rs_recv, dq_loc, dq_snd, dq_rcv, dk_loc, dk_snd, dk_rcv):
    me = lax.axis_index('cp')
    cp = 2 * nz
    z, core = me // 2, me % 2
    other = 1 - core
    sib = 2 * z + other
    right = 2 * lax.rem(z + 1, nz) + core
    left = 2 * lax.rem(z + nz - 1, nz) + core
    tok = 2 * chunk
    rows = tok * per_kv

    def wrap(i):
        return lax.rem(i + 2 * nz, nz)

    barrier = pltpu.get_barrier_semaphore()

    def say(i, carry):
        pl.semaphore_signal(barrier, inc=1, device_id={'cp': lax.rem(me + i, cp)}, device_id_type=MESH)
        return carry

    lax.fori_loop(1, cp, say, 0)

    def my_off(el):
        return pl.multiple_of((core if el == 0 else other) * chunk, chunk)

    def sib_off(el):
        return pl.multiple_of((other if el == 0 else core) * chunk, chunk)

    kv_loads, loads = [], []
    for h in range(2):
        for el in range(2):
            kv_loads.append(pltpu.make_async_copy(kv_hbm.at[core, h, el], kvall.at[z, h, el, :, pl.ds(my_off(el), chunk), :], kl_sem.at[h, el]))
    tables = [pltpu.make_async_copy(cos_hbm, cos_t, tab_sem.at[0]), pltpu.make_async_copy(sin_hbm, sin_t, tab_sem.at[1])]
    for h in range(2):
        for el in range(2):
            heads = lambda c: pl.ds(pl.multiple_of((2 * c + h) * per_kv, per_kv), per_kv)
            src = pl.ds(el * chunk, chunk)
            dst = pl.ds(my_off(el), chunk)
            row = []
            for i, (hbm, buf) in enumerate(((q_hbm, xq), (do_hbm, xdo), (out_hbm, xout))):
                row.append((pltpu.make_async_copy(hbm.at[src, heads(core), :], buf.at[h, el, dst], ld_sem.at[h, el, i]),
                            pltpu.make_async_remote_copy(hbm.at[src, heads(other), :], buf.at[h, el, dst], xs_sem.at[h, el, i],
                                                         xr_sem.at[h, el, i], device_id={'cp': sib}, device_id_type=MESH)))
            row.append((pltpu.make_async_copy(lse_hbm.at[core, h, src], lse.at[h, el, dst], ld_sem.at[h, el, 3]),
                        pltpu.make_async_remote_copy(lse_hbm.at[other, h, src], lse.at[h, el, dst], xs_sem.at[h, el, 3],
                                                     xr_sem.at[h, el, 3], device_id={'cp': sib}, device_id_type=MESH)))
            loads.append(row)
    for cpy in kv_loads + tables:
        cpy.start()
    for row in loads:
        for loc, _ in row:
            loc.start()
    pl.semaphore_wait(barrier, cp - 1)

    kv_swaps = []
    for h in range(2):
        for el in range(2):
            kv_swaps.append(pltpu.make_async_remote_copy(
                kv_hbm.at[other, h, el], kvall.at[z, h, el, :, pl.ds(my_off(el), chunk), :], ks_sem.at[h, el], kr_sem.at[h, el],
                device_id={'cp': sib}, device_id_type=MESH))
    for cpy in kv_swaps:
        cpy.start()
    for row in loads:
        for _, rem in row:
            rem.start()

    def reach(direction, h):
        return jnp.where(h == 0, REACH[0][direction], REACH[1][direction])

    def gather_copy(direction, h, s, el):
        owner = wrap(z - (s - 1)) if direction == 0 else wrap(z + (s - 1))
        ref = kvall.at[owner, h, el]
        return pltpu.make_async_remote_copy(ref, ref, ag_send.at[direction, h, s - 1, el], ag_recv.at[direction, h, s - 1, el],
                                            device_id={'cp': (right, left)[direction]}, device_id_type=MESH)

    def gather_arrival(direction, h, s, el):
        owner = wrap(z - s) if direction == 0 else wrap(z + s)
        ref = kvall.at[owner, h, el]
        return pltpu.make_async_remote_copy(ref, ref, ag_send.at[direction, h, s - 1, el], ag_recv.at[direction, h, s - 1, el],
                                            device_id={'cp': (right, left)[direction]}, device_id_type=MESH)

    def gather_sends(direction, h, s, el):
        dist = reach(direction, h)
        if direction == 0:
            ok = (el == 0) | (wrap(z - (s - 1)) + dist >= nz)
        else:
            ok = (el == 0) | ((z >= 1) & (z + s - 1 <= nz - 1))
        return (s <= dist) & ok

    def gather_arrives(direction, h, s, el):
        dist = reach(direction, h)
        if direction == 0:
            ok = (el == 0) | (wrap(z - s) + dist >= nz)
        else:
            ok = (el == 0) | (z + s <= nz - 1)
        return (s >= 1) & (s <= dist) & ok

    def gather_step(a):
        h, s, el = a // 10, lax.rem(a, 10) // 2 + 1, lax.rem(a, 2)
        for direction in range(2):
            @pl.when(gather_arrives(direction, h, s - 1, el))
            def _():
                gather_arrival(direction, h, jnp.maximum(s - 1, 1), el).wait_recv()

            @pl.when(gather_sends(direction, h, s, el))
            def _():
                gather_copy(direction, h, jnp.minimum(s, 4), el).start()

    def reduce_copy(direction, h, d, el):
        owner = wrap(z + d) if direction == 0 else wrap(z - d)
        return pltpu.make_async_remote_copy(acc.at[owner, h, el], rsb.at[direction, d - 1, h, el],
                                            rs_send.at[direction, d - 1, h, el], rs_recv.at[direction, d - 1, h, el],
                                            device_id={'cp': (right, left)[direction]}, device_id_type=MESH)

    def reduce_sends(direction, h, d, el):
        dist = reach(direction, h)
        if direction == 0:
            ok = (el == 0) | (z + d <= nz - 1)
        else:
            ok = (el == 0) | (wrap(z - d) + dist >= nz)
        return (d >= 1) & (d <= dist) & ok

    def reduce_arrives(direction, h, d, el):
        dist = reach(direction, h)
        if direction == 0:
            ok = (el == 0) | ((z >= 1) & (z + d <= nz - 1))
        else:
            ok = (el == 0) | (wrap(z - d) + dist >= nz)
        return (d + 1 <= dist) & ok

    def reduce_step(b):
        h, d, el = b // 10, 4 - lax.rem(b, 10) // 2, lax.rem(b, 2)
        for direction in range(2):
            owner = wrap(z + d) if direction == 0 else wrap(z - d)

            @pl.when(reduce_arrives(direction, h, d, el))
            def _():
                slot = jnp.minimum(d, 3)
                pltpu.make_async_remote_copy(acc.at[owner, h, el], rsb.at[direction, slot, h, el],
                                             rs_send.at[direction, slot, h, el], rs_recv.at[direction, slot, h, el],
                                             device_id={'cp': (right, left)[direction]}, device_id_type=MESH).wait_recv()
                acc[owner, h, el] += rsb[direction, slot, h, el]

            @pl.when(reduce_sends(direction, h, d, el))
            def _():
                reduce_copy(direction, h, jnp.maximum(d, 1), el).start()

    def ticks(g):
        a = lookup(g, GATHER_AT)

        @pl.when(a > 0)
        def _():
            gather_step(a - 1)

        b = lookup(g, REDUCE_AT)

        @pl.when(b > 0)
        def _():
            reduce_step(b - 1)

    for i in range(4):
        kv_loads[i].wait()
        kv_swaps[i].wait_recv()
        if i < 2:
            gather_step(jnp.int32(i))

    sub = PREP_TOKENS
    weight = w_ref[...]
    ones = jnp.ones((2 * HEAD_DIM, HEAD_DIM), BF16)
    lane3 = lax.broadcasted_iota(jnp.int32, (sub, per_kv, HEAD_DIM), 2)
    head3 = lax.broadcasted_iota(jnp.int32, (sub, per_kv, HEAD_DIM), 1)
    n_l = 3 * per_kv
    lse_mask = (lane3 - head3 == 0) | (lane3 - head3 == per_kv) | (lane3 - head3 == 2 * per_kv)
    flat = lambda x: x.reshape(x.shape[0] * per_kv, HEAD_DIM)

    def prepare(h, el, i):
        toks = pl.ds(pl.multiple_of(i * sub, sub), sub)
        tabs = pl.ds(pl.multiple_of(el * tok + i * sub, sub), sub)
        dst = pl.ds(pl.multiple_of(((h * 2 + el) * tok + i * sub) * per_kv, sub * per_kv), sub * per_kv)
        x = xq[h, el, toks].astype(F32)
        ms = row_sum(flat(x * x), ones) * (1.0 / HEAD_DIM)
        y = flat(x) * lax.rsqrt(ms + NORM_EPS) * weight
        y3 = y.reshape(x.shape)
        qr = y3 * cos_t[tabs] + roll_half(y3) * sin_t[tabs]
        qb[dst, :] = flat(qr).astype(BF16)
        prod = flat(xdo[h, el, toks].astype(F32) * xout[h, el, toks].astype(F32))
        r0 = -row_sum(prod, ones)
        r1 = r0 - r0.astype(BF16).astype(F32)
        r2 = r1 - r1.astype(BF16).astype(F32)
        lane = lax.broadcasted_iota(jnp.int32, r0.shape, 1)
        dpart = jnp.where(lane == n_l, r0, jnp.where(lane == n_l + 1, r1, jnp.where(lane == n_l + 2, r2, 0.0)))
        aux[dst, :] = flat(jnp.where(lse_mask, lse[h, el, toks], dpart.reshape(x.shape))).astype(BF16)

    for t in tables:
        t.wait()
    for h in range(2):
        for el in range(2):
            for loc, rem in loads[h * 2 + el]:
                loc.wait()
                rem.wait_recv()
            pl.loop(0, tok // sub)(functools.partial(prepare, h, el))
        if h == 0:
            gather_step(jnp.int32(2))

    acc[...] = jnp.zeros_like(acc)
    dq[...] = jnp.zeros_like(dq)

    keys = tok
    half_rows = rows // 2
    klane = lax.broadcasted_iota(jnp.int32, (keys, HEAD_DIM), 1)
    ones_k = jnp.where(klane < n_l, 1.0, 0.0).astype(BF16)
    ones_v = jnp.where((klane >= n_l) & (klane < n_l + 3), 1.0, 0.0).astype(BF16)
    own_steps = 6
    head_steps = own_steps + 4 * (nz - 1)

    def work(g, carry):
        h = jnp.where(g >= head_steps, 1, 0)
        u = g - h * head_steps
        own = jnp.where(h == 0, u < own_steps, u >= 4 * (nz - 1))
        ou = jnp.where(h == 0, u, u - 4 * (nz - 1))
        bu = jnp.where(h == 0, u - own_steps, u)
        bu = jnp.clip(bu, 0, 4 * (nz - 1) - 1)
        ou = jnp.clip(ou, 0, own_steps - 1)
        k_idx, j = bu // 4, lax.rem(bu, 4) // 2
        half = jnp.where(own, lax.rem(ou, 2), lax.rem(bu, 2))
        delta = jnp.where(h == 0, select_const(k_idx, ORDER_A), select_const(k_idx, ORDER_B))
        kz = jnp.where(own, z, wrap(z + delta))
        lower = kz < z
        q_late = jnp.where(own, jnp.where(ou >= 2, 1, 0), jnp.where(lower, j, 1))
        k_late = jnp.where(own, jnp.where(ou >= 4, 1, 0), jnp.where(lower, 0, j))
        q_blk = jnp.where(q_late == 1, 2 * nz - 1 - z, z)
        k_blk = jnp.where(k_late == 1, 2 * nz - 1 - kz, kz)
        off = (q_blk - k_blk) * tok + half * chunk
        r = pl.ds(pl.multiple_of(((h * 2 + q_late) * 2 + half) * half_rows, half_rows), half_rows)
        k, v = kvall[kz, h, k_late, 0], kvall[kz, h, k_late, 1]
        qq, ax = qb[r, :], aux[r, :]
        dd = flat(xdo[h, q_late, pl.ds(pl.multiple_of(half * chunk, chunk), chunk)])
        s = dot(jnp.concatenate([qq, ax], 1), jnp.concatenate([k, ones_k], 1), 1, 1)
        dp = dot(jnp.concatenate([dd, ax], 1), jnp.concatenate([v, ones_v], 1), 1, 1)
        p = jnp.exp2(s * EXP_SCALE)
        klan = lax.broadcasted_iota(jnp.int32, (per_kv, keys), 1)
        p = jnp.concatenate([jnp.where(klan <= off + t, p[per_kv * t:per_kv * (t + 1)], 0.0) for t in range(chunk)], 0)
        ds = (p * dp).astype(BF16)
        pb = p.astype(BF16)
        acc[kz, h, k_late, 0] += dot(qq, ds, 0, 0)
        acc[kz, h, k_late, 1] += dot(dd, pb, 0, 0)
        dq[r, :] += dot(ds, k, 1, 0)
        ticks(g)
        return carry

    n_steps = 2 * head_steps
    lax.fori_loop(0, n_steps, work, 0)

    ftok = 4 * tok // FIN_STEPS
    per_blk = FIN_STEPS // 4

    def finish(i, carry):
        hel = i // per_blk
        h, el, part = hel // 2, lax.rem(hel, 2), lax.rem(i, per_blk)

        def piece(jj, wsum):
            t0 = part * ftok + jj * sub
            toks = pl.ds(pl.multiple_of(t0, sub), sub)
            tabs = pl.ds(pl.multiple_of(el * tok + t0, sub), sub)
            src = pl.ds(pl.multiple_of((hel * tok + t0) * per_kv, sub * per_kv), sub * per_kv)
            x3 = xq[h, el, toks].astype(F32)
            x = flat(x3)
            rstd = lax.rsqrt(row_sum(x * x, ones) * (1.0 / HEAD_DIM) + NORM_EPS)
            xhat = x * rstd
            gq = (dq[src, :] * SM_SCALE).reshape(x3.shape)
            dy = flat(gq * cos_t[tabs] - roll_half(gq) * sin_t[tabs])
            wsum = wsum + jnp.sum((dy * xhat).reshape(sub * per_kv // 8, 8, HEAD_DIM), axis=0)
            dxh = dy * weight
            dx = rstd * (dxh - xhat * jnp.mean(dxh * xhat, axis=-1, keepdims=True))
            xq[h, el, toks] = dx.reshape(x3.shape).astype(BF16)
            return wsum

        wsum = lax.fori_loop(0, ftok // sub, piece, jnp.zeros((8, HEAD_DIM), F32))
        dw_ref[...] += wsum
        ticks(n_steps + i)
        return carry

    dw_ref[...] = jnp.zeros_like(dw_ref)
    lax.fori_loop(0, FIN_STEPS, finish, 0)

    outs = []
    for h in range(2):
        for el in range(2):
            heads = pl.ds(pl.multiple_of((2 * core + h) * per_kv, per_kv), per_kv)
            dst = dq_hbm.at[pl.ds(el * chunk, chunk), heads, :]
            outs.append((pltpu.make_async_copy(xq.at[h, el, pl.ds(my_off(el), chunk)], dst, dq_loc.at[h, el]),
                         pltpu.make_async_remote_copy(xq.at[h, el, pl.ds(sib_off(el), chunk)], dst, dq_snd.at[h, el], dq_rcv.at[h, el],
                                                      device_id={'cp': sib}, device_id_type=MESH)))
    for loc, rem in outs:
        loc.start()
        rem.start()

    def rest(b, carry):
        reduce_step(b)
        return carry

    done = sum(1 for at in REDUCE_AT if at < n_steps + FIN_STEPS)
    lax.fori_loop(done, len(REDUCE_AT), rest, 0)

    for h in range(2):
        for el in range(2):
            dst = dkv_hbm.at[2 * core + h, el]
            outs.append((pltpu.make_async_copy(acc.at[z, h, el, :, :, pl.ds(my_off(el), chunk)], dst, dk_loc.at[h, el]),
                         pltpu.make_async_remote_copy(acc.at[z, h, el, :, :, pl.ds(sib_off(el), chunk)], dst, dk_snd.at[h, el],
                                                      dk_rcv.at[h, el], device_id={'cp': sib}, device_id_type=MESH)))
    for loc, rem in outs[4:]:
        loc.start()
        rem.start()

    for cpy in kv_swaps:
        cpy.wait_send()
    for row in loads:
        for _, rem in row:
            rem.wait_send()

    def drain(i, carry):
        h, s, el = i // 8, lax.rem(i, 8) // 2 + 1, lax.rem(i, 2)
        for direction in range(2):
            @pl.when(gather_sends(direction, h, s, el))
            def _():
                gather_copy(direction, h, s, el).wait_send()

            @pl.when(reduce_sends(direction, h, s, el))
            def _():
                reduce_copy(direction, h, s, el).wait_send()
        return carry

    lax.fori_loop(0, 16, drain, 0)
    for loc, rem in outs:
        loc.wait()
        rem.wait()


def mega(nz, q_raw, d_out, out_fwd, lse_arr, kv_loc, cos3, sin3, weight):
    tokens, heads, hd = q_raw.shape
    chunk, per_kv = tokens // 2, 16
    tok = tokens
    any_spec = pl.BlockSpec(memory_space=pl.ANY)
    vmem = pl.BlockSpec(memory_space=pltpu.VMEM)
    dma = pltpu.SemaphoreType.DMA
    x_shape = (2, 2, tok, per_kv, hd)
    n_rows = 4 * tok * per_kv
    hbm = lambda a: pltpu.with_memory_space_constraint(a, pltpu.HBM)
    return pl.pallas_call(
        functools.partial(mega_kernel, nz, chunk, per_kv),
        in_specs=[any_spec] * 7 + [vmem],
        out_specs=[any_spec, any_spec, vmem],
        out_shape=[jax.ShapeDtypeStruct(q_raw.shape, BF16), jax.ShapeDtypeStruct((4, 2, 2, hd, chunk), F32),
                   jax.ShapeDtypeStruct((8, hd), F32)],
        scratch_shapes=[
            pltpu.VMEM(x_shape, BF16), pltpu.VMEM(x_shape, BF16), pltpu.VMEM(x_shape, BF16),
            pltpu.VMEM((n_rows, hd), BF16), pltpu.VMEM((n_rows, hd), BF16), pltpu.VMEM((n_rows, hd), F32),
            pltpu.VMEM((nz, 2, 2, 2, tok, hd), BF16),
            pltpu.VMEM((nz, 2, 2, 2, hd, tok), F32),
            pltpu.VMEM((2, 4, 2, 2, 2, hd, tok), F32),
            pltpu.VMEM((2, 2, tok, 1, hd), F32),
            pltpu.VMEM((2 * tok, 1, hd), F32), pltpu.VMEM((2 * tok, 1, hd), F32),
            dma((2, 2, 4)), dma((2, 2, 4)), dma((2, 2, 4)),
            dma((2, 2)), dma((2, 2)), dma((2, 2)), dma((2,)),
            dma((2, 2, 4, 2)), dma((2, 2, 4, 2)), dma((2, 4, 2, 2)), dma((2, 4, 2, 2)),
            dma((2, 2)), dma((2, 2)), dma((2, 2)), dma((2, 2)), dma((2, 2)), dma((2, 2)),
        ],
        name='attn_bwd',
        compiler_params=pltpu.CompilerParams(vmem_limit_bytes=67000000, collective_id=0, has_side_effects=True),
    )(*[hbm(a) for a in (q_raw, d_out, out_fwd, lse_arr, kv_loc, cos3, sin3)], weight)


def sum_kernel(cp, x_ref, o_ref, slots, send_sem, recv_sem):
    me = lax.axis_index('cp')
    barrier = pltpu.get_barrier_semaphore()

    def say(i, carry):
        pl.semaphore_signal(barrier, inc=1, device_id={'cp': lax.rem(me + i, cp)}, device_id_type=MESH)
        return carry

    lax.fori_loop(1, cp, say, 0)
    pl.semaphore_wait(barrier, cp - 1)

    def copy(i):
        return pltpu.make_async_remote_copy(x_ref, slots.at[cp - i], send_sem.at[i], recv_sem.at[cp - i],
                                            device_id={'cp': lax.rem(me + i, cp)}, device_id_type=MESH)

    for i in range(1, cp):
        copy(i).start()
    total = x_ref[...]
    for i in range(1, cp):
        pltpu.make_async_remote_copy(x_ref, slots.at[i], send_sem.at[i], recv_sem.at[i],
                                     device_id={'cp': lax.rem(me + i, cp)}, device_id_type=MESH).wait_recv()
    slots[0] = x_ref[...]

    def add(i, acc):
        return acc + slots[lax.rem(i - me + cp, cp)]

    o_ref[...] = lax.fori_loop(0, cp, add, jnp.zeros_like(total))
    for i in range(1, cp):
        copy(i).wait_send()


def sum_over_ring(cp, x):
    vmem = pl.BlockSpec(memory_space=pltpu.VMEM)
    return pl.pallas_call(
        functools.partial(sum_kernel, cp),
        in_specs=[vmem], out_specs=vmem,
        out_shape=jax.ShapeDtypeStruct(x.shape, F32),
        scratch_shapes=[pltpu.VMEM((cp,) + x.shape, F32), pltpu.SemaphoreType.DMA((cp,)), pltpu.SemaphoreType.DMA((cp,))],
        name='weight_sum',
        compiler_params=pltpu.CompilerParams(collective_id=1, has_side_effects=True),
    )(x)


def solution(mesh):
    cp_size = mesh.shape['cp']
    nz = cp_size // 2

    def local_grads(q_raw, k_raw, v_proj, out_fwd, lse_fwd, d_out, q_norm, k_norm):
        dev_rank = lax.axis_index('cp')
        z = dev_rank // 2
        tokens, num_heads = q_raw.shape[0], q_raw.shape[1]
        chunk = tokens // 2
        kv_heads = k_raw.shape[1]
        per_kv = num_heads // kv_heads
        offsets = jnp.arange(chunk)
        positions = jnp.concatenate([dev_rank * chunk + offsets, (2 * cp_size - 1 - dev_rank) * chunk + offsets])
        cos_t, sin_t = rope_tables(positions)
        k_full, pull_k = jax.vjp(lambda a, w: norm_rope(a, w, cos_t[:, None], sin_t[:, None]), k_raw.astype(F32), k_norm)
        kv = jnp.stack([k_full.astype(BF16), v_proj], axis=0)
        kv = kv.reshape(2, 2, chunk, 2, kv_heads // 2, HEAD_DIM).transpose(3, 4, 1, 0, 2, 5)
        chip_off = jnp.arange(tokens)
        chip_pos = jnp.concatenate([z * tokens + chip_off, (2 * nz - 1 - z) * tokens + chip_off])
        cos_c, sin_c = rope_tables(chip_pos)
        neg = (lse_fwd * (-1.0 / SM_SCALE)).reshape(tokens, 2, kv_heads // 2, per_kv)
        hi = lax.reduce_precision(neg, 8, 7)
        mid = lax.reduce_precision(neg - hi, 8, 7)
        low = neg - hi - mid
        zero = jnp.zeros((tokens, 2, kv_heads // 2, HEAD_DIM - 3 * per_kv), F32)
        lse_arr = jnp.concatenate([hi, mid, low, zero], -1).transpose(1, 2, 0, 3)[:, :, :, None, :]
        dq_raw, dkv, dw = mega(nz, q_raw, d_out, out_fwd, lse_arr, kv, cos_c[:, None], sin_c[:, None], q_norm.reshape(1, HEAD_DIM))
        total = dkv.transpose(2, 1, 4, 0, 3).reshape(2, tokens, kv_heads, HEAD_DIM)
        dk_raw, dk_weight = pull_k(total[0] * SM_SCALE)
        sums = jnp.concatenate([jnp.sum(dw, axis=0)[None], dk_weight[None], jnp.zeros((6, HEAD_DIM), F32)], axis=0)
        sums = sum_over_ring(cp_size, sums)
        return dq_raw, dk_raw.astype(BF16), total[1].astype(BF16), sums[0], sums[1]

    row_spec = P(('dp', 'cp'))
    in_specs = (row_spec, row_spec, row_spec, row_spec, row_spec, row_spec, P(), P())
    out_specs = (row_spec, row_spec, row_spec, P('dp'), P('dp'))
    return jax.shard_map(local_grads, mesh=mesh, in_specs=in_specs, out_specs=out_specs, check_vma=False)
```

```python
import functools

import jax
import jax.numpy as jnp
import numpy as np
from jax import lax
from jax.experimental import pallas as pl
from jax.experimental.pallas import tpu as pltpu
from jax.sharding import PartitionSpec as P

HEAD_DIM = 128
ROPE_THETA = 1000000.0
NORM_EPS = 1e-6
SM_SCALE = HEAD_DIM ** -0.5
EXP_SCALE = SM_SCALE * 1.4426950408889634
F32, BF16 = jnp.float32, jnp.bfloat16
MESH = pl.DeviceIdType.MESH
PAIR = range(2)

ORDER = (43817265, 48172635)
GATHER = (3, 2, 229, 292, 519, 550, 585, 595, 616, 658, 683, 693, 682, 724, 823, 822, 1016, 1049, 1178, 1179)
REDUCE = (400, 402, 654, 652, 717, 719, 970, 971, 1097, 1158, 1223, 1392, 1394, 1477, 1647, 1646, 1709, 1667, 1708, 1899, 1962,
    2089, 2598, 2791, 2789, 3171, 3201, 3233)
GATHER_RIGHT = (34444334, 34344333, 443, 4333)
GATHER_LEFT = (43333443, 43433444, 1234334, 1233444)
REDUCE_RIGHT = (43434433, 33444334, 1233344, 1233443)
REDUCE_LEFT = (34343344, 44333443, 4433, 4334)
PREP_TOKENS = 32


def digits(numbers):
    return [int(c) for n in numbers for c in str(n).zfill(8)]


GATHER_REACH = (digits(GATHER_RIGHT), digits(GATHER_LEFT))
REDUCE_REACH = (digits(REDUCE_RIGHT), digits(REDUCE_LEFT))
GATHER_AT = [n // 32 for n in GATHER]
GATHER_CODE = [n % 32 for n in GATHER]
REDUCE_AT = [n // 64 for n in REDUCE]
REDUCE_CODE = [n % 64 for n in REDUCE]
SLOTS = [[4 * int(d) + j for d in str(order) for j in range(3 if d == '4' else 2)] for order in ORDER]


def dot(a, b, ca, cb):
    return lax.dot_general(a, b, (((ca,), (cb,)), ((), ())), preferred_element_type=F32)


def lane_sum(x):
    return jnp.sum(x, axis=-1, keepdims=True)


def lane_mean(x):
    return lane_sum(x) * (1.0 / HEAD_DIM)


def roll_half(x):
    return pltpu.roll(x, HEAD_DIM // 2, axis=x.ndim - 1)


def row_sum(prod, ones):
    high = prod.astype(BF16)
    low = (prod - high.astype(F32)).astype(BF16)
    return dot(jnp.concatenate([high, low], 1), ones, 1, 0)


def select_const(index, values):
    if len(values) == 1:
        return jnp.int32(values[0])
    top = 1 << ((len(values) - 1).bit_length() - 1)
    low, high = select_const(index, values[:top]), select_const(index, values[top:])
    return jnp.where((index & top) != 0, high, low)


def packed(index, values, bits):
    per, shift = (4, 2) if bits > 3 else (8, 3)
    words = []
    for i in range(0, len(values), per):
        words.append(sum(v << (bits * k) for k, v in enumerate(values[i:i + per])))
    return (select_const(index >> shift, words) >> ((index & (per - 1)) * bits)) & ((1 << bits) - 1)


def split(code, *bits):
    out = []
    for b in reversed(bits):
        out.append(code & ((1 << b) - 1))
        code = code >> b
    return out[::-1]


def action_masks(nz, sequence, active):
    words = []
    for direction in PAIR:
        chips = [[int(active(direction, zz, *act)) for act in sequence] for zz in range(nz)]
        words.append([[sum(bit << k for k, bit in enumerate(c[i:i + 16])) for c in chips] for i in range(0, len(sequence), 16)])
    return words


def count_at(table, last):
    return [sum(1 for at in table if at == g) for g in range(last)]


def mega_kernel(nz, chunk, per_kv, kv_heads,
                q_hbm, do_hbm, out_hbm, lse_hbm, k_hbm, v_hbm, offc3_hbm, offs3_hbm, offc_hbm, offs_hbm, basec_ref, bases_ref, qw_ref, kw_ref,
                dq_hbm, dkv_hbm, w_ref,
                xq, xdo, xout, qb_a, qb_b, aux_a, aux_b, dq, dq_b, kvall, acc, rsb, kland, lland, pieces, cos_t, sin_t, cos_d, sin_d, kout, dwq, wmine, wslots,
                in_sem, sw_snd, sw_rcv, ld_sem, xs_sem, xr_sem, tab_sem,
                ag_send, ag_recv, rs_send, rs_recv, dq_loc, dq_snd, dq_rcv, dk_loc, dk_snd, dk_rcv, w_snd, w_rcv):
    me = lax.axis_index('cp')
    cp = 2 * nz
    z, core = me // 2, me % 2
    other = 1 - core
    sib = 2 * z + other
    right = 2 * lax.rem(z + 1, nz) + core
    left = 2 * lax.rem(z + nz - 1, nz) + core
    tok = 2 * chunk
    rows = tok * per_kv
    qb, aux, dqs = (qb_a, qb_b), (aux_a, aux_b), (dq, dq_b)
    k_rows = tok * kv_heads

    def wrap(i):
        return (i + 2 * nz) & (nz - 1)

    def to(device):
        return dict(device_id={'cp': device}, device_id_type=MESH)

    barrier = pltpu.get_barrier_semaphore()

    def say(i, carry):
        pl.semaphore_signal(barrier, inc=1, **to(lax.rem(me + i, cp)))
        return carry

    lax.fori_loop(1, cp, say, 0)

    def off_of(el, mine):
        return pl.multiple_of((core if (el == 0) == mine else other) * chunk, chunk)

    def x_rows(h, el, token, count):
        return pl.ds(pl.multiple_of(((h * 2 + el) * tok + token) * per_kv, chunk), count * per_kv)

    def h_rows(el, token, count):
        return pl.ds(pl.multiple_of((el * tok + token) * per_kv, chunk), count * per_kv)

    lands = ((k_hbm, kland.at[0]), (v_hbm, kland.at[1]), (lse_hbm, lland))
    own_in = [pltpu.make_async_copy(hbm, buf.at[0], in_sem.at[i]) for i, (hbm, buf) in enumerate(lands)]
    swaps = [pltpu.make_async_remote_copy(hbm, buf.at[1], sw_snd.at[i], sw_rcv.at[i], **to(sib)) for i, (hbm, buf) in enumerate(lands)]
    tables = [pltpu.make_async_copy(src, dst, tab_sem.at[i]) for i, (src, dst) in enumerate((
        (offc_hbm, cos_d.at[pl.ds(0, tok)]), (offs_hbm, sin_d.at[pl.ds(0, tok)]),
        (offc3_hbm, cos_t.at[pl.ds(0, tok)]), (offs3_hbm, sin_t.at[pl.ds(0, tok)])))]
    loads = []
    for h in PAIR:
        for el in PAIR:
            heads = lambda c: pl.ds(pl.multiple_of((2 * c + h) * per_kv, per_kv), per_kv)
            src = pl.ds(el * chunk, chunk)
            dst = x_rows(h, el, off_of(el, True), chunk)
            row = []
            for i, (hbm, buf) in enumerate(((q_hbm, xq), (do_hbm, xdo), (out_hbm, xout))):
                there = buf.at[dst].reshape(chunk, per_kv, HEAD_DIM)
                row.append((pltpu.make_async_copy(hbm.at[src, heads(core), :], there, ld_sem.at[h, el, i]),
                            pltpu.make_async_remote_copy(hbm.at[src, heads(other), :], there, xs_sem.at[h, el, i], xr_sem.at[h, el, i],
                                                         **to(sib))))
            loads.append(row)
    for cpy in own_in + tables:
        cpy.start()
    for row in loads:
        for loc, _ in row:
            loc.start()
    acc[...] = jnp.zeros_like(acc)
    dq_b[...] = jnp.zeros_like(dq_b)

    def base(el):
        blk = z if el == 0 else 2 * nz - 1 - z
        return basec_ref[blk], bases_ref[blk]

    def turn(cos_ref, sin_ref, lift):
        for el in (1, 0):
            bc, bs = base(el)
            bc, bs = lift(bc), lift(bs)
            step = 32

            def part(i, carry):
                src = pl.ds(pl.multiple_of(i * step, step), step)
                dst = pl.ds(pl.multiple_of(el * tok + i * step, step), step)
                oc, os = cos_ref[src], sin_ref[src]
                cos_ref[dst] = bc * oc - bs * os
                sin_ref[dst] = bs * oc + bc * os
                return carry

            lax.fori_loop(0, tok // step, part, 0)

    for t in tables:
        t.wait()
    turn(cos_d, sin_d, lambda x: x)
    turn(cos_t, sin_t, lambda x: x[:, None, :])

    def raw_rows(what, side):
        return pl.ds((what * 2 + side) * k_rows, k_rows)

    def raw(what, side, h, el):
        return dq[pl.ds((what * 2 + side) * k_rows + el * chunk * kv_heads + 2 * core + h, chunk, stride=kv_heads), :]

    def unpack_keys(what, side):
        dq[raw_rows(what, side), :] = kland[what, side].astype(F32)

    kw = kw_ref[...]

    def keys_of(side):
        for i in PAIR:
            unpack_keys(i, side)
        for h in PAIR:
            for el in PAIR:
                off = off_of(el, side == 0)
                x = raw(0, side, h, el)
                y = x * lax.rsqrt(lane_mean(x * x) + NORM_EPS) * kw
                tabs = pl.ds(pl.multiple_of(el * tok + off, chunk), chunk)
                kvall[z, h, el, 0, pl.ds(off, chunk), :] = (y * cos_d[tabs] + roll_half(y) * sin_d[tabs]).astype(BF16)
                kvall[z, h, el, 1, pl.ds(off, chunk), :] = raw(1, side, h, el).astype(BF16)

    n_l = 3 * per_kv
    lane_c = lax.broadcasted_iota(jnp.int32, (chunk, HEAD_DIM), 1)

    def pieces_of(side):
        for h in PAIR:
            for el in PAIR:
                val = lland[side, pl.ds(el * chunk, chunk), :] * (-1.0 / SM_SCALE)
                val = jnp.concatenate([val, jnp.zeros((chunk, HEAD_DIM - val.shape[1]), F32)], axis=1)
                val = pltpu.roll(val, (HEAD_DIM - (2 * core + h) * per_kv) & (HEAD_DIM - 1), axis=1)
                hi = val.astype(BF16).astype(F32)
                mid = (val - hi).astype(BF16).astype(F32)
                low = val - hi - mid
                pc = jnp.where(lane_c < per_kv, hi, jnp.where(lane_c < 2 * per_kv, pltpu.roll(mid, per_kv, axis=1),
                               jnp.where(lane_c < n_l, pltpu.roll(low, 2 * per_kv, axis=1), 0.0)))
                pieces[h, pl.ds(pl.multiple_of(el * tok + off_of(el, side == 0), chunk), chunk)] = pc[:, None, :]

    for cpy in own_in:
        cpy.wait()
    keys_of(0)
    pieces_of(0)
    pl.semaphore_wait(barrier, cp - 1)
    for cpy in swaps:
        cpy.start()
    for row in loads:
        for _, rem in row:
            rem.start()
    for i in PAIR:
        swaps[i].wait_recv()
    keys_of(1)

    def lives(reach, el, h, hop, owner):
        return 1 <= hop <= reach[(el * 2 + h) * nz + owner % nz]

    sides = (1, -1)
    g_seq, r_seq = [split(c, 1, 3, 1) for c in GATHER_CODE], [split(c, 1, 3, 1, 1) for c in REDUCE_CODE]
    g_wait, g_send, r_wait, r_send = (
        [[select_const(z, w) for w in words] for words in action_masks(nz, seq, active)] for seq, active in (
            (g_seq, lambda dr, zz, h, s, el: lives(GATHER_REACH[dr], el, h, s - 1, zz - sides[dr] * (s - 1))),
            (g_seq, lambda dr, zz, h, s, el: lives(GATHER_REACH[dr], el, h, s, zz - sides[dr] * (s - 1))),
            (r_seq, lambda dr, zz, h, d, el, on: on and lives(REDUCE_REACH[dr], el, h, d + 1, zz + sides[dr] * d)),
            (r_seq, lambda dr, zz, h, d, el, on: lives(REDUCE_REACH[dr], el, h, d, zz + sides[dr] * d)
             and on == lives(REDUCE_REACH[dr], el, h, d + 1, zz + sides[dr] * d))))

    def on(words, index):
        word = words[0]
        for i, w in enumerate(words[1:], 1):
            word = jnp.where(index >> 4 == i, w, word)
        return (word >> (index & 15)) & 1 == 1

    def gather_owner(direction, s):
        return wrap(z - sides[direction] * s)

    def gather_copy(direction, h, s, el):
        ref = kvall.at[gather_owner(direction, s - 1), h, el]
        return pltpu.make_async_remote_copy(ref, ref, ag_send.at[direction, h, s - 1, el], ag_recv.at[direction, h, s - 1, el],
                                            **to((right, left)[direction]))

    def gather_arrival(direction, h, s, el):
        ref = kvall.at[gather_owner(direction, s), h, el]
        return pltpu.make_async_remote_copy(ref, ref, ag_send.at[direction, h, s - 1, el], ag_recv.at[direction, h, s - 1, el],
                                            **to((right, left)[direction]))

    def gather_step(a):
        h, s, el = split(packed(a, GATHER_CODE, 5), 1, 3, 1)
        for direction in PAIR:
            @pl.when(on(g_wait[direction], a))
            def _():
                gather_arrival(direction, h, s - 1, el).wait_recv()

            @pl.when(on(g_send[direction], a))
            def _():
                gather_copy(direction, h, s, el).start()

    def reduce_copy(direction, h, d, el):
        return pltpu.make_async_remote_copy(acc.at[wrap(z + sides[direction] * d), h, el], rsb.at[direction, d - 1, h, el],
                                            rs_send.at[direction, d - 1, h, el], rs_recv.at[direction, d - 1, h, el],
                                            **to((right, left)[direction]))

    def reduce_arrival(direction, h, d, el):
        return pltpu.make_async_remote_copy(acc.at[wrap(z + sides[direction] * d), h, el], rsb.at[direction, d, h, el],
                                            rs_send.at[direction, d, h, el], rs_recv.at[direction, d, h, el],
                                            **to((right, left)[direction]))

    def reduce_step(b):
        h, d, el, _ = split(packed(b, REDUCE_CODE, 6), 1, 3, 1, 1)
        for direction in PAIR:
            @pl.when(on(r_wait[direction], b))
            def _():
                reduce_arrival(direction, h, d, el).wait_recv()
                acc[wrap(z + sides[direction] * d), h, el] += rsb[direction, d, h, el]

            @pl.when(on(r_send[direction], b))
            def _():
                reduce_copy(direction, h, d, el).start()

    def run_actions(step, first, count):
        def one(i, carry):
            step(i)
            return carry

        lax.fori_loop(first, first + count, one, 0)
        return first + count

    head_steps = 3 + 2 * (nz - 1)
    n_steps = 2 * head_steps
    n_pieces = 2 * tok // PREP_TOKENS
    first = n_pieces + 1
    n_ticks = n_steps + n_pieces
    gather_counts = count_at(GATHER_AT, first + n_ticks)
    reduce_counts = count_at(REDUCE_AT, n_ticks)

    def ticks(g, done):
        ga = run_actions(gather_step, done[0], packed(first + g, gather_counts, 3))
        ra = run_actions(reduce_step, done[1], packed(g, reduce_counts, 4))
        return ga, ra

    gathered = run_actions(gather_step, 0, gather_counts[0])

    dq[...] = jnp.zeros_like(dq)

    swaps[2].wait_recv()
    pieces_of(1)

    sub = PREP_TOKENS
    weight = qw_ref[...]
    ones = jnp.ones((2 * HEAD_DIM, HEAD_DIM), BF16)
    lane = lax.broadcasted_iota(jnp.int32, (sub * per_kv, HEAD_DIM), 1)
    head = lax.rem(lax.broadcasted_iota(jnp.int32, (sub * per_kv, HEAD_DIM), 0), per_kv)
    lse_mask = (lane == head) | (lane == head + per_kv) | (lane == head + 2 * per_kv)
    flat = lambda x: x.reshape(x.shape[0] * per_kv, HEAD_DIM)
    tall = lambda x: x.reshape(x.shape[0] // per_kv, per_kv, HEAD_DIM)

    def sums(prod, on_mxu):
        return row_sum(prod, ones) if on_mxu else lane_sum(prod)

    def prepare(h, el, t0, on_mxu):
        tabs = pl.ds(pl.multiple_of(el * tok + t0, sub), sub)
        r = x_rows(h, el, t0, sub)
        x = xq[r, :].astype(F32)
        ms = sums(x * x, on_mxu) * (1.0 / HEAD_DIM)
        y = tall(x * lax.rsqrt(ms + NORM_EPS) * weight)
        hr = h_rows(el, t0, sub)
        qb[h][hr, :] = flat(y * cos_t[tabs] + roll_half(y) * sin_t[tabs]).astype(BF16)
        r0 = -sums(xdo[r, :].astype(F32) * xout[r, :].astype(F32), on_mxu)
        r1 = r0 - r0.astype(BF16).astype(F32)
        r2 = r1 - r1.astype(BF16).astype(F32)
        dpart = jnp.where(lane == n_l, r0, jnp.where(lane == n_l + 1, r1, jnp.where(lane == n_l + 2, r2, 0.0)))
        consts = flat(jnp.broadcast_to(pieces[h, tabs], (sub, per_kv, HEAD_DIM)))
        aux[h][hr, :] = jnp.where(lse_mask, consts, dpart).astype(BF16)

    def finish(h, el, t0, on_mxu):
        tabs = pl.ds(pl.multiple_of(el * tok + t0, sub), sub)
        r = x_rows(h, el, t0, sub)
        x = xq[r, :].astype(F32)
        rstd = lax.rsqrt(sums(x * x, on_mxu) * (1.0 / HEAD_DIM) + NORM_EPS)
        xhat = x * rstd
        hr = h_rows(el, t0, sub)
        gq = tall(dqs[h][hr, :] * SM_SCALE)
        dy = flat(gq * cos_t[tabs] - roll_half(gq) * sin_t[tabs])
        dxh = dy * weight
        qb[h][hr, :] = (rstd * (dxh - xhat * lane_mean(dxh * xhat))).astype(BF16)
        return jnp.sum((dy * xhat).reshape(-1, 8, HEAD_DIM), axis=0)

    def piece_at(i):
        el = jnp.where(i >= n_pieces // 2, 1, 0)
        return el, (i - el * (n_pieces // 2)) * sub

    for part in PAIR:
        for el in PAIR:
            for loc, rem in loads[el]:
                if part == 0:
                    loc.wait()
                else:
                    rem.wait_recv()
        n = chunk // sub

        def piece(i, gathered):
            el = jnp.where(i >= n, 1, 0)
            mine = core if part == 0 else other
            prepare(0, el, jnp.where(el == 0, mine, 1 - mine) * chunk + (i - el * n) * sub, True)
            return run_actions(gather_step, gathered, packed(1 + part * 2 * n + i, gather_counts, 3))

        gathered = lax.fori_loop(0, 2 * n, piece, gathered)
    for el in PAIR:
        for loc, rem in loads[2 + el]:
            loc.wait()
            rem.wait_recv()
    dwq[...] = jnp.zeros_like(dwq)

    keys = tok
    klane = lax.broadcasted_iota(jnp.int32, (keys, HEAD_DIM), 1)
    ones_k = jnp.where(klane < n_l, 1.0, 0.0).astype(BF16)
    ones_v = jnp.where((klane >= n_l) & (klane < n_l + 3), 1.0, 0.0).astype(BF16)
    klan = lax.broadcasted_iota(jnp.int32, (per_kv, keys), 1)

    def work(h, g, done):
        u = g - h * head_steps
        slot = packed(u, SLOTS[h], 6)
        delta, j = (slot >> 2) - 4, slot & 3
        own = delta == 0
        kz = wrap(z + delta)
        lower = kz < z
        q_late = jnp.where(own, jnp.where(j >= 1, 1, 0), jnp.where(lower, j, 1))
        k_late = jnp.where(own, jnp.where(j >= 2, 1, 0), jnp.where(lower, 0, j))
        q_blk = jnp.where(q_late == 1, 2 * nz - 1 - z, z)
        k_blk = jnp.where(k_late == 1, 2 * nz - 1 - kz, kz)
        off = (q_blk - k_blk) * tok
        r = pl.ds(pl.multiple_of((h * 2 + q_late) * rows, rows), rows)
        k, v = kvall[kz, h, k_late, 0], kvall[kz, h, k_late, 1]
        hr = pl.ds(pl.multiple_of(q_late * rows, rows), rows)
        qq, ax, dd = qb[h][hr, :], aux[h][hr, :], xdo[r, :]
        s = dot(jnp.concatenate([qq, ax], 1), jnp.concatenate([k, ones_k], 1), 1, 1)
        dp = dot(jnp.concatenate([dd, ax], 1), jnp.concatenate([v, ones_v], 1), 1, 1)
        p = jnp.exp2(s * EXP_SCALE)
        p = jnp.concatenate([jnp.where(klan <= off + t, p[per_kv * t:per_kv * (t + 1)], 0.0) for t in range(tok)], 0)
        ds = (p * dp).astype(BF16)
        pb = p.astype(BF16)
        dqs[h][hr, :] += dot(ds, k, 1, 0)
        acc[kz, h, k_late, 0] += dot(qq, ds, 0, 0)
        acc[kz, h, k_late, 1] += dot(dd, pb, 0, 0)
        el, t0 = piece_at(jnp.minimum(u, n_pieces - 1))
        if h == 0:
            prepare(1, el, t0, False)
        else:
            dwq[...] += jnp.where(u < n_pieces, finish(0, el, t0, False), 0.0)
        return ticks(g, done)

    done = (gathered, jnp.int32(0))
    for h in PAIR:
        done = lax.fori_loop(h * head_steps, (h + 1) * head_steps, functools.partial(work, h), done)

    def last(i, done):
        el, t0 = piece_at(i)
        dwq[...] += finish(1, el, t0, True)
        return ticks(n_steps + i, done)

    done = lax.fori_loop(0, n_pieces, last, done)

    def back(x, ssum, g, cos, sin, w):
        rstd = lax.rsqrt(ssum * (1.0 / HEAD_DIM) + NORM_EPS)
        xhat = x * rstd
        dy = g * cos - roll_half(g) * sin
        dxh = dy * w
        dx = rstd * (dxh - xhat * lane_mean(dxh * xhat))
        return dx, jnp.sum((dy * xhat).reshape(-1, 8, HEAD_DIM), axis=0)

    outs = []
    for h in PAIR:
        for el in PAIR:
            heads = pl.ds(pl.multiple_of((2 * core + h) * per_kv, per_kv), per_kv)
            dst = dq_hbm.at[pl.ds(el * chunk, chunk), heads, :]
            part = lambda mine: qb[h].at[h_rows(el, off_of(el, mine), chunk)].reshape(chunk, per_kv, HEAD_DIM)
            outs.append((pltpu.make_async_copy(part(True), dst, dq_loc.at[h, el]),
                         pltpu.make_async_remote_copy(part(False), dst, dq_snd.at[h, el], dq_rcv.at[h, el], **to(sib))))
    for loc, rem in outs:
        loc.start()
        rem.start()
    for side in PAIR:
        unpack_keys(0, side)

    run_actions(reduce_step, done[1], len(REDUCE) - done[1])

    hold = 4 * k_rows
    dwk = jnp.zeros((8, HEAD_DIM), F32)
    for h in PAIR:
        for el in PAIR:
            kout[h, el, 1] = acc[z, h, el, 1].T.astype(BF16)
            dq[pl.ds(hold, tok), :] = acc[z, h, el, 0].T * SM_SCALE
            for side in PAIR:
                off = off_of(el, side == 0)
                x = raw(0, side, h, el)
                tabs = pl.ds(pl.multiple_of(el * tok + off, chunk), chunk)
                dx, dwp = back(x, lane_sum(x * x), dq[pl.ds(pl.multiple_of(hold + off, chunk), chunk), :],
                               cos_d[tabs], sin_d[tabs], kw)
                kout[h, el, 0, pl.ds(off, chunk), :] = dx.astype(BF16)
                dwk = dwk + dwp
            hold += tok
    top = lax.broadcasted_iota(jnp.int32, (8, HEAD_DIM), 0)
    wmine[...] = jnp.where(top == 0, jnp.sum(dwq[...], axis=0, keepdims=True),
                           jnp.where(top == 1, jnp.sum(dwk, axis=0, keepdims=True), 0.0))

    def weight_copy(i):
        return pltpu.make_async_remote_copy(wmine, wslots.at[cp - i], w_snd.at[i], w_rcv.at[cp - i], **to(lax.rem(me + i, cp)))

    def weight_send(i, carry):
        weight_copy(i).start()
        return carry

    lax.fori_loop(1, cp, weight_send, 0)
    for h in PAIR:
        for el in PAIR:
            dst = dkv_hbm.at[2 * core + h, el]
            outs.append((pltpu.make_async_copy(kout.at[h, el, :, pl.ds(off_of(el, True), chunk), :], dst, dk_loc.at[h, el]),
                         pltpu.make_async_remote_copy(kout.at[h, el, :, pl.ds(off_of(el, False), chunk), :], dst, dk_snd.at[h, el],
                                                      dk_rcv.at[h, el], **to(sib))))
    for loc, rem in outs[4:]:
        loc.start()
        rem.start()

    for cpy in swaps:
        cpy.wait_send()
    for row in loads:
        for _, rem in row:
            rem.wait_send()

    def drain_gather(a, carry):
        h, s, el = split(packed(a, GATHER_CODE, 5), 1, 3, 1)
        for direction in PAIR:
            @pl.when(on(g_send[direction], a))
            def _():
                gather_copy(direction, h, s, el).wait_send()
        return carry

    def drain_reduce(b, carry):
        h, d, el, _ = split(packed(b, REDUCE_CODE, 6), 1, 3, 1, 1)
        for direction in PAIR:
            @pl.when(on(r_send[direction], b))
            def _():
                reduce_copy(direction, h, d, el).wait_send()
        return carry

    lax.fori_loop(0, len(GATHER), drain_gather, 0)
    lax.fori_loop(0, len(REDUCE), drain_reduce, 0)

    def weight_wait(i, carry):
        pltpu.make_async_remote_copy(wmine, wslots.at[i], w_snd.at[i], w_rcv.at[i], **to(lax.rem(me + i, cp))).wait()
        return carry

    lax.fori_loop(1, cp, weight_wait, 0)
    wslots[0] = wmine[...]
    w_ref[...] = lax.fori_loop(0, cp, lambda i, total: total + wslots[lax.rem(i - me + cp, cp)], jnp.zeros((8, HEAD_DIM), F32))
    for loc, rem in outs:
        loc.wait()
        rem.wait()


def mega(nz, kv_heads, q_raw, d_out, out_fwd, lse, k_rows, v_rows, offc, offs, basec, bases, qw, kw):
    tok, heads, hd = q_raw.shape
    chunk, per_kv = tok // 2, heads // kv_heads
    any_spec = pl.BlockSpec(memory_space=pl.ANY)
    vmem = pl.BlockSpec(memory_space=pltpu.VMEM)
    dma, scr = pltpu.SemaphoreType.DMA, pltpu.VMEM
    n_rows = 2 * tok * per_kv
    hbm = lambda a: pltpu.with_memory_space_constraint(a, pltpu.HBM)
    args = [q_raw, d_out, out_fwd, lse, k_rows, v_rows, offc[:, None], offs[:, None], offc, offs]
    return pl.pallas_call(
        functools.partial(mega_kernel, nz, chunk, per_kv, kv_heads),
        in_specs=[any_spec] * len(args) + [vmem] * 4,
        out_specs=[any_spec, any_spec, vmem],
        out_shape=[jax.ShapeDtypeStruct(q_raw.shape, BF16), jax.ShapeDtypeStruct((kv_heads, 2, 2, chunk, hd), BF16),
                   jax.ShapeDtypeStruct((8, hd), F32)],
        scratch_shapes=[
            *[scr((2 * n_rows, hd), BF16)] * 3, *[scr((n_rows, hd), BF16)] * 4, *[scr((n_rows, hd), F32)] * 2,
            scr((nz, 2, 2, 2, tok, hd), BF16), scr((nz, 2, 2, 2, hd, tok), F32), scr((2, 4, 2, 2, 2, hd, tok), F32),
            scr((2, 2) + k_rows.shape, BF16), scr((2,) + lse.shape, F32), scr((2, 2 * tok, 1, hd), F32),
            *[scr((2 * tok, 1, hd), F32)] * 2, *[scr((2 * tok, hd), F32)] * 2,
            scr((2, 2, 2, tok, hd), BF16), *[scr((8, hd), F32)] * 2, scr((2 * nz, 8, hd), F32),
            *[dma((3,))] * 3, *[dma((2, 2, 3))] * 3, dma((4,)), *[dma((2, 2, 4, 2))] * 2, *[dma((2, 4, 2, 2))] * 2,
            *[dma((2, 2))] * 6, *[dma((2 * nz,))] * 2,
        ],
        name='attn_bwd',
        compiler_params=pltpu.CompilerParams(vmem_limit_bytes=67000000, collective_id=0, has_side_effects=True),
    )(*[hbm(a) for a in args], basec, bases, qw, kw)


def emit_kernel(dq_in, dkv_in, dq_out, dk_out, dv_out):
    dq_out[...] = dq_in[...]
    for ref, i in ((dk_out, 0), (dv_out, 1)):
        x = dkv_in[:, 0, i].astype(F32)
        ref[...] = jnp.stack([x[h] for h in range(x.shape[0])], axis=1).astype(BF16)


def emit(dq, dkv):
    tok, heads, hd = dq.shape
    kv_heads, _, _, chunk, _ = dkv.shape
    step = 32
    per = chunk // step
    return pl.pallas_call(
        emit_kernel,
        grid=(tok // step,),
        in_specs=[pl.BlockSpec((step, heads, hd), lambda i: (i, 0, 0)),
                  pl.BlockSpec((kv_heads, 1, 2, step, hd), lambda i: (0, i // per, 0, i % per, 0))],
        out_specs=[pl.BlockSpec((step, heads, hd), lambda i: (i, 0, 0)), pl.BlockSpec((step, kv_heads, hd), lambda i: (i, 0, 0)),
                   pl.BlockSpec((step, kv_heads, hd), lambda i: (i, 0, 0))],
        out_shape=[jax.ShapeDtypeStruct(dq.shape, BF16)] + [jax.ShapeDtypeStruct((tok, kv_heads, hd), BF16)] * 2,
        name='emit',
    )(dq, dkv)


def solution(mesh):
    cp_size = mesh.shape['cp']
    nz = cp_size // 2

    def local_grads(q_raw, k_raw, v_proj, out_fwd, lse_fwd, d_out, q_norm, k_norm):
        tok, kv_heads = k_raw.shape[0], k_raw.shape[1]
        inv_freq = ROPE_THETA ** (-np.arange(0, HEAD_DIM, 2, dtype=np.float64) / HEAD_DIM)
        inv_freq = np.concatenate([inv_freq, inv_freq])
        sign = np.where(np.arange(HEAD_DIM) < HEAD_DIM // 2, -1.0, 1.0)
        off_ang = np.arange(tok)[:, None] * inv_freq
        base_ang = (np.arange(cp_size) * tok)[:, None] * inv_freq
        table = lambda x: jnp.asarray(x, F32)
        rows = lambda a: a.reshape(tok * kv_heads, HEAD_DIM)
        dq_raw, dkv, sums = mega(nz, kv_heads, q_raw, d_out, out_fwd, lse_fwd, rows(k_raw), rows(v_proj),
                                 table(np.cos(off_ang)), table(np.sin(off_ang) * sign),
                                 table(np.cos(base_ang))[:, None], table(np.sin(base_ang) * sign)[:, None],
                                 q_norm.reshape(1, HEAD_DIM), k_norm.reshape(1, HEAD_DIM))
        dq_raw, dk_raw, dv = emit(dq_raw, dkv)
        return dq_raw, dk_raw, dv, sums[0], sums[1]

    row_spec = P(('dp', 'cp'))
    in_specs = (row_spec, row_spec, row_spec, row_spec, row_spec, row_spec, P(), P())
    out_specs = (row_spec, row_spec, row_spec, P('dp'), P('dp'))
    return jax.shard_map(local_grads, mesh=mesh, in_specs=in_specs, out_specs=out_specs, check_vma=False)
```

```python
import functools

import jax
import jax.numpy as jnp
import numpy as np
from jax import lax
from jax.experimental import pallas as pl
from jax.experimental.pallas import tpu as pltpu
from jax.sharding import PartitionSpec as P

HEAD_DIM = 128
ROPE_THETA = 1000000.0
NORM_EPS = 1e-6
SM_SCALE = HEAD_DIM ** -0.5
EXP_SCALE = SM_SCALE * 1.4426950408889634
F32, BF16 = jnp.float32, jnp.bfloat16
MESH = pl.DeviceIdType.MESH
PAIR = range(2)

ORDER = (46781235, 78136245)
GATHER = (356001960000600070, 1674014820106000388, 2382023180218402120, 2578024720244402508, 2704027680264202664,
    2982029880302802918, 3306031800303002964, 3566035680337003376, 4212040820401403892, 459804402)
REDUCE = (1106010420078000650, 1614014170148701232, 2054018070186901678, 2505023150225102053, 2759026950260802674,
    3246031170305202738, 3819035250350303311, 4073040100388303753, 5315048670496704645, 5861057980576105287, 6497063710617706209,
    6435)
GATHER_RIGHT = (33344444, 44444333, 333, 333)
GATHER_LEFT = (44433333, 33333444, 1234444, 1234444)
REDUCE_RIGHT = (33333333, 44444444, 1233444, 1234333)
REDUCE_LEFT = (44444444, 33333333, 4333, 444)
PREP_TOKENS = 32


def digits(numbers):
    return [int(c) for n in numbers for c in str(n).zfill(8)]


GATHER_REACH = (digits(GATHER_RIGHT), digits(GATHER_LEFT))
REDUCE_REACH = (digits(REDUCE_RIGHT), digits(REDUCE_LEFT))


def unpacked(numbers):
    out = []
    for n in numbers:
        while n:
            out.append(n % 100000)
            n //= 100000
    return out


G_SEQ, R_SEQ = unpacked(GATHER), unpacked(REDUCE)
GATHER_AT, GATHER_CODE = [n >> 7 for n in G_SEQ], [n & 127 for n in G_SEQ]
REDUCE_AT, REDUCE_CODE = [n >> 7 for n in R_SEQ], [n & 127 for n in R_SEQ]
SLOTS = [[4 * int(d) + j for d in str(order) for j in range(3 if d == '4' else 2)] for order in ORDER]


def dot(a, b, ca, cb):
    return lax.dot_general(a, b, (((ca,), (cb,)), ((), ())), preferred_element_type=F32)


def lane_sum(x):
    return jnp.sum(x, axis=-1, keepdims=True)


def lane_mean(x):
    return lane_sum(x) * (1.0 / HEAD_DIM)


def roll_half(x):
    return pltpu.roll(x, HEAD_DIM // 2, axis=x.ndim - 1)


def row_sum(prod, ones):
    high = prod.astype(BF16)
    low = (prod - high.astype(F32)).astype(BF16)
    return dot(jnp.concatenate([high, low], 1), ones, 1, 0)


def select_const(index, values):
    if len(values) == 1:
        return jnp.int32(values[0])
    top = 1 << ((len(values) - 1).bit_length() - 1)
    low, high = select_const(index, values[:top]), select_const(index, values[top:])
    return jnp.where((index & top) != 0, high, low)


def packed(index, values, bits):
    per, shift = (4, 2) if bits > 3 else (8, 3)
    assert max(values) < 1 << bits
    words = []
    for i in range(0, len(values), per):
        words.append(sum(v << (bits * k) for k, v in enumerate(values[i:i + per])))
    return (select_const(index >> shift, words) >> ((index & (per - 1)) * bits)) & ((1 << bits) - 1)


def split(code, *bits):
    out = []
    for b in reversed(bits):
        out.append(code & ((1 << b) - 1))
        code = code >> b
    return out[::-1]


def action_masks(nz, sequence, active):
    chips = [[int(active(zz, *act)) for act in sequence] for zz in range(nz)]
    return [[sum(bit << k for k, bit in enumerate(c[i:i + 16])) for c in chips] for i in range(0, len(sequence), 16)]


def count_at(table, last):
    return [sum(1 for at in table if at == g) for g in range(last)]


def mega_kernel(nz, chunk, per_kv, kv_heads,
                q_hbm, do_hbm, out_hbm, lse_hbm, k_hbm, v_hbm, offc3_hbm, offs3_hbm, offc_hbm, offs_hbm, basec_ref, bases_ref, qw_ref, kw_ref,
                dq_hbm, dkv_hbm, w_ref,
                xq, xdo, xout, qb_a, qb_b, aux_a, aux_b, dq, dq_b, kvall, acc, rsb, kland, lland, pieces, cos_t, sin_t, cos_d, sin_d, kout, dwq, wmine, wslots,
                in_sem, sw_snd, sw_rcv, ld_sem, xs_sem, xr_sem, tab_sem,
                ag_send, ag_recv, rs_send, rs_recv, dq_loc, dq_snd, dq_rcv, dk_loc, dk_snd, dk_rcv, w_snd, w_rcv):
    me = lax.axis_index('cp')
    cp = 2 * nz
    z, core = me // 2, me % 2
    other = 1 - core
    sib = 2 * z + other
    right = 2 * lax.rem(z + 1, nz) + core
    left = 2 * lax.rem(z + nz - 1, nz) + core
    tok = 2 * chunk
    rows = tok * per_kv
    qb, aux, dqs = (qb_a, qb_b), (aux_a, aux_b), (dq, dq_b)
    k_rows = tok * kv_heads

    def wrap(i):
        return (i + 2 * nz) & (nz - 1)

    def to(device):
        return dict(device_id={'cp': device}, device_id_type=MESH)

    barrier = pltpu.get_barrier_semaphore()

    def say(i, carry):
        pl.semaphore_signal(barrier, inc=1, **to(lax.rem(me + i, cp)))
        return carry

    lax.fori_loop(1, cp, say, 0)

    def off_of(el, mine):
        return pl.multiple_of((core if (el == 0) == mine else other) * chunk, chunk)

    def x_rows(h, el, token, count):
        return pl.ds(pl.multiple_of(((h * 2 + el) * tok + token) * per_kv, chunk), count * per_kv)

    def h_rows(el, token, count):
        return pl.ds(pl.multiple_of((el * tok + token) * per_kv, chunk), count * per_kv)

    lands = ((k_hbm, kland.at[0]), (v_hbm, kland.at[1]), (lse_hbm, lland))
    own_in = [pltpu.make_async_copy(hbm, buf.at[0], in_sem.at[i]) for i, (hbm, buf) in enumerate(lands)]
    swaps = [pltpu.make_async_remote_copy(hbm, buf.at[1], sw_snd.at[i], sw_rcv.at[i], **to(sib)) for i, (hbm, buf) in enumerate(lands)]
    tables = [pltpu.make_async_copy(src, dst, tab_sem.at[i]) for i, (src, dst) in enumerate((
        (offc_hbm, cos_d.at[pl.ds(0, tok)]), (offs_hbm, sin_d.at[pl.ds(0, tok)]),
        (offc3_hbm, cos_t.at[pl.ds(0, tok)]), (offs3_hbm, sin_t.at[pl.ds(0, tok)])))]
    loads = []
    for h in PAIR:
        for el in PAIR:
            heads = lambda c: pl.ds(pl.multiple_of((2 * c + h) * per_kv, per_kv), per_kv)
            src = pl.ds(el * chunk, chunk)
            dst = x_rows(h, el, off_of(el, True), chunk)
            row = []
            for i, (hbm, buf) in enumerate(((q_hbm, xq), (do_hbm, xdo), (out_hbm, xout))):
                there = buf.at[dst].reshape(chunk, per_kv, HEAD_DIM)
                row.append((pltpu.make_async_copy(hbm.at[src, heads(core), :], there, ld_sem.at[h, el, i]),
                            pltpu.make_async_remote_copy(hbm.at[src, heads(other), :], there, xs_sem.at[h, el, i], xr_sem.at[h, el, i],
                                                         **to(sib))))
            loads.append(row)
    for cpy in own_in + tables:
        cpy.start()
    for row in loads:
        for loc, _ in row:
            loc.start()
    def base(el):
        blk = z if el == 0 else 2 * nz - 1 - z
        return basec_ref[blk], bases_ref[blk]

    def turn(cos_ref, sin_ref, lift):
        for el in (1, 0):
            bc, bs = base(el)
            bc, bs = lift(bc), lift(bs)
            step = 32

            def part(i, carry):
                src = pl.ds(pl.multiple_of(i * step, step), step)
                dst = pl.ds(pl.multiple_of(el * tok + i * step, step), step)
                oc, os = cos_ref[src], sin_ref[src]
                cos_ref[dst] = bc * oc - bs * os
                sin_ref[dst] = bs * oc + bc * os
                return carry

            lax.fori_loop(0, tok // step, part, 0)

    for t in tables:
        t.wait()
    turn(cos_d, sin_d, lambda x: x)

    def raw_rows(what, side):
        return pl.ds((what * 2 + side) * k_rows, k_rows)

    def raw(what, side, h, el):
        return dq[pl.ds((what * 2 + side) * k_rows + el * chunk * kv_heads + 2 * core + h, chunk, stride=kv_heads), :]

    def unpack_keys(what, side):
        dq[raw_rows(what, side), :] = kland[what, side].astype(F32)

    kw = kw_ref[...]

    def keys_of(side):
        for i in PAIR:
            unpack_keys(i, side)
        for h in PAIR:
            for el in PAIR:
                off = off_of(el, side == 0)
                x = raw(0, side, h, el)
                y = x * lax.rsqrt(lane_mean(x * x) + NORM_EPS) * kw
                tabs = pl.ds(pl.multiple_of(el * tok + off, chunk), chunk)
                kvall[z, h, el, 0, pl.ds(off, chunk), :] = (y * cos_d[tabs] + roll_half(y) * sin_d[tabs]).astype(BF16)
                kvall[z, h, el, 1, pl.ds(off, chunk), :] = raw(1, side, h, el).astype(BF16)

    n_l = 3 * per_kv
    lane_c = lax.broadcasted_iota(jnp.int32, (chunk, HEAD_DIM), 1)

    def pieces_of(side):
        for h in PAIR:
            for el in PAIR:
                val = (lland[side, :, pl.ds(el * chunk, chunk)] * (-1.0 / SM_SCALE)).T
                val = jnp.concatenate([val, jnp.zeros((chunk, HEAD_DIM - val.shape[1]), F32)], axis=1)
                val = pltpu.roll(val, (HEAD_DIM - (2 * core + h) * per_kv) & (HEAD_DIM - 1), axis=1)
                hi = val.astype(BF16).astype(F32)
                mid = (val - hi).astype(BF16).astype(F32)
                low = val - hi - mid
                pc = jnp.where(lane_c < per_kv, hi, jnp.where(lane_c < 2 * per_kv, pltpu.roll(mid, per_kv, axis=1),
                               jnp.where(lane_c < n_l, pltpu.roll(low, 2 * per_kv, axis=1), 0.0)))
                pieces[h, pl.ds(pl.multiple_of(el * tok + off_of(el, side == 0), chunk), chunk)] = pc[:, None, :]

    for cpy in own_in:
        cpy.wait()
    keys_of(0)
    pl.semaphore_wait(barrier, cp - 1)
    for cpy in swaps:
        cpy.start()
    for row in loads:
        for _, rem in row:
            rem.start()
    acc[...] = jnp.zeros_like(acc)
    for i in PAIR:
        swaps[i].wait_recv()
    keys_of(1)

    def lives(reach, el, h, hop, owner):
        return 1 <= hop <= reach[(el * 2 + h) * nz + owner % nz]

    def sign(direction):
        return 1 - 2 * direction

    g_seq, r_seq = [split(c, 1, 1, 3, 1, 1) for c in GATHER_CODE], [split(c, 1, 1, 3, 1, 1) for c in REDUCE_CODE]
    g_wait, g_send, r_wait, r_send = (
        [select_const(z, w) for w in action_masks(nz, seq, active)] for seq, active in (
            (g_seq, lambda zz, dr, h, s, el, _: lives(GATHER_REACH[dr], el, h, s - 1, zz - sign(dr) * (s - 1))),
            (g_seq, lambda zz, dr, h, s, el, _: lives(GATHER_REACH[dr], el, h, s, zz - sign(dr) * (s - 1))),
            (r_seq, lambda zz, dr, h, d, el, on: on and lives(REDUCE_REACH[dr], el, h, d + 1, zz + sign(dr) * d)),
            (r_seq, lambda zz, dr, h, d, el, on: lives(REDUCE_REACH[dr], el, h, d, zz + sign(dr) * d)
             and on == lives(REDUCE_REACH[dr], el, h, d + 1, zz + sign(dr) * d))))

    def on(words, index):
        word = words[0]
        for i, w in enumerate(words[1:], 1):
            word = jnp.where(index >> 4 == i, w, word)
        return (word >> (index & 15)) & 1 == 1

    def neighbour(direction):
        return to(jnp.where(direction == 0, right, left))

    def gather_copy(direction, h, s, el):
        ref = kvall.at[wrap(z - sign(direction) * (s - 1)), h, el]
        return pltpu.make_async_remote_copy(ref, ref, ag_send.at[direction, h, s - 1, el], ag_recv.at[direction, h, s - 1, el],
                                            **neighbour(direction))

    def gather_arrival(direction, h, s, el):
        ref = kvall.at[wrap(z - sign(direction) * s), h, el]
        return pltpu.make_async_remote_copy(ref, ref, ag_send.at[direction, h, s - 1, el], ag_recv.at[direction, h, s - 1, el],
                                            **neighbour(direction))

    def gather_step(a):
        direction, h, s, el, _ = split(packed(a, GATHER_CODE, 7), 1, 1, 3, 1, 1)

        @pl.when(on(g_wait, a))
        def _():
            gather_arrival(direction, h, s - 1, el).wait_recv()

        @pl.when(on(g_send, a))
        def _():
            gather_copy(direction, h, s, el).start()

    def reduce_copy(direction, h, d, el):
        return pltpu.make_async_remote_copy(acc.at[wrap(z + sign(direction) * d), h, el], rsb.at[direction, d - 1, h, el],
                                            rs_send.at[direction, d - 1, h, el], rs_recv.at[direction, d - 1, h, el],
                                            **neighbour(direction))

    def reduce_arrival(direction, h, d, el):
        return pltpu.make_async_remote_copy(acc.at[wrap(z + sign(direction) * d), h, el], rsb.at[direction, d, h, el],
                                            rs_send.at[direction, d, h, el], rs_recv.at[direction, d, h, el],
                                            **neighbour(direction))

    def reduce_step(b):
        direction, h, d, el, _ = split(packed(b, REDUCE_CODE, 7), 1, 1, 3, 1, 1)

        @pl.when(on(r_wait, b))
        def _():
            reduce_arrival(direction, h, d, el).wait_recv()
            acc[wrap(z + sign(direction) * d), h, el] += rsb[direction, d, h, el]

        @pl.when(on(r_send, b))
        def _():
            reduce_copy(direction, h, d, el).start()

    def run_actions(step, first, count):
        def one(i, carry):
            step(i)
            return carry

        lax.fori_loop(first, first + count, one, 0)
        return first + count

    head_steps = 3 + 2 * (nz - 1)
    n_steps = 2 * head_steps
    n_pieces = 2 * tok // PREP_TOKENS
    first = n_pieces + 1
    n_ticks = n_steps + n_pieces
    gather_counts = count_at(GATHER_AT, first + n_ticks)
    prep_counts = gather_counts[:1] + [a + b for a, b in zip(gather_counts[1:first:2], gather_counts[2:first:2])]
    reduce_counts = count_at(REDUCE_AT, n_ticks)

    def ticks(g, done):
        ga = run_actions(gather_step, done[0], packed(first + g, gather_counts, 4))
        ra = run_actions(reduce_step, done[1], packed(g, reduce_counts, 4))
        return ga, ra

    gathered = run_actions(gather_step, 0, gather_counts[0])

    turn(cos_t, sin_t, lambda x: x[:, None, :])
    pieces_of(0)
    dq[...] = jnp.zeros_like(dq)
    dq_b[...] = jnp.zeros_like(dq_b)

    swaps[2].wait_recv()
    pieces_of(1)

    sub = PREP_TOKENS
    weight = qw_ref[...]
    ones = jnp.ones((2 * HEAD_DIM, HEAD_DIM), BF16)

    def masks(count):
        lane = lax.broadcasted_iota(jnp.int32, (count * per_kv, HEAD_DIM), 1)
        head = lax.broadcasted_iota(jnp.int32, (count * per_kv, HEAD_DIM), 0) & (per_kv - 1)
        return count, (lane == head) | (lane == head + per_kv) | (lane == head + 2 * per_kv), lane

    flat = lambda x: x.reshape(x.shape[0] * per_kv, HEAD_DIM)
    tall = lambda x: x.reshape(x.shape[0] // per_kv, per_kv, HEAD_DIM)

    def sums(prod, on_mxu):
        return row_sum(prod, ones) if on_mxu else lane_sum(prod)

    def prepare(h, el, t0, sub, lse_mask, lane):
        tabs = pl.ds(pl.multiple_of(el * tok + t0, sub), sub)
        r = x_rows(h, el, t0, sub)
        x = xq[r, :].astype(F32)
        ms = lane_mean(x * x)
        y = tall(x * lax.rsqrt(ms + NORM_EPS) * weight)
        hr = h_rows(el, t0, sub)
        qb[h][hr, :] = flat(y * cos_t[tabs] + roll_half(y) * sin_t[tabs]).astype(BF16)
        r0 = -lane_sum(xdo[r, :].astype(F32) * xout[r, :].astype(F32))
        r1 = r0 - r0.astype(BF16).astype(F32)
        r2 = r1 - r1.astype(BF16).astype(F32)
        dpart = jnp.where(lane == n_l, r0, jnp.where(lane == n_l + 1, r1, jnp.where(lane == n_l + 2, r2, 0.0)))
        consts = flat(jnp.broadcast_to(pieces[h, tabs], (sub, per_kv, HEAD_DIM)))
        aux[h][hr, :] = jnp.where(lse_mask, consts, dpart).astype(BF16)

    def finish(h, el, t0, on_mxu):
        tabs = pl.ds(pl.multiple_of(el * tok + t0, sub), sub)
        r = x_rows(h, el, t0, sub)
        x = xq[r, :].astype(F32)
        rstd = lax.rsqrt(sums(x * x, on_mxu) * (1.0 / HEAD_DIM) + NORM_EPS)
        xhat = x * rstd
        hr = h_rows(el, t0, sub)
        gq = tall(dqs[h][hr, :] * SM_SCALE)
        dy = flat(gq * cos_t[tabs] - roll_half(gq) * sin_t[tabs])
        dxh = dy * weight
        qb[h][hr, :] = (rstd * (dxh - xhat * lane_mean(dxh * xhat))).astype(BF16)
        return jnp.sum((dy * xhat).reshape(-1, 8, HEAD_DIM), axis=0)

    def piece_at(i):
        el = jnp.where(i >= n_pieces // 2, 1, 0)
        return el, (i - el * (n_pieces // 2)) * sub

    for part in PAIR:
        for el in PAIR:
            for loc, rem in loads[el]:
                if part == 0:
                    loc.wait()
                else:
                    rem.wait_recv()
        n = chunk // (2 * sub)

        def piece(i, gathered):
            el = jnp.where(i >= n, 1, 0)
            mine = core if part == 0 else other
            prepare(0, el, jnp.where(el == 0, mine, 1 - mine) * chunk + (i - el * n) * 2 * sub, *masks(2 * sub))
            return run_actions(gather_step, gathered, packed(1 + part * 2 * n + i, prep_counts, 4))

        gathered = lax.fori_loop(0, 2 * n, piece, gathered)
    for el in PAIR:
        for loc, rem in loads[2 + el]:
            loc.wait()
            rem.wait_recv()
    dwq[...] = jnp.zeros_like(dwq)

    keys = tok
    klane = lax.broadcasted_iota(jnp.int32, (keys, HEAD_DIM), 1)
    ones_k = jnp.where(klane < n_l, 1.0, 0.0).astype(BF16)
    ones_v = jnp.where((klane >= n_l) & (klane < n_l + 3), 1.0, 0.0).astype(BF16)
    klan = lax.broadcasted_iota(jnp.int32, (per_kv, keys), 1)

    def work(h, g, done):
        u = g - h * head_steps
        slot = packed(u, SLOTS[h], 6)
        delta, j = (slot >> 2) - 4, slot & 3
        own = delta == 0
        kz = wrap(z + delta)
        lower = kz < z
        q_late = jnp.where(own, jnp.where(j >= 1, 1, 0), jnp.where(lower, j, 1))
        k_late = jnp.where(own, jnp.where(j >= 2, 1, 0), jnp.where(lower, 0, j))
        q_blk = jnp.where(q_late == 1, 2 * nz - 1 - z, z)
        k_blk = jnp.where(k_late == 1, 2 * nz - 1 - kz, kz)
        off = (q_blk - k_blk) * tok
        r = pl.ds(pl.multiple_of((h * 2 + q_late) * rows, rows), rows)
        k, v = kvall[kz, h, k_late, 0], kvall[kz, h, k_late, 1]
        hr = pl.ds(pl.multiple_of(q_late * rows, rows), rows)
        qq, ax, dd = qb[h][hr, :], aux[h][hr, :], xdo[r, :]
        s = dot(jnp.concatenate([qq, ax], 1), jnp.concatenate([k, ones_k], 1), 1, 1)
        dp = dot(jnp.concatenate([dd, ax], 1), jnp.concatenate([v, ones_v], 1), 1, 1)
        p = jnp.exp2(s * EXP_SCALE)
        p = jnp.concatenate([jnp.where(klan <= off + t, p[per_kv * t:per_kv * (t + 1)], 0.0) for t in range(tok)], 0)
        ds = (p * dp).astype(BF16)
        pb = p.astype(BF16)
        dqs[h][hr, :] += dot(ds, k, 1, 0)
        acc[kz, h, k_late, 0] += dot(qq, ds, 0, 0)
        acc[kz, h, k_late, 1] += dot(dd, pb, 0, 0)
        el, t0 = piece_at(jnp.minimum(u, n_pieces - 1))
        if h == 0:
            prepare(1, el, t0, *masks(sub))
        else:
            dwq[...] += jnp.where(u < n_pieces, finish(0, el, t0, False), 0.0)
        return ticks(g, done)

    done = (gathered, jnp.int32(0))
    for h in PAIR:
        done = lax.fori_loop(h * head_steps, (h + 1) * head_steps, functools.partial(work, h), done)

    def last(i, done):
        el, t0 = piece_at(i)
        dwq[...] += finish(1, el, t0, True)
        return ticks(n_steps + i, done)

    done = lax.fori_loop(0, n_pieces, last, done)

    def back(x, ssum, g, cos, sin, w):
        rstd = lax.rsqrt(ssum * (1.0 / HEAD_DIM) + NORM_EPS)
        xhat = x * rstd
        dy = g * cos - roll_half(g) * sin
        dxh = dy * w
        dx = rstd * (dxh - xhat * lane_mean(dxh * xhat))
        return dx, jnp.sum((dy * xhat).reshape(-1, 8, HEAD_DIM), axis=0)

    outs = []
    for h in PAIR:
        for el in PAIR:
            heads = pl.ds(pl.multiple_of((2 * core + h) * per_kv, per_kv), per_kv)
            dst = dq_hbm.at[pl.ds(el * chunk, chunk), heads, :]
            part = lambda mine: qb[h].at[h_rows(el, off_of(el, mine), chunk)].reshape(chunk, per_kv, HEAD_DIM)
            outs.append((pltpu.make_async_copy(part(True), dst, dq_loc.at[h, el]),
                         pltpu.make_async_remote_copy(part(False), dst, dq_snd.at[h, el], dq_rcv.at[h, el], **to(sib))))
    for loc, rem in outs:
        loc.start()
        rem.start()
    for side in PAIR:
        unpack_keys(0, side)

    def drain_gather(a, carry):
        direction, h, s, el, _ = split(packed(a, GATHER_CODE, 7), 1, 1, 3, 1, 1)

        @pl.when(on(g_send, a))
        def _():
            gather_copy(direction, h, s, el).wait_send()

        return carry

    lax.fori_loop(0, len(G_SEQ), drain_gather, 0)
    for cpy in swaps:
        cpy.wait_send()
    for row in loads:
        for _, rem in row:
            rem.wait_send()

    hold = 4 * k_rows

    def key_gradients(h, dwk):
        for el in PAIR:
            kout[h, el, 1] = acc[z, h, el, 1].T.astype(BF16)
            dq[pl.ds(hold, tok), :] = acc[z, h, el, 0].T * SM_SCALE
            for s in PAIR:
                off = off_of(el, s == 0)
                x = raw(0, s, h, el)
                tabs = pl.ds(pl.multiple_of(el * tok + off, chunk), chunk)
                dx, dwp = back(x, lane_sum(x * x), dq[pl.ds(pl.multiple_of(hold + off, chunk), chunk), :], cos_d[tabs], sin_d[tabs], kw)
                kout[h, el, 0, pl.ds(off, chunk), :] = dx.astype(BF16)
                dwk = dwk + dwp
            dst = dkv_hbm.at[2 * core + h, el]
            both = (pltpu.make_async_copy(kout.at[h, el, :, pl.ds(off_of(el, True), chunk), :], dst, dk_loc.at[h, el]),
                    pltpu.make_async_remote_copy(kout.at[h, el, :, pl.ds(off_of(el, False), chunk), :], dst, dk_snd.at[h, el],
                                                 dk_rcv.at[h, el], **to(sib)))
            outs.append(both)
            for cpy in both:
                cpy.start()
        return dwk

    assert all(at < n_ticks for at, (_, h, d, _, _) in zip(REDUCE_AT, r_seq) if h == 0 and d == 0)
    dwk = key_gradients(0, jnp.zeros((8, HEAD_DIM), F32))
    run_actions(reduce_step, done[1], len(R_SEQ) - done[1])
    dwk = key_gradients(1, dwk)
    top = lax.broadcasted_iota(jnp.int32, (8, HEAD_DIM), 0)
    wmine[...] = jnp.where(top == 0, jnp.sum(dwq[...], axis=0, keepdims=True),
                           jnp.where(top == 1, jnp.sum(dwk, axis=0, keepdims=True), 0.0))

    def weight_copy(i):
        return pltpu.make_async_remote_copy(wmine, wslots.at[cp - i], w_snd.at[i], w_rcv.at[cp - i], **to(lax.rem(me + i, cp)))

    def weight_send(i, carry):
        weight_copy(i).start()
        return carry

    lax.fori_loop(1, cp, weight_send, 0)

    def drain_reduce(b, carry):
        direction, h, d, el, _ = split(packed(b, REDUCE_CODE, 7), 1, 1, 3, 1, 1)

        @pl.when(on(r_send, b))
        def _():
            reduce_copy(direction, h, d, el).wait_send()

        return carry

    lax.fori_loop(0, len(R_SEQ), drain_reduce, 0)

    def weight_wait(i, carry):
        pltpu.make_async_remote_copy(wmine, wslots.at[i], w_snd.at[i], w_rcv.at[i], **to(lax.rem(me + i, cp))).wait()
        return carry

    lax.fori_loop(1, cp, weight_wait, 0)
    wslots[0] = wmine[...]
    w_ref[...] = lax.fori_loop(0, cp, lambda i, total: total + wslots[lax.rem(i - me + cp, cp)], jnp.zeros((8, HEAD_DIM), F32))
    for loc, rem in outs:
        loc.wait()
        rem.wait()


def mega(nz, kv_heads, q_raw, d_out, out_fwd, lse, k_rows, v_rows, offc, offs, basec, bases, qw, kw):
    tok, heads, hd = q_raw.shape
    chunk, per_kv = tok // 2, heads // kv_heads
    any_spec = pl.BlockSpec(memory_space=pl.ANY)
    vmem = pl.BlockSpec(memory_space=pltpu.VMEM)
    dma, scr = pltpu.SemaphoreType.DMA, pltpu.VMEM
    n_rows = 2 * tok * per_kv
    hbm = lambda a: pltpu.with_memory_space_constraint(a, pltpu.HBM)
    args = [q_raw, d_out, out_fwd, lse, k_rows, v_rows, offc[:, None], offs[:, None], offc, offs]
    return pl.pallas_call(
        functools.partial(mega_kernel, nz, chunk, per_kv, kv_heads),
        in_specs=[any_spec] * len(args) + [vmem] * 4,
        out_specs=[any_spec, any_spec, vmem],
        out_shape=[jax.ShapeDtypeStruct(q_raw.shape, BF16), jax.ShapeDtypeStruct((kv_heads, 2, 2, chunk, hd), BF16),
                   jax.ShapeDtypeStruct((8, hd), F32)],
        scratch_shapes=[
            *[scr((2 * n_rows, hd), BF16)] * 3, *[scr((n_rows, hd), BF16)] * 4, *[scr((n_rows, hd), F32)] * 2,
            scr((nz, 2, 2, 2, tok, hd), BF16), scr((nz, 2, 2, 2, hd, tok), F32), scr((2, 4, 2, 2, 2, hd, tok), F32),
            scr((2, 2) + k_rows.shape, BF16), scr((2,) + lse.shape, F32), scr((2, 2 * tok, 1, hd), F32),
            *[scr((2 * tok, 1, hd), F32)] * 2, *[scr((2 * tok, hd), F32)] * 2,
            scr((2, 2, 2, tok, hd), BF16), *[scr((8, hd), F32)] * 2, scr((2 * nz, 8, hd), F32),
            *[dma((3,))] * 3, *[dma((2, 2, 3))] * 3, dma((4,)), *[dma((2, 2, 4, 2))] * 2, *[dma((2, 4, 2, 2))] * 2,
            *[dma((2, 2))] * 6, *[dma((2 * nz,))] * 2,
        ],
        name='attn_bwd',
        compiler_params=pltpu.CompilerParams(vmem_limit_bytes=67000000, collective_id=0, has_side_effects=True),
    )(*[hbm(a) for a in args], basec, bases, qw, kw)


def emit_kernel(n, dq_in, dkv_in, w_in, dq_out, dk_out, dv_out, wq_out, wk_out, buf, in_sem, out_sem):
    step = dq_in.shape[0] // n
    part = lambda ref, i: ref.at[pl.ds(i * step, step)]
    reads = [pltpu.make_async_copy(part(dq_in, i), part(buf, i), in_sem.at[i]) for i in range(n)]
    writes = [pltpu.make_async_copy(part(buf, i), part(dq_out, i), out_sem.at[i]) for i in range(n)]
    for cpy in reads:
        cpy.start()
    wq_out[...], wk_out[...] = w_in[0:1, :], w_in[1:2, :]
    kv_heads, halves, _, chunk, _ = dkv_in.shape
    for i in range(n):
        reads[i].wait()
        writes[i].start()
        if i < 2 * halves:
            ref, half, what = (dk_out, dv_out)[i & 1], i >> 1, i & 1
            x = dkv_in[:, half, what].astype(F32)
            ref[pl.ds(half * chunk, chunk)] = jnp.stack([x[h] for h in range(kv_heads)], axis=1).astype(BF16)
    for cpy in writes:
        cpy.wait()


def emit(dq, dkv, weights):
    tok, _, hd = dq.shape
    kv_heads = dkv.shape[0]
    n = 8
    any_spec, vmem = pl.BlockSpec(memory_space=pl.ANY), pl.BlockSpec(memory_space=pltpu.VMEM)
    return pl.pallas_call(
        functools.partial(emit_kernel, n),
        in_specs=[any_spec, vmem, vmem],
        out_specs=[any_spec] + [vmem] * 4,
        out_shape=[jax.ShapeDtypeStruct(dq.shape, BF16)] + [jax.ShapeDtypeStruct((tok, kv_heads, hd), BF16)] * 2
        + [jax.ShapeDtypeStruct((1, hd), F32)] * 2,
        scratch_shapes=[pltpu.VMEM(dq.shape, BF16), *[pltpu.SemaphoreType.DMA((n,))] * 2],
        name='emit',
    )(pltpu.with_memory_space_constraint(dq, pltpu.HBM), dkv, weights)


def solution(mesh):
    cp_size = mesh.shape['cp']
    nz = cp_size // 2

    def local_grads(q_raw, k_raw, v_proj, out_fwd, lse_fwd, d_out, q_norm, k_norm):
        tok, kv_heads = k_raw.shape[0], k_raw.shape[1]
        inv_freq = ROPE_THETA ** (-np.arange(0, HEAD_DIM, 2, dtype=np.float64) / HEAD_DIM)
        inv_freq = np.concatenate([inv_freq, inv_freq])
        sign = np.where(np.arange(HEAD_DIM) < HEAD_DIM // 2, -1.0, 1.0)
        off_ang = np.arange(tok)[:, None] * inv_freq
        base_ang = (np.arange(cp_size) * tok)[:, None] * inv_freq
        table = lambda x: jnp.asarray(x, F32)
        rows = lambda a: a.reshape(tok * kv_heads, HEAD_DIM)
        dq_raw, dkv, sums = mega(nz, kv_heads, q_raw, d_out, out_fwd, lse_fwd.T, rows(k_raw), rows(v_proj),
                                 table(np.cos(off_ang)), table(np.sin(off_ang) * sign),
                                 table(np.cos(base_ang))[:, None], table(np.sin(base_ang) * sign)[:, None],
                                 q_norm.reshape(1, HEAD_DIM), k_norm.reshape(1, HEAD_DIM))
        dq_raw, dk_raw, dv, wq, wk = emit(dq_raw, dkv, sums)
        return dq_raw, dk_raw, dv, wq.reshape(HEAD_DIM), wk.reshape(HEAD_DIM)

    row_spec = P(('dp', 'cp'))
    in_specs = (row_spec, row_spec, row_spec, row_spec, row_spec, row_spec, P(), P())
    out_specs = (row_spec, row_spec, row_spec, P('dp'), P('dp'))
    return jax.shard_map(local_grads, mesh=mesh, in_specs=in_specs, out_specs=out_specs, check_vma=False)
```

```python
import functools

import jax
import jax.numpy as jnp
import numpy as np
from jax import lax
from jax.experimental import pallas as pl
from jax.experimental.pallas import tpu as pltpu
from jax.sharding import PartitionSpec as P

HEAD_DIM = 128
ROPE_THETA = 1000000.0
NORM_EPS = 1e-6
SM_SCALE = HEAD_DIM ** -0.5
EXP_SCALE = SM_SCALE * 1.4426950408889634
F32, BF16 = jnp.float32, jnp.bfloat16
MESH = pl.DeviceIdType.MESH
PAIR = range(2)

ORDER = (56817234, 87162354)
GATHER = (452004200007000004, 1608009020084200776, 2252021500206002126, 2342023200238602186, 2532024460238402472,
    2730027940264602580, 2988029680290602920, 3376033080311803054, 4214040180395203698, 4730044080434004148, 4856)
REDUCE = (784006460072000658, 1228011670116600974, 1611014210142001357, 1929018650167501674, 2416023540218302119,
    2862026290260402546, 3183029910305302821, 3689034990337003369, 4197038770394703905, 5351051230426204135, 6305060830592305377,
    637106369)
GATHER_RIGHT = (54555555, 22554322, 22, 322)
GATHER_LEFT = (23222222, 55223455, 1234555, 1234455)
REDUCE_RIGHT = (33443444, 33333333, 1234444, 1234333)
REDUCE_LEFT = (44334333, 44444444, 333, 444)
PREP_TOKENS = 32


def digits(numbers):
    return [int(c) for n in numbers for c in str(n).zfill(8)]


GATHER_REACH = (digits(GATHER_RIGHT), digits(GATHER_LEFT))
REDUCE_REACH = (digits(REDUCE_RIGHT), digits(REDUCE_LEFT))


def unpacked(numbers):
    out = []
    for n in numbers:
        while n:
            out.append(n % 100000)
            n //= 100000
    return out


G_SEQ, R_SEQ = unpacked(GATHER), unpacked(REDUCE)
GATHER_AT, GATHER_CODE = [n >> 7 for n in G_SEQ], [n & 127 for n in G_SEQ]
REDUCE_AT, REDUCE_CODE = [n >> 7 for n in R_SEQ], [n & 127 for n in R_SEQ]
MAX_HOP = max(map(max, GATHER_REACH + REDUCE_REACH))
SLOTS = [[4 * int(d) + j for d in str(order) for j in range(3 if d == '4' else 2)] for order in ORDER]


def dot(a, b, ca, cb):
    return lax.dot_general(a, b, (((ca,), (cb,)), ((), ())), preferred_element_type=F32)


def lane_sum(x):
    return jnp.sum(x, axis=-1, keepdims=True)


def lane_mean(x):
    return lane_sum(x) * (1.0 / HEAD_DIM)


def roll_half(x):
    return pltpu.roll(x, HEAD_DIM // 2, axis=x.ndim - 1)


def row_sum(prod, ones):
    high = prod.astype(BF16)
    low = (prod - high.astype(F32)).astype(BF16)
    return dot(jnp.concatenate([high, low], 1), ones, 1, 0)


def select_const(index, values):
    if len(values) == 1:
        return jnp.int32(values[0])
    top = 1 << ((len(values) - 1).bit_length() - 1)
    low, high = select_const(index, values[:top]), select_const(index, values[top:])
    return jnp.where((index & top) != 0, high, low)


def packed(index, values, bits):
    per, shift = (4, 2) if bits > 3 else (8, 3)
    assert max(values) < 1 << bits
    words = []
    for i in range(0, len(values), per):
        words.append(sum(v << (bits * k) for k, v in enumerate(values[i:i + per])))
    return (select_const(index >> shift, words) >> ((index & (per - 1)) * bits)) & ((1 << bits) - 1)


def split(code, *bits):
    out = []
    for b in reversed(bits):
        out.append(code & ((1 << b) - 1))
        code = code >> b
    return out[::-1]


def action_masks(nz, sequence, active):
    chips = [[int(active(zz, *act)) for act in sequence] for zz in range(nz)]
    return [[sum(bit << k for k, bit in enumerate(c[i:i + 16])) for c in chips] for i in range(0, len(sequence), 16)]


def landing_slots(nz, sequence, reach):
    slots, users = {}, []
    for key in sorted({act[:4] for act in sequence if act[4]}):
        dr, h, d, el = key
        chips = {zz for zz in range(nz) if d + 1 <= reach[dr][(el * 2 + h) * nz + (zz + (1 - 2 * dr) * d) % nz]}
        n = next((i for i, u in enumerate(users) if not u & chips), len(users))
        users[n:n + 1] = [(users[n] if n < len(users) else set()) | chips]
        slots[key] = n
    return slots, len(users)


def count_at(table, last):
    return [sum(1 for at in table if at == g) for g in range(last)]


def mega_kernel(nz, chunk, per_kv, kv_heads,
                q_hbm, do_hbm, out_hbm, lse_hbm, k_hbm, v_hbm, offc3_hbm, offs3_hbm, offc_hbm, offs_hbm, basec_ref, bases_ref, qw_ref, kw_ref,
                dq_hbm, dkv_hbm, w_ref,
                xq, xdo, xout, qb_a, qb_b, aux_a, aux_b, dq, dq_b, kvall, acc, rsb, kland, lland, pieces, cos_t, sin_t, cos_d, sin_d, kout, dwq, wmine, wslots,
                in_sem, sw_snd, sw_rcv, ld_sem, xs_sem, xr_sem, tab_sem,
                ag_send, ag_recv, rs_send, rs_recv, dq_loc, dq_snd, dq_rcv, dk_loc, dk_snd, dk_rcv, w_snd, w_rcv):
    me = lax.axis_index('cp')
    cp = 2 * nz
    z, core = me >> 1, me & 1
    other = 1 - core
    sib = 2 * z + other
    right = 2 * ((z + 1) & (nz - 1)) + core
    left = 2 * ((z + nz - 1) & (nz - 1)) + core
    tok = 2 * chunk
    rows = tok * per_kv
    qb, aux, dqs = (qb_a, qb_b), (aux_a, aux_b), (dq, dq_b)
    k_rows = tok * kv_heads

    def wrap(i):
        return (i + 2 * nz) & (nz - 1)

    def to(device):
        return dict(device_id={'cp': device}, device_id_type=MESH)

    barrier = pltpu.get_barrier_semaphore()

    def say(i, carry):
        pl.semaphore_signal(barrier, inc=1, **to((me + i) & (cp - 1)))
        return carry

    lax.fori_loop(1, cp, say, 0)

    def off_of(el, mine):
        return pl.multiple_of((core if (el == 0) == mine else other) * chunk, chunk)

    def x_rows(h, el, token, count):
        return pl.ds(pl.multiple_of(((h * 2 + el) * tok + token) * per_kv, chunk), count * per_kv)

    def h_rows(el, token, count):
        return pl.ds(pl.multiple_of((el * tok + token) * per_kv, chunk), count * per_kv)

    lands = ((k_hbm, kland.at[0]), (v_hbm, kland.at[1]), (lse_hbm, lland))
    own_in = [pltpu.make_async_copy(hbm, buf.at[0], in_sem.at[i]) for i, (hbm, buf) in enumerate(lands)]
    swaps = [pltpu.make_async_remote_copy(hbm, buf.at[1], sw_snd.at[i], sw_rcv.at[i], **to(sib)) for i, (hbm, buf) in enumerate(lands)]
    tables = [pltpu.make_async_copy(src, dst, tab_sem.at[i]) for i, (src, dst) in enumerate((
        (offc_hbm, cos_d.at[pl.ds(0, tok)]), (offs_hbm, sin_d.at[pl.ds(0, tok)]),
        (offc3_hbm, cos_t.at[pl.ds(0, tok)]), (offs3_hbm, sin_t.at[pl.ds(0, tok)])))]
    loads = []
    for h in PAIR:
        for el in PAIR:
            heads = lambda c: pl.ds(pl.multiple_of((2 * c + h) * per_kv, per_kv), per_kv)
            src = pl.ds(el * chunk, chunk)
            dst = x_rows(h, el, off_of(el, True), chunk)
            row = []
            for i, (hbm, buf) in enumerate(((q_hbm, xq), (do_hbm, xdo), (out_hbm, xout))):
                there = buf.at[dst].reshape(chunk, per_kv, HEAD_DIM)
                row.append((pltpu.make_async_copy(hbm.at[src, heads(core), :], there, ld_sem.at[h, el, i]),
                            pltpu.make_async_remote_copy(hbm.at[src, heads(other), :], there, xs_sem.at[h, el, i], xr_sem.at[h, el, i],
                                                         **to(sib))))
            loads.append(row)
    for cpy in own_in + tables:
        cpy.start()
    for row in loads:
        for loc, _ in row:
            loc.start()
    def base(el):
        blk = z if el == 0 else 2 * nz - 1 - z
        return basec_ref[blk], bases_ref[blk]

    def turn(cos_ref, sin_ref, lift):
        for el in (1, 0):
            bc, bs = base(el)
            bc, bs = lift(bc), lift(bs)
            step = 32

            def part(i, carry):
                src = pl.ds(pl.multiple_of(i * step, step), step)
                dst = pl.ds(pl.multiple_of(el * tok + i * step, step), step)
                oc, os = cos_ref[src], sin_ref[src]
                cos_ref[dst] = bc * oc - bs * os
                sin_ref[dst] = bs * oc + bc * os
                return carry

            lax.fori_loop(0, tok // step, part, 0)

    for t in tables:
        t.wait()
    turn(cos_d, sin_d, lambda x: x)

    def raw_rows(what, side):
        return pl.ds((what * 2 + side) * k_rows, k_rows)

    def raw(what, side, h, el):
        return dq[pl.ds((what * 2 + side) * k_rows + el * chunk * kv_heads + 2 * core + h, chunk, stride=kv_heads), :]

    def unpack_keys(what, side):
        dq[raw_rows(what, side), :] = kland[what, side].astype(F32)

    kw = kw_ref[...]

    def keys_of(side):
        for i in PAIR:
            unpack_keys(i, side)
        for h in PAIR:
            for el in PAIR:
                off = off_of(el, side == 0)
                x = raw(0, side, h, el)
                y = x * lax.rsqrt(lane_mean(x * x) + NORM_EPS) * kw
                tabs = pl.ds(pl.multiple_of(el * tok + off, chunk), chunk)
                kvall[z, h, el, 0, :, pl.ds(off, chunk)] = (y * cos_d[tabs] + roll_half(y) * sin_d[tabs]).T.astype(BF16)
                kvall[z, h, el, 1, :, pl.ds(off, chunk)] = raw(1, side, h, el).T.astype(BF16)

    n_l = 3 * per_kv
    lane_c = lax.broadcasted_iota(jnp.int32, (chunk, HEAD_DIM), 1)

    def pieces_of(side):
        for h in PAIR:
            for el in PAIR:
                val = (lland[side, :, pl.ds(el * chunk, chunk)] * (-1.0 / SM_SCALE)).T
                val = jnp.concatenate([val, jnp.zeros((chunk, HEAD_DIM - val.shape[1]), F32)], axis=1)
                val = pltpu.roll(val, (HEAD_DIM - (2 * core + h) * per_kv) & (HEAD_DIM - 1), axis=1)
                hi = val.astype(BF16).astype(F32)
                mid = (val - hi).astype(BF16).astype(F32)
                low = val - hi - mid
                pc = jnp.where(lane_c < per_kv, hi, jnp.where(lane_c < 2 * per_kv, pltpu.roll(mid, per_kv, axis=1),
                               jnp.where(lane_c < n_l, pltpu.roll(low, 2 * per_kv, axis=1), 0.0)))
                pieces[h, pl.ds(pl.multiple_of(el * tok + off_of(el, side == 0), chunk), chunk)] = pc[:, None, :]

    for cpy in own_in:
        cpy.wait()
    keys_of(0)
    pl.semaphore_wait(barrier, cp - 1)
    for cpy in swaps:
        cpy.start()
    for row in loads:
        for _, rem in row:
            rem.start()
    acc[...] = jnp.zeros_like(acc)
    for i in PAIR:
        swaps[i].wait_recv()
    keys_of(1)

    def lives(reach, el, h, hop, owner):
        return 1 <= hop <= reach[(el * 2 + h) * nz + owner % nz]

    def sign(direction):
        return 1 - 2 * direction

    g_seq, r_seq = [[tuple(split(c, 1, 1, 3, 1, 1)) for c in codes] for codes in (GATHER_CODE, REDUCE_CODE)]
    slots, _ = landing_slots(nz, r_seq, REDUCE_REACH)
    slot_in = [slots.get(act[:4], 0) for act in r_seq]
    slot_out = [slots.get((dr, h, d - 1, el), 0) for dr, h, d, el, _ in r_seq]
    g_wait, g_send, r_wait, r_send = (
        [select_const(z, w) for w in action_masks(nz, seq, active)] for seq, active in (
            (g_seq, lambda zz, dr, h, s, el, _: lives(GATHER_REACH[dr], el, h, s - 1, zz - sign(dr) * (s - 1))),
            (g_seq, lambda zz, dr, h, s, el, _: lives(GATHER_REACH[dr], el, h, s, zz - sign(dr) * (s - 1))),
            (r_seq, lambda zz, dr, h, d, el, on: on and lives(REDUCE_REACH[dr], el, h, d + 1, zz + sign(dr) * d)),
            (r_seq, lambda zz, dr, h, d, el, on: lives(REDUCE_REACH[dr], el, h, d, zz + sign(dr) * d)
             and on == lives(REDUCE_REACH[dr], el, h, d + 1, zz + sign(dr) * d))))

    def on(words, index):
        word = words[0]
        for i, w in enumerate(words[1:], 1):
            word = jnp.where(index >> 4 == i, w, word)
        return (word >> (index & 15)) & 1 == 1

    def neighbour(direction):
        return to(jnp.where(direction == 0, right, left))

    def gather_copy(direction, h, s, el):
        ref = kvall.at[wrap(z - sign(direction) * (s - 1)), h, el]
        return pltpu.make_async_remote_copy(ref, ref, ag_send.at[direction, h, s - 1, el], ag_recv.at[direction, h, s - 1, el],
                                            **neighbour(direction))

    def gather_arrival(direction, h, s, el):
        ref = kvall.at[wrap(z - sign(direction) * s), h, el]
        return pltpu.make_async_remote_copy(ref, ref, ag_send.at[direction, h, s - 1, el], ag_recv.at[direction, h, s - 1, el],
                                            **neighbour(direction))

    def gather_step(a):
        direction, h, s, el, _ = split(packed(a, GATHER_CODE, 7), 1, 1, 3, 1, 1)

        @pl.when(on(g_wait, a))
        def _():
            gather_arrival(direction, h, s - 1, el).wait_recv()

        @pl.when(on(g_send, a))
        def _():
            gather_copy(direction, h, s, el).start()

    def reduce_copy(direction, h, d, el, slot):
        return pltpu.make_async_remote_copy(acc.at[wrap(z + sign(direction) * d), h, el], rsb.at[slot],
                                            rs_send.at[direction, d - 1, h, el], rs_recv.at[direction, d - 1, h, el],
                                            **neighbour(direction))

    def reduce_arrival(direction, h, d, el, slot):
        return pltpu.make_async_remote_copy(acc.at[wrap(z + sign(direction) * d), h, el], rsb.at[slot],
                                            rs_send.at[direction, d, h, el], rs_recv.at[direction, d, h, el],
                                            **neighbour(direction))

    def reduce_step(b):
        direction, h, d, el, _ = split(packed(b, REDUCE_CODE, 7), 1, 1, 3, 1, 1)

        @pl.when(on(r_wait, b))
        def _():
            slot = packed(b, slot_in, 7)
            reduce_arrival(direction, h, d, el, slot).wait_recv()
            acc[wrap(z + sign(direction) * d), h, el] += rsb[slot]

        @pl.when(on(r_send, b))
        def _():
            reduce_copy(direction, h, d, el, packed(b, slot_out, 7)).start()

    def run_actions(step, first, count):
        def one(i, carry):
            step(i)
            return carry

        lax.fori_loop(first, first + count, one, 0)
        return first + count

    head_steps = 3 + 2 * (nz - 1)
    n_steps = 2 * head_steps
    n_pieces = 2 * tok // PREP_TOKENS
    first = n_pieces + 1
    n_ticks = n_steps + n_pieces
    gather_counts = count_at(GATHER_AT, first + n_ticks)
    prep_counts = gather_counts[:1] + [a + b for a, b in zip(gather_counts[1:first:2], gather_counts[2:first:2])]
    reduce_counts = count_at(REDUCE_AT, n_ticks)

    def ticks(g, done):
        ga = run_actions(gather_step, done[0], packed(first + g, gather_counts, 4))
        ra = run_actions(reduce_step, done[1], packed(g, reduce_counts, 4))
        return ga, ra

    gathered = run_actions(gather_step, 0, gather_counts[0])

    turn(cos_t, sin_t, lambda x: x[:, None, :])
    pieces_of(0)

    swaps[2].wait_recv()
    pieces_of(1)

    sub = PREP_TOKENS
    weight = qw_ref[...]
    ones = jnp.ones((2 * HEAD_DIM, HEAD_DIM), BF16)

    def masks(count):
        lane = lax.broadcasted_iota(jnp.int32, (count * per_kv, HEAD_DIM), 1)
        head = lax.broadcasted_iota(jnp.int32, (count * per_kv, HEAD_DIM), 0) & (per_kv - 1)
        return count, (lane == head) | (lane == head + per_kv) | (lane == head + 2 * per_kv), lane

    flat = lambda x: x.reshape(x.shape[0] * per_kv, HEAD_DIM)
    tall = lambda x: x.reshape(x.shape[0] // per_kv, per_kv, HEAD_DIM)

    def sums(prod, on_mxu):
        return row_sum(prod, ones) if on_mxu else lane_sum(prod)

    def prepare(h, el, t0, sub, lse_mask, lane):
        tabs = pl.ds(pl.multiple_of(el * tok + t0, sub), sub)
        r = x_rows(h, el, t0, sub)
        x = xq[r, :].astype(F32)
        ms = lane_mean(x * x)
        y = tall(x * lax.rsqrt(ms + NORM_EPS) * weight)
        hr = h_rows(el, t0, sub)
        qb[h][hr, :] = flat(y * cos_t[tabs] + roll_half(y) * sin_t[tabs]).astype(BF16)
        r0 = -lane_sum(xdo[r, :].astype(F32) * xout[r, :].astype(F32))
        r1 = r0 - r0.astype(BF16).astype(F32)
        r2 = r1 - r1.astype(BF16).astype(F32)
        dpart = jnp.where(lane == n_l, r0, jnp.where(lane == n_l + 1, r1, jnp.where(lane == n_l + 2, r2, 0.0)))
        consts = flat(jnp.broadcast_to(pieces[h, tabs], (sub, per_kv, HEAD_DIM)))
        aux[h][hr, :] = jnp.where(lse_mask, consts, dpart).astype(BF16)
        dqs[h][hr, :] = jnp.zeros((sub * per_kv, HEAD_DIM), F32)

    def finish(h, el, t0, on_mxu):
        tabs = pl.ds(pl.multiple_of(el * tok + t0, sub), sub)
        r = x_rows(h, el, t0, sub)
        x = xq[r, :].astype(F32)
        rstd = lax.rsqrt(sums(x * x, on_mxu) * (1.0 / HEAD_DIM) + NORM_EPS)
        xhat = x * rstd
        hr = h_rows(el, t0, sub)
        gq = tall(dqs[h][hr, :] * SM_SCALE)
        dy = flat(gq * cos_t[tabs] - roll_half(gq) * sin_t[tabs])
        dxh = dy * weight
        qb[h][hr, :] = (rstd * (dxh - xhat * lane_mean(dxh * xhat))).astype(BF16)
        return jnp.sum((dy * xhat).reshape(-1, 8, HEAD_DIM), axis=0)

    def piece_at(i):
        el = jnp.where(i >= n_pieces // 2, 1, 0)
        return el, (i - el * (n_pieces // 2)) * sub

    for el in PAIR:
        for loc, _ in loads[el]:
            loc.wait()
    quarter = chunk // (2 * sub)
    wide = masks(2 * sub)

    def piece(i, gathered):
        @pl.when(i == 2 * quarter)
        def _():
            for el in PAIR:
                for _, rem in loads[el]:
                    rem.wait_recv()

        part, k = jnp.where(i >= 2 * quarter, 1, 0), i & (2 * quarter - 1)
        el = jnp.where(k >= quarter, 1, 0)
        prepare(0, el, (core ^ part ^ el) * chunk + (k - el * quarter) * 2 * sub, *wide)
        return run_actions(gather_step, gathered, packed(1 + i, prep_counts, 4))

    gathered = lax.fori_loop(0, 4 * quarter, piece, gathered)
    for el in PAIR:
        for loc, rem in loads[2 + el]:
            loc.wait()
            rem.wait_recv()
    dwq[...] = jnp.zeros_like(dwq)

    keys = tok
    krow = lax.broadcasted_iota(jnp.int32, (HEAD_DIM, keys), 0)
    ones_k = jnp.where(krow < n_l, 1.0, 0.0).astype(BF16)
    ones_v = jnp.where((krow >= n_l) & (krow < n_l + 3), 1.0, 0.0).astype(BF16)
    klan = lax.broadcasted_iota(jnp.int32, (per_kv, keys), 1)

    def work(h, g, done):
        u = g - h * head_steps
        slot = packed(u, SLOTS[h], 6)
        delta, j = (slot >> 2) - 4, slot & 3
        own = delta == 0
        kz = wrap(z + delta)
        lower = kz < z
        q_late = jnp.where(own, jnp.where(j >= 1, 1, 0), jnp.where(lower, j, 1))
        k_late = jnp.where(own, jnp.where(j >= 2, 1, 0), jnp.where(lower, 0, j))
        q_blk = jnp.where(q_late == 1, 2 * nz - 1 - z, z)
        k_blk = jnp.where(k_late == 1, 2 * nz - 1 - kz, kz)
        off = (q_blk - k_blk) * tok
        r = pl.ds(pl.multiple_of((h * 2 + q_late) * rows, rows), rows)
        k, v = kvall[kz, h, k_late, 0], kvall[kz, h, k_late, 1]
        hr = pl.ds(pl.multiple_of(q_late * rows, rows), rows)
        qq, ax, dd = qb[h][hr, :], aux[h][hr, :], xdo[r, :]
        s = dot(jnp.concatenate([qq, ax], 1), jnp.concatenate([k, ones_k], 0), 1, 0)
        dp = dot(jnp.concatenate([dd, ax], 1), jnp.concatenate([v, ones_v], 0), 1, 0)
        p = jnp.exp2(s * EXP_SCALE)
        p = jnp.concatenate([jnp.where(klan <= off + t, p[per_kv * t:per_kv * (t + 1)], 0.0) for t in range(tok)], 0)
        ds = (p * dp).astype(BF16)
        pb = p.astype(BF16)
        dqs[h][hr, :] += dot(ds, k, 1, 1)
        acc[kz, h, k_late, 0] += dot(qq, ds, 0, 0)
        acc[kz, h, k_late, 1] += dot(dd, pb, 0, 0)
        el, t0 = piece_at(jnp.minimum(u, n_pieces - 1))
        if h == 0:
            prepare(1, el, t0, *masks(sub))
        else:
            dwq[...] += jnp.where(u < n_pieces, finish(0, el, t0, False), 0.0)
        return ticks(g, done)

    done = (gathered, jnp.int32(0))
    for h in PAIR:
        done = lax.fori_loop(h * head_steps, (h + 1) * head_steps, functools.partial(work, h), done)

    def last(i, done):
        el, t0 = piece_at(i)
        dwq[...] += finish(1, el, t0, True)
        return ticks(n_steps + i, done)

    done = lax.fori_loop(0, n_pieces, last, done)

    def back(x, ssum, g, cos, sin, w):
        rstd = lax.rsqrt(ssum * (1.0 / HEAD_DIM) + NORM_EPS)
        xhat = x * rstd
        dy = g * cos - roll_half(g) * sin
        dxh = dy * w
        dx = rstd * (dxh - xhat * lane_mean(dxh * xhat))
        return dx, jnp.sum((dy * xhat).reshape(-1, 8, HEAD_DIM), axis=0)

    outs = []
    for h in PAIR:
        for el in PAIR:
            heads = pl.ds(pl.multiple_of((2 * core + h) * per_kv, per_kv), per_kv)
            dst = dq_hbm.at[pl.ds(el * chunk, chunk), heads, :]
            part = lambda mine: qb[h].at[h_rows(el, off_of(el, mine), chunk)].reshape(chunk, per_kv, HEAD_DIM)
            outs.append((pltpu.make_async_copy(part(True), dst, dq_loc.at[h, el]),
                         pltpu.make_async_remote_copy(part(False), dst, dq_snd.at[h, el], dq_rcv.at[h, el], **to(sib))))
    for loc, rem in outs:
        loc.start()
        rem.start()
    for side in PAIR:
        unpack_keys(0, side)

    def drain_gather(a, carry):
        direction, h, s, el, _ = split(packed(a, GATHER_CODE, 7), 1, 1, 3, 1, 1)

        @pl.when(on(g_send, a))
        def _():
            gather_copy(direction, h, s, el).wait_send()

        return carry

    lax.fori_loop(0, len(G_SEQ), drain_gather, 0)
    for cpy in swaps:
        cpy.wait_send()
    for row in loads:
        for _, rem in row:
            rem.wait_send()

    hold = 4 * k_rows

    def key_gradients(h, dwk):
        for el in PAIR:
            kout[h, el, 1] = acc[z, h, el, 1].T.astype(BF16)
            dq[pl.ds(hold, tok), :] = acc[z, h, el, 0].T * SM_SCALE
            for s in PAIR:
                off = off_of(el, s == 0)
                x = raw(0, s, h, el)
                tabs = pl.ds(pl.multiple_of(el * tok + off, chunk), chunk)
                dx, dwp = back(x, lane_sum(x * x), dq[pl.ds(pl.multiple_of(hold + off, chunk), chunk), :], cos_d[tabs], sin_d[tabs], kw)
                kout[h, el, 0, pl.ds(off, chunk), :] = dx.astype(BF16)
                dwk = dwk + dwp
            dst = dkv_hbm.at[2 * core + h, el]
            both = (pltpu.make_async_copy(kout.at[h, el, :, pl.ds(off_of(el, True), chunk), :], dst, dk_loc.at[h, el]),
                    pltpu.make_async_remote_copy(kout.at[h, el, :, pl.ds(off_of(el, False), chunk), :], dst, dk_snd.at[h, el],
                                                 dk_rcv.at[h, el], **to(sib)))
            outs.append(both)
            for cpy in both:
                cpy.start()
        return dwk

    assert all(at < n_ticks for at, (_, h, d, _, _) in zip(REDUCE_AT, r_seq) if h == 0 and d == 0)
    dwk = key_gradients(0, jnp.zeros((8, HEAD_DIM), F32))
    run_actions(reduce_step, done[1], len(R_SEQ) - done[1])
    dwk = key_gradients(1, dwk)
    top = lax.broadcasted_iota(jnp.int32, (8, HEAD_DIM), 0)
    wmine[...] = jnp.where(top == 0, jnp.sum(dwq[...], axis=0, keepdims=True),
                           jnp.where(top == 1, jnp.sum(dwk, axis=0, keepdims=True), 0.0))

    def weight_copy(i):
        return pltpu.make_async_remote_copy(wmine, wslots.at[cp - i], w_snd.at[i], w_rcv.at[cp - i], **to((me + i) & (cp - 1)))

    def weight_send(i, carry):
        weight_copy(i).start()
        return carry

    lax.fori_loop(1, cp, weight_send, 0)

    def drain_reduce(b, carry):
        direction, h, d, el, _ = split(packed(b, REDUCE_CODE, 7), 1, 1, 3, 1, 1)

        @pl.when(on(r_send, b))
        def _():
            reduce_copy(direction, h, d, el, 0).wait_send()

        return carry

    lax.fori_loop(0, len(R_SEQ), drain_reduce, 0)

    def weight_wait(i, carry):
        pltpu.make_async_remote_copy(wmine, wslots.at[i], w_snd.at[i], w_rcv.at[i], **to((me + i) & (cp - 1))).wait()
        return carry

    lax.fori_loop(1, cp, weight_wait, 0)
    wslots[0] = wmine[...]
    w_ref[...] = lax.fori_loop(0, cp, lambda i, total: total + wslots[(i - me + cp) & (cp - 1)], jnp.zeros((8, HEAD_DIM), F32))
    for loc, rem in outs:
        loc.wait()
        rem.wait()


def mega(nz, kv_heads, q_raw, d_out, out_fwd, lse, k_rows, v_rows, offc, offs, basec, bases, qw, kw):
    tok, heads, hd = q_raw.shape
    chunk, per_kv = tok // 2, heads // kv_heads
    any_spec = pl.BlockSpec(memory_space=pl.ANY)
    vmem = pl.BlockSpec(memory_space=pltpu.VMEM)
    dma, scr = pltpu.SemaphoreType.DMA, pltpu.VMEM
    n_rows = 2 * tok * per_kv
    _, n_slots = landing_slots(nz, [tuple(split(c, 1, 1, 3, 1, 1)) for c in REDUCE_CODE], REDUCE_REACH)
    hbm = lambda a: pltpu.with_memory_space_constraint(a, pltpu.HBM)
    args = [q_raw, d_out, out_fwd, lse, k_rows, v_rows, offc[:, None], offs[:, None], offc, offs]
    return pl.pallas_call(
        functools.partial(mega_kernel, nz, chunk, per_kv, kv_heads),
        in_specs=[any_spec] * len(args) + [vmem] * 4,
        out_specs=[any_spec, any_spec, vmem],
        out_shape=[jax.ShapeDtypeStruct(q_raw.shape, BF16), jax.ShapeDtypeStruct((kv_heads, 2, 2, chunk, hd), BF16),
                   jax.ShapeDtypeStruct((8, hd), F32)],
        scratch_shapes=[
            *[scr((2 * n_rows, hd), BF16)] * 3, *[scr((n_rows, hd), BF16)] * 4, *[scr((n_rows, hd), F32)] * 2,
            scr((nz, 2, 2, 2, hd, tok), BF16), scr((nz, 2, 2, 2, hd, tok), F32), scr((n_slots, 2, hd, tok), F32),
            scr((2, 2) + k_rows.shape, BF16), scr((2,) + lse.shape, F32), scr((2, 2 * tok, 1, hd), F32),
            *[scr((2 * tok, 1, hd), F32)] * 2, *[scr((2 * tok, hd), F32)] * 2,
            scr((2, 2, 2, tok, hd), BF16), *[scr((8, hd), F32)] * 2, scr((2 * nz, 8, hd), F32),
            *[dma((3,))] * 3, *[dma((2, 2, 3))] * 3, dma((4,)), *[dma((2, 2, MAX_HOP, 2))] * 2, *[dma((2, MAX_HOP, 2, 2))] * 2,
            *[dma((2, 2))] * 6, *[dma((2 * nz,))] * 2,
        ],
        name='attn_bwd',
        compiler_params=pltpu.CompilerParams(vmem_limit_bytes=67000000, collective_id=0, has_side_effects=True),
    )(*[hbm(a) for a in args], basec, bases, qw, kw)


def emit_kernel(n, dq_in, dkv_in, w_in, dq_out, dk_out, dv_out, wq_out, wk_out, buf, kv_buf, k_buf, v_buf, kv_sem, in_sem, out_sem):
    step = dq_in.shape[0] // n
    part = lambda ref, i: ref.at[pl.ds(i * step, step)]
    reads = [pltpu.make_async_copy(part(dq_in, i), part(buf, i), in_sem.at[i]) for i in range(n)]
    writes = [pltpu.make_async_copy(part(buf, i), part(dq_out, i), out_sem.at[i]) for i in range(n)]
    kv_heads, halves, _, chunk, _ = dkv_in.shape
    rows = lambda ref, half: ref.at[pl.ds(half * chunk, chunk)]
    kv_reads = [pltpu.make_async_copy(dkv_in.at[:, half], kv_buf.at[:, half], kv_sem.at[half]) for half in range(halves)]
    for cpy in kv_reads + reads:
        cpy.start()
    wq_out[...], wk_out[...] = w_in[0:1, :], w_in[1:2, :]
    for half in range(halves):
        kv_reads[half].wait()
        for what, (ref, out) in enumerate(((k_buf, dk_out), (v_buf, dv_out))):
            x = kv_buf[:, half, what].astype(F32)
            ref[pl.ds(half * chunk, chunk)] = jnp.stack([x[h] for h in range(kv_heads)], axis=1).astype(BF16)
            writes.append(pltpu.make_async_copy(rows(ref, half), rows(out, half), kv_sem.at[halves + 2 * half + what]))
    for i in range(n):
        reads[i].wait()
        writes[i].start()
    for cpy in writes[n:]:
        cpy.start()
    for cpy in writes:
        cpy.wait()


def emit(dq, dkv, weights):
    tok, _, hd = dq.shape
    kv_heads = dkv.shape[0]
    n = 8
    any_spec, vmem = pl.BlockSpec(memory_space=pl.ANY), pl.BlockSpec(memory_space=pltpu.VMEM)
    kv_shape = (tok, kv_heads, hd)
    hbm = lambda a: pltpu.with_memory_space_constraint(a, pltpu.HBM)
    dma = pltpu.SemaphoreType.DMA
    return pl.pallas_call(
        functools.partial(emit_kernel, n),
        in_specs=[any_spec, any_spec, vmem],
        out_specs=[any_spec] * 3 + [vmem] * 2,
        out_shape=[jax.ShapeDtypeStruct(dq.shape, BF16)] + [jax.ShapeDtypeStruct(kv_shape, BF16)] * 2
        + [jax.ShapeDtypeStruct((1, hd), F32)] * 2,
        scratch_shapes=[*[pltpu.VMEM(shape, BF16) for shape in (dq.shape, dkv.shape, kv_shape, kv_shape)], dma((n,)), *[dma((n,))] * 2],
        name='emit',
    )(hbm(dq), hbm(dkv), weights)


def solution(mesh):
    cp_size = mesh.shape['cp']
    nz = cp_size // 2

    def local_grads(q_raw, k_raw, v_proj, out_fwd, lse_fwd, d_out, q_norm, k_norm):
        tok, kv_heads = k_raw.shape[0], k_raw.shape[1]
        inv_freq = ROPE_THETA ** (-np.arange(0, HEAD_DIM, 2, dtype=np.float64) / HEAD_DIM)
        inv_freq = np.concatenate([inv_freq, inv_freq])
        sign = np.where(np.arange(HEAD_DIM) < HEAD_DIM // 2, -1.0, 1.0)
        off_ang = np.arange(tok)[:, None] * inv_freq
        base_ang = (np.arange(cp_size) * tok)[:, None] * inv_freq
        table = lambda x: jnp.asarray(x, F32)
        rows = lambda a: a.reshape(tok * kv_heads, HEAD_DIM)
        dq_raw, dkv, sums = mega(nz, kv_heads, q_raw, d_out, out_fwd, lse_fwd.T, rows(k_raw), rows(v_proj),
                                 table(np.cos(off_ang)), table(np.sin(off_ang) * sign),
                                 table(np.cos(base_ang))[:, None], table(np.sin(base_ang) * sign)[:, None],
                                 q_norm.reshape(1, HEAD_DIM), k_norm.reshape(1, HEAD_DIM))
        dq_raw, dk_raw, dv, wq, wk = emit(dq_raw, dkv, sums)
        return dq_raw, dk_raw, dv, wq.reshape(HEAD_DIM), wk.reshape(HEAD_DIM)

    row_spec = P(('dp', 'cp'))
    in_specs = (row_spec, row_spec, row_spec, row_spec, row_spec, row_spec, P(), P())
    out_specs = (row_spec, row_spec, row_spec, P('dp'), P('dp'))
    return jax.shard_map(local_grads, mesh=mesh, in_specs=in_specs, out_specs=out_specs, check_vma=False)
```

```python
import functools

import jax
import jax.numpy as jnp
import numpy as np
from jax import lax
from jax.experimental import pallas as pl
from jax.experimental.pallas import tpu as pltpu
from jax.sharding import PartitionSpec as P

HEAD_DIM = 128
ROPE_THETA = 1000000.0
NORM_EPS = 1e-6
SM_SCALE = HEAD_DIM ** -0.5
EXP_SCALE = SM_SCALE * 1.4426950408889634
F32, BF16 = jnp.float32, jnp.bfloat16
MESH = pl.DeviceIdType.MESH
PAIR = range(2)

ORDER = (43215687, 78135264)
GATHER = (260003560000600070, 1994019300138201092, 2376023180228002184, 2706027940257202468, 3020030520296002894,
    3348032380318203112, 3736038240362603478, 4268039200392203954, 4858045260446804470, 485604784)
REDUCE = (1354013000104600968, 1991019390180901861, 2422023180218902066, 2826026970244702420, 3393031850308302931,
    3591035900343903333, 4010038800394703693, 4227042910422504201, 5093047110464604389, 6369061150604905287, 6435)
GATHER_RIGHT = (55554445, 22333322, 4444, 22)
GATHER_LEFT = (22223332, 55444455, 1233333, 1234555)
REDUCE_RIGHT = (55555555, 22222222, 1234555, 1222222)
REDUCE_LEFT = (22222222, 55555555, 22, 55555)
PREP_TOKENS = 32


def digits(numbers):
    return [int(c) for n in numbers for c in str(n).zfill(8)]


GATHER_REACH = (digits(GATHER_RIGHT), digits(GATHER_LEFT))
REDUCE_REACH = (digits(REDUCE_RIGHT), digits(REDUCE_LEFT))


def unpacked(numbers):
    out = []
    for n in numbers:
        while n:
            out.append(n % 100000)
            n //= 100000
    return out


G_SEQ, R_SEQ = unpacked(GATHER), unpacked(REDUCE)
GATHER_AT, GATHER_CODE = [n >> 7 for n in G_SEQ], [n & 127 for n in G_SEQ]
REDUCE_AT, REDUCE_CODE = [n >> 7 for n in R_SEQ], [n & 127 for n in R_SEQ]
MAX_HOP = max(map(max, GATHER_REACH + REDUCE_REACH))
SLOTS = [[4 * int(d) + j for d in str(order) for j in range(3 if d == '4' else 2)] for order in ORDER]


def dot(a, b, ca, cb):
    return lax.dot_general(a, b, (((ca,), (cb,)), ((), ())), preferred_element_type=F32)


def lane_sum(x):
    return jnp.sum(x, axis=-1, keepdims=True)


def lane_mean(x):
    return lane_sum(x) * (1.0 / HEAD_DIM)


def roll_half(x):
    return pltpu.roll(x, HEAD_DIM // 2, axis=x.ndim - 1)


def row_sum(prod, ones):
    high = prod.astype(BF16)
    low = (prod - high.astype(F32)).astype(BF16)
    return dot(jnp.concatenate([high, low], 1), ones, 1, 0)


def select_const(index, values):
    if len(values) == 1:
        return jnp.int32(values[0])
    top = 1 << ((len(values) - 1).bit_length() - 1)
    low, high = select_const(index, values[:top]), select_const(index, values[top:])
    return jnp.where((index & top) != 0, high, low)


def packed(index, values, bits):
    per, shift = (4, 2) if bits > 3 else (8, 3)
    assert max(values) < 1 << bits
    words = []
    for i in range(0, len(values), per):
        words.append(sum(v << (bits * k) for k, v in enumerate(values[i:i + per])))
    return (select_const(index >> shift, words) >> ((index & (per - 1)) * bits)) & ((1 << bits) - 1)


def split(code, *bits):
    out = []
    for b in reversed(bits):
        out.append(code & ((1 << b) - 1))
        code = code >> b
    return out[::-1]


def action_masks(nz, sequence, active):
    chips = [[int(active(zz, *act)) for act in sequence] for zz in range(nz)]
    return [[sum(bit << k for k, bit in enumerate(c[i:i + 16])) for c in chips] for i in range(0, len(sequence), 16)]


def landing_slots(nz, sequence, reach):
    slots, users = {}, []
    for key in sorted({act[:4] for act in sequence if act[4]}):
        dr, h, d, el = key
        chips = {zz for zz in range(nz) if d + 1 <= reach[dr][(el * 2 + h) * nz + (zz + (1 - 2 * dr) * d) % nz]}
        n = next((i for i, u in enumerate(users) if not u & chips), len(users))
        users[n:n + 1] = [(users[n] if n < len(users) else set()) | chips]
        slots[key] = n
    return slots, len(users)


def count_at(table, last):
    return [sum(1 for at in table if at == g) for g in range(last)]


def mega_kernel(nz, chunk, per_kv, kv_heads,
                q_hbm, do_hbm, out_hbm, lse_hbm, k_hbm, v_hbm, offc3_hbm, offs3_hbm, offc_hbm, offs_hbm, basec_ref, bases_ref, qw_ref, kw_ref,
                dq_hbm, dkv_hbm, w_ref,
                xq, xdo, xout, qb_a, qb_b, aux_a, aux_b, dq, dq_b, kvall, acc, rsb, kland, lland, pieces, cos_t, sin_t, cos_d, sin_d, kout, dwq, wmine, wslots,
                in_sem, sw_snd, sw_rcv, ld_sem, xs_sem, xr_sem, tab_sem,
                ag_send, ag_recv, rs_send, rs_recv, dq_loc, dq_snd, dq_rcv, dk_loc, dk_snd, dk_rcv, w_snd, w_rcv):
    me = lax.axis_index('cp')
    cp = 2 * nz
    z, core = me >> 1, me & 1
    other = 1 - core
    sib = 2 * z + other
    right = 2 * ((z + 1) & (nz - 1)) + core
    left = 2 * ((z + nz - 1) & (nz - 1)) + core
    tok = 2 * chunk
    rows = tok * per_kv
    qb, aux, dqs = (qb_a, qb_b), (aux_a, aux_b), (dq, dq_b)
    k_rows = tok * kv_heads

    def wrap(i):
        return (i + 2 * nz) & (nz - 1)

    def to(device):
        return dict(device_id={'cp': device}, device_id_type=MESH)

    barrier = pltpu.get_barrier_semaphore()

    def say(i, carry):
        pl.semaphore_signal(barrier, inc=1, **to((me + i) & (cp - 1)))
        return carry

    lax.fori_loop(1, cp, say, 0)

    def off_of(el, mine):
        return pl.multiple_of((core if (el == 0) == mine else other) * chunk, chunk)

    def x_rows(h, el, token, count):
        return pl.ds(pl.multiple_of(((h * 2 + el) * tok + token) * per_kv, chunk), count * per_kv)

    def h_rows(el, token, count):
        return pl.ds(pl.multiple_of((el * tok + token) * per_kv, chunk), count * per_kv)

    lands = ((k_hbm, kland.at[0]), (v_hbm, kland.at[1]), (lse_hbm, lland))
    own_in = [pltpu.make_async_copy(hbm, buf.at[0], in_sem.at[i]) for i, (hbm, buf) in enumerate(lands)]
    swaps = [pltpu.make_async_remote_copy(hbm, buf.at[1], sw_snd.at[i], sw_rcv.at[i], **to(sib)) for i, (hbm, buf) in enumerate(lands)]
    tables = [pltpu.make_async_copy(src, dst, tab_sem.at[i]) for i, (src, dst) in enumerate((
        (offc_hbm, cos_d.at[pl.ds(0, tok)]), (offs_hbm, sin_d.at[pl.ds(0, tok)]),
        (offc3_hbm, cos_t.at[pl.ds(0, tok)]), (offs3_hbm, sin_t.at[pl.ds(0, tok)])))]
    loads = []
    for h in PAIR:
        for el in PAIR:
            heads = lambda c: pl.ds(pl.multiple_of((2 * c + h) * per_kv, per_kv), per_kv)
            src = pl.ds(el * chunk, chunk)
            dst = x_rows(h, el, off_of(el, True), chunk)
            row = []
            for i, (hbm, buf) in enumerate(((q_hbm, xq), (do_hbm, xdo), (out_hbm, xout))):
                there = buf.at[dst].reshape(chunk, per_kv, HEAD_DIM)
                row.append((pltpu.make_async_copy(hbm.at[src, heads(core), :], there, ld_sem.at[h, el, i]),
                            pltpu.make_async_remote_copy(hbm.at[src, heads(other), :], there, xs_sem.at[h, el, i], xr_sem.at[h, el, i],
                                                         **to(sib))))
            loads.append(row)
    for cpy in own_in + tables:
        cpy.start()
    for row in loads:
        for loc, _ in row:
            loc.start()
    def base(el):
        blk = z if el == 0 else 2 * nz - 1 - z
        return basec_ref[blk], bases_ref[blk]

    def turn(cos_ref, sin_ref, lift):
        for el in (1, 0):
            bc, bs = base(el)
            bc, bs = lift(bc), lift(bs)
            step = 32

            def part(i, carry):
                src = pl.ds(pl.multiple_of(i * step, step), step)
                dst = pl.ds(pl.multiple_of(el * tok + i * step, step), step)
                oc, os = cos_ref[src], sin_ref[src]
                cos_ref[dst] = bc * oc - bs * os
                sin_ref[dst] = bs * oc + bc * os
                return carry

            lax.fori_loop(0, tok // step, part, 0)


    def raw_rows(what, side):
        return pl.ds((what * 2 + side) * k_rows, k_rows)

    def raw(what, side, h, el):
        return dq[pl.ds((what * 2 + side) * k_rows + el * chunk * kv_heads + 2 * core + h, chunk, stride=kv_heads), :]

    def unpack_keys(what, side):
        dq[raw_rows(what, side), :] = kland[what, side].astype(F32)

    kw = kw_ref[...]

    def keys_of(side):
        for i in PAIR:
            unpack_keys(i, side)
        for h in PAIR:
            for el in PAIR:
                off = off_of(el, side == 0)
                x = raw(0, side, h, el)
                y = x * lax.rsqrt(lane_mean(x * x) + NORM_EPS) * kw
                tabs = pl.ds(pl.multiple_of(el * tok + off, chunk), chunk)
                kvall[z, h, el, 0, :, pl.ds(off, chunk)] = (y * cos_d[tabs] + roll_half(y) * sin_d[tabs]).T.astype(BF16)
                kvall[z, h, el, 1, :, pl.ds(off, chunk)] = raw(1, side, h, el).T.astype(BF16)

    n_l = 3 * per_kv
    lane_c = lax.broadcasted_iota(jnp.int32, (chunk, HEAD_DIM), 1)

    def pieces_of(side):
        for h in PAIR:
            for el in PAIR:
                val = (lland[side, :, pl.ds(el * chunk, chunk)] * (-1.0 / SM_SCALE)).T
                val = jnp.concatenate([val, jnp.zeros((chunk, HEAD_DIM - val.shape[1]), F32)], axis=1)
                val = pltpu.roll(val, (HEAD_DIM - (2 * core + h) * per_kv) & (HEAD_DIM - 1), axis=1)
                hi = val.astype(BF16).astype(F32)
                mid = (val - hi).astype(BF16).astype(F32)
                low = val - hi - mid
                pc = jnp.where(lane_c < per_kv, hi, jnp.where(lane_c < 2 * per_kv, pltpu.roll(mid, per_kv, axis=1),
                               jnp.where(lane_c < n_l, pltpu.roll(low, 2 * per_kv, axis=1), 0.0)))
                pieces[h, pl.ds(pl.multiple_of(el * tok + off_of(el, side == 0), chunk), chunk)] = pc[:, None, :]

    pl.semaphore_wait(barrier, cp - 1)
    for cpy in swaps:
        cpy.start()
    for row in loads:
        for _, rem in row:
            rem.start()
    for t in tables:
        t.wait()
    turn(cos_d, sin_d, lambda x: x)
    for cpy in own_in:
        cpy.wait()
    keys_of(0)
    turn(cos_t, sin_t, lambda x: x[:, None, :])
    pieces_of(0)
    acc[...] = jnp.zeros_like(acc)
    for i in PAIR:
        swaps[i].wait_recv()
    keys_of(1)

    def lives(reach, el, h, hop, owner):
        return 1 <= hop <= reach[(el * 2 + h) * nz + owner % nz]

    def sign(direction):
        return 1 - 2 * direction

    g_seq, r_seq = [[tuple(split(c, 1, 1, 3, 1, 1)) for c in codes] for codes in (GATHER_CODE, REDUCE_CODE)]
    slots, _ = landing_slots(nz, r_seq, REDUCE_REACH)
    slot_in = [slots.get(act[:4], 0) for act in r_seq]
    slot_out = [slots.get((dr, h, d - 1, el), 0) for dr, h, d, el, _ in r_seq]
    g_wait, g_send, r_wait, r_send = (
        [select_const(z, w) for w in action_masks(nz, seq, active)] for seq, active in (
            (g_seq, lambda zz, dr, h, s, el, _: lives(GATHER_REACH[dr], el, h, s - 1, zz - sign(dr) * (s - 1))),
            (g_seq, lambda zz, dr, h, s, el, _: lives(GATHER_REACH[dr], el, h, s, zz - sign(dr) * (s - 1))),
            (r_seq, lambda zz, dr, h, d, el, on: on and lives(REDUCE_REACH[dr], el, h, d + 1, zz + sign(dr) * d)),
            (r_seq, lambda zz, dr, h, d, el, on: lives(REDUCE_REACH[dr], el, h, d, zz + sign(dr) * d)
             and on == lives(REDUCE_REACH[dr], el, h, d + 1, zz + sign(dr) * d))))

    def on(words, index):
        word = words[0]
        for i, w in enumerate(words[1:], 1):
            word = jnp.where(index >> 4 == i, w, word)
        return (word >> (index & 15)) & 1 == 1

    def neighbour(direction):
        return to(jnp.where(direction == 0, right, left))

    def gather_copy(direction, h, s, el):
        ref = kvall.at[wrap(z - sign(direction) * (s - 1)), h, el]
        return pltpu.make_async_remote_copy(ref, ref, ag_send.at[direction, h, s - 1, el], ag_recv.at[direction, h, s - 1, el],
                                            **neighbour(direction))

    def gather_arrival(direction, h, s, el):
        ref = kvall.at[wrap(z - sign(direction) * s), h, el]
        return pltpu.make_async_remote_copy(ref, ref, ag_send.at[direction, h, s - 1, el], ag_recv.at[direction, h, s - 1, el],
                                            **neighbour(direction))

    def gather_step(a):
        direction, h, s, el, _ = split(packed(a, GATHER_CODE, 7), 1, 1, 3, 1, 1)

        @pl.when(on(g_wait, a))
        def _():
            gather_arrival(direction, h, s - 1, el).wait_recv()

        @pl.when(on(g_send, a))
        def _():
            gather_copy(direction, h, s, el).start()

    def reduce_copy(direction, h, d, el, slot):
        return pltpu.make_async_remote_copy(acc.at[wrap(z + sign(direction) * d), h, el], rsb.at[slot],
                                            rs_send.at[direction, d - 1, h, el], rs_recv.at[direction, d - 1, h, el],
                                            **neighbour(direction))

    def reduce_arrival(direction, h, d, el, slot):
        return pltpu.make_async_remote_copy(acc.at[wrap(z + sign(direction) * d), h, el], rsb.at[slot],
                                            rs_send.at[direction, d, h, el], rs_recv.at[direction, d, h, el],
                                            **neighbour(direction))

    def reduce_step(b):
        direction, h, d, el, _ = split(packed(b, REDUCE_CODE, 7), 1, 1, 3, 1, 1)

        @pl.when(on(r_wait, b))
        def _():
            slot = packed(b, slot_in, 7)
            reduce_arrival(direction, h, d, el, slot).wait_recv()
            acc[wrap(z + sign(direction) * d), h, el] += rsb[slot]

        @pl.when(on(r_send, b))
        def _():
            reduce_copy(direction, h, d, el, packed(b, slot_out, 7)).start()

    def run_actions(step, first, count):
        def one(i, carry):
            step(i)
            return carry

        lax.fori_loop(first, first + count, one, 0)
        return first + count

    head_steps = 3 + 2 * (nz - 1)
    n_steps = 2 * head_steps
    n_pieces = 2 * tok // PREP_TOKENS
    first = n_pieces + 1
    n_ticks = n_steps + n_pieces
    gather_counts = count_at(GATHER_AT, first + n_ticks)
    prep_counts = gather_counts[:1] + [a + b for a, b in zip(gather_counts[1:first:2], gather_counts[2:first:2])]
    reduce_counts = count_at(REDUCE_AT, n_ticks)

    def ticks(g, done):
        ga = run_actions(gather_step, done[0], packed(first + g, gather_counts, 4))
        ra = run_actions(reduce_step, done[1], packed(g, reduce_counts, 4))
        return ga, ra

    gathered = run_actions(gather_step, 0, gather_counts[0])


    swaps[2].wait_recv()
    pieces_of(1)

    sub = PREP_TOKENS
    weight = qw_ref[...]
    ones = jnp.ones((2 * HEAD_DIM, HEAD_DIM), BF16)

    def masks(count):
        lane = lax.broadcasted_iota(jnp.int32, (count * per_kv, HEAD_DIM), 1)
        head = lax.broadcasted_iota(jnp.int32, (count * per_kv, HEAD_DIM), 0) & (per_kv - 1)
        return count, (lane == head) | (lane == head + per_kv) | (lane == head + 2 * per_kv), lane

    flat = lambda x: x.reshape(x.shape[0] * per_kv, HEAD_DIM)
    tall = lambda x: x.reshape(x.shape[0] // per_kv, per_kv, HEAD_DIM)

    def sums(prod, on_mxu):
        return row_sum(prod, ones) if on_mxu else lane_sum(prod)

    def prepare(h, el, t0, sub, lse_mask, lane):
        tabs = pl.ds(pl.multiple_of(el * tok + t0, sub), sub)
        r = x_rows(h, el, t0, sub)
        x = xq[r, :].astype(F32)
        ms = lane_mean(x * x)
        y = tall(x * lax.rsqrt(ms + NORM_EPS) * weight)
        hr = h_rows(el, t0, sub)
        qb[h][hr, :] = flat(y * cos_t[tabs] + roll_half(y) * sin_t[tabs]).astype(BF16)
        r0 = -lane_sum(xdo[r, :].astype(F32) * xout[r, :].astype(F32))
        r1 = r0 - r0.astype(BF16).astype(F32)
        r2 = r1 - r1.astype(BF16).astype(F32)
        dpart = jnp.where(lane == n_l, r0, jnp.where(lane == n_l + 1, r1, jnp.where(lane == n_l + 2, r2, 0.0)))
        consts = flat(jnp.broadcast_to(pieces[h, tabs], (sub, per_kv, HEAD_DIM)))
        aux[h][hr, :] = jnp.where(lse_mask, consts, dpart).astype(BF16)
        dqs[h][hr, :] = jnp.zeros((sub * per_kv, HEAD_DIM), F32)

    def finish(h, el, t0, on_mxu):
        tabs = pl.ds(pl.multiple_of(el * tok + t0, sub), sub)
        r = x_rows(h, el, t0, sub)
        x = xq[r, :].astype(F32)
        rstd = lax.rsqrt(sums(x * x, on_mxu) * (1.0 / HEAD_DIM) + NORM_EPS)
        xhat = x * rstd
        hr = h_rows(el, t0, sub)
        gq = tall(dqs[h][hr, :] * SM_SCALE)
        dy = flat(gq * cos_t[tabs] - roll_half(gq) * sin_t[tabs])
        dxh = dy * weight
        qb[h][hr, :] = (rstd * (dxh - xhat * lane_mean(dxh * xhat))).astype(BF16)
        return jnp.sum((dy * xhat).reshape(-1, 8, HEAD_DIM), axis=0)

    def piece_at(i):
        el = jnp.where(i >= n_pieces // 2, 1, 0)
        return el, (i - el * (n_pieces // 2)) * sub

    for el in PAIR:
        for loc, _ in loads[el]:
            loc.wait()
    quarter = chunk // (2 * sub)
    wide = masks(2 * sub)

    def piece(i, gathered):
        @pl.when(i == 2 * quarter)
        def _():
            for el in PAIR:
                for _, rem in loads[el]:
                    rem.wait_recv()

        part, k = jnp.where(i >= 2 * quarter, 1, 0), i & (2 * quarter - 1)
        el = jnp.where(k >= quarter, 1, 0)
        prepare(0, el, (core ^ part ^ el) * chunk + (k - el * quarter) * 2 * sub, *wide)
        return run_actions(gather_step, gathered, packed(1 + i, prep_counts, 4))

    gathered = lax.fori_loop(0, 4 * quarter, piece, gathered)
    for el in PAIR:
        for loc, rem in loads[2 + el]:
            loc.wait()
            rem.wait_recv()
    dwq[...] = jnp.zeros_like(dwq)

    keys = tok
    krow = lax.broadcasted_iota(jnp.int32, (HEAD_DIM, keys), 0)
    ones_k = jnp.where(krow < n_l, 1.0, 0.0).astype(BF16)
    ones_v = jnp.where((krow >= n_l) & (krow < n_l + 3), 1.0, 0.0).astype(BF16)
    klan = lax.broadcasted_iota(jnp.int32, (per_kv, keys), 1)

    def work(h, g, done):
        u = g - h * head_steps
        slot = packed(u, SLOTS[h], 6)
        delta, j = (slot >> 2) - 4, slot & 3
        own = delta == 0
        kz = wrap(z + delta)
        lower = kz < z
        q_late = jnp.where(own, jnp.where(j >= 1, 1, 0), jnp.where(lower, j, 1))
        k_late = jnp.where(own, jnp.where(j >= 2, 1, 0), jnp.where(lower, 0, j))
        q_blk = jnp.where(q_late == 1, 2 * nz - 1 - z, z)
        k_blk = jnp.where(k_late == 1, 2 * nz - 1 - kz, kz)
        off = (q_blk - k_blk) * tok
        r = pl.ds(pl.multiple_of((h * 2 + q_late) * rows, rows), rows)
        k, v = kvall[kz, h, k_late, 0], kvall[kz, h, k_late, 1]
        hr = pl.ds(pl.multiple_of(q_late * rows, rows), rows)
        qq, ax, dd = qb[h][hr, :], aux[h][hr, :], xdo[r, :]
        s = dot(jnp.concatenate([qq, ax], 1), jnp.concatenate([k, ones_k], 0), 1, 0)
        dp = dot(jnp.concatenate([dd, ax], 1), jnp.concatenate([v, ones_v], 0), 1, 0)
        p = jnp.exp2(s * EXP_SCALE)
        p = jnp.concatenate([jnp.where(klan <= off + t, p[per_kv * t:per_kv * (t + 1)], 0.0) for t in range(tok)], 0)
        ds = (p * dp).astype(BF16)
        pb = p.astype(BF16)
        dqs[h][hr, :] += dot(ds, k, 1, 1)
        acc[kz, h, k_late, 0] += dot(qq, ds, 0, 0)
        acc[kz, h, k_late, 1] += dot(dd, pb, 0, 0)
        el, t0 = piece_at(jnp.minimum(u, n_pieces - 1))
        if h == 0:
            prepare(1, el, t0, *masks(sub))
        else:
            dwq[...] += jnp.where(u < n_pieces, finish(0, el, t0, False), 0.0)
        return ticks(g, done)

    done = (gathered, jnp.int32(0))
    for h in PAIR:
        done = lax.fori_loop(h * head_steps, (h + 1) * head_steps, functools.partial(work, h), done)

    def last(i, done):
        el, t0 = piece_at(i)
        dwq[...] += finish(1, el, t0, True)
        return ticks(n_steps + i, done)

    def back(x, ssum, g, cos, sin, w):
        rstd = lax.rsqrt(ssum * (1.0 / HEAD_DIM) + NORM_EPS)
        xhat = x * rstd
        dy = g * cos - roll_half(g) * sin
        dxh = dy * w
        dx = rstd * (dxh - xhat * lane_mean(dxh * xhat))
        return dx, jnp.sum((dy * xhat).reshape(-1, 8, HEAD_DIM), axis=0)

    outs = []

    def send_queries(h, el):
        heads = pl.ds(pl.multiple_of((2 * core + h) * per_kv, per_kv), per_kv)
        dst = dq_hbm.at[pl.ds(el * chunk, chunk), heads, :]
        part = lambda mine: qb[h].at[h_rows(el, off_of(el, mine), chunk)].reshape(chunk, per_kv, HEAD_DIM)
        both = (pltpu.make_async_remote_copy(part(False), dst, dq_snd.at[h, el], dq_rcv.at[h, el], **to(sib)),
                pltpu.make_async_copy(part(True), dst, dq_loc.at[h, el]))
        outs.append(both)
        for cpy in both:
            cpy.start()

    hold = 4 * k_rows

    def key_gradients(h, dwk):
        for el in PAIR:
            kout[h, el, 1] = acc[z, h, el, 1].T.astype(BF16)
            dq[pl.ds(hold, tok), :] = acc[z, h, el, 0].T * SM_SCALE
            for s in PAIR:
                off = off_of(el, s == 0)
                x = raw(0, s, h, el)
                tabs = pl.ds(pl.multiple_of(el * tok + off, chunk), chunk)
                dx, dwp = back(x, lane_sum(x * x), dq[pl.ds(pl.multiple_of(hold + off, chunk), chunk), :], cos_d[tabs], sin_d[tabs], kw)
                kout[h, el, 0, pl.ds(off, chunk), :] = dx.astype(BF16)
                dwk = dwk + dwp
            dst = dkv_hbm.at[2 * core + h, el]
            both = (pltpu.make_async_copy(kout.at[h, el, :, pl.ds(off_of(el, True), chunk), :], dst, dk_loc.at[h, el]),
                    pltpu.make_async_remote_copy(kout.at[h, el, :, pl.ds(off_of(el, False), chunk), :], dst, dk_snd.at[h, el],
                                                 dk_rcv.at[h, el], **to(sib)))
            outs.append(both)
            for cpy in both:
                cpy.start()
        return dwk

    assert all(at < n_steps for at, (_, h, d, _, _) in zip(REDUCE_AT, r_seq) if h == 0 and d == 0)
    for el in PAIR:
        send_queries(0, el)
    for side in PAIR:
        unpack_keys(0, side)
    dwk = key_gradients(0, jnp.zeros((8, HEAD_DIM), F32))

    def drain_gather(a, carry):
        direction, h, s, el, _ = split(packed(a, GATHER_CODE, 7), 1, 1, 3, 1, 1)

        @pl.when(on(g_send, a))
        def _():
            gather_copy(direction, h, s, el).wait_send()

        return carry

    lax.fori_loop(0, len(G_SEQ), drain_gather, 0)
    for cpy in swaps:
        cpy.wait_send()
    for row in loads:
        for _, rem in row:
            rem.wait_send()

    for el in PAIR:
        done = lax.fori_loop(el * n_pieces // 2, (el + 1) * n_pieces // 2, last, done)
        send_queries(1, el)
    run_actions(reduce_step, done[1], len(R_SEQ) - done[1])
    dwk = key_gradients(1, dwk)
    top = lax.broadcasted_iota(jnp.int32, (8, HEAD_DIM), 0)
    wmine[...] = jnp.where(top == 0, jnp.sum(dwq[...], axis=0, keepdims=True),
                           jnp.where(top == 1, jnp.sum(dwk, axis=0, keepdims=True), 0.0))

    def weight_copy(i):
        return pltpu.make_async_remote_copy(wmine, wslots.at[cp - i], w_snd.at[i], w_rcv.at[cp - i], **to((me + i) & (cp - 1)))

    def weight_send(i, carry):
        weight_copy(i).start()
        return carry

    lax.fori_loop(1, cp, weight_send, 0)

    def drain_reduce(b, carry):
        direction, h, d, el, _ = split(packed(b, REDUCE_CODE, 7), 1, 1, 3, 1, 1)

        @pl.when(on(r_send, b))
        def _():
            reduce_copy(direction, h, d, el, 0).wait_send()

        return carry

    lax.fori_loop(0, len(R_SEQ), drain_reduce, 0)

    def weight_wait(i, carry):
        pltpu.make_async_remote_copy(wmine, wslots.at[i], w_snd.at[i], w_rcv.at[i], **to((me + i) & (cp - 1))).wait()
        return carry

    lax.fori_loop(1, cp, weight_wait, 0)
    wslots[0] = wmine[...]
    w_ref[...] = lax.fori_loop(0, cp, lambda i, total: total + wslots[(i - me + cp) & (cp - 1)], jnp.zeros((8, HEAD_DIM), F32))
    for loc, rem in outs:
        loc.wait()
        rem.wait()


def mega(nz, kv_heads, q_raw, d_out, out_fwd, lse, k_rows, v_rows, offc, offs, basec, bases, qw, kw):
    tok, heads, hd = q_raw.shape
    chunk, per_kv = tok // 2, heads // kv_heads
    any_spec = pl.BlockSpec(memory_space=pl.ANY)
    vmem = pl.BlockSpec(memory_space=pltpu.VMEM)
    dma, scr = pltpu.SemaphoreType.DMA, pltpu.VMEM
    n_rows = 2 * tok * per_kv
    _, n_slots = landing_slots(nz, [tuple(split(c, 1, 1, 3, 1, 1)) for c in REDUCE_CODE], REDUCE_REACH)
    hbm = lambda a: pltpu.with_memory_space_constraint(a, pltpu.HBM)
    args = [q_raw, d_out, out_fwd, lse, k_rows, v_rows, offc[:, None], offs[:, None], offc, offs]
    return pl.pallas_call(
        functools.partial(mega_kernel, nz, chunk, per_kv, kv_heads),
        in_specs=[any_spec] * len(args) + [vmem] * 4,
        out_specs=[any_spec, any_spec, vmem],
        out_shape=[jax.ShapeDtypeStruct(q_raw.shape, BF16), jax.ShapeDtypeStruct((kv_heads, 2, 2, chunk, hd), BF16),
                   jax.ShapeDtypeStruct((8, hd), F32)],
        scratch_shapes=[
            *[scr((2 * n_rows, hd), BF16)] * 3, *[scr((n_rows, hd), BF16)] * 4, *[scr((n_rows, hd), F32)] * 2,
            scr((nz, 2, 2, 2, hd, tok), BF16), scr((nz, 2, 2, 2, hd, tok), F32), scr((n_slots, 2, hd, tok), F32),
            scr((2, 2) + k_rows.shape, BF16), scr((2,) + lse.shape, F32), scr((2, 2 * tok, 1, hd), F32),
            *[scr((2 * tok, 1, hd), F32)] * 2, *[scr((2 * tok, hd), F32)] * 2,
            scr((2, 2, 2, tok, hd), BF16), *[scr((8, hd), F32)] * 2, scr((2 * nz, 8, hd), F32),
            *[dma((3,))] * 3, *[dma((2, 2, 3))] * 3, dma((4,)), *[dma((2, 2, MAX_HOP, 2))] * 2, *[dma((2, MAX_HOP, 2, 2))] * 2,
            *[dma((2, 2))] * 6, *[dma((2 * nz,))] * 2,
        ],
        name='attn_bwd',
        compiler_params=pltpu.CompilerParams(vmem_limit_bytes=67000000, collective_id=0, has_side_effects=True),
    )(*[hbm(a) for a in args], basec, bases, qw, kw)


def emit_kernel(n, dq_in, dkv_in, w_in, dq_out, dk_out, dv_out, wq_out, wk_out, buf, in_sem, out_sem):
    step = dq_in.shape[0] // n
    part = lambda ref, i: ref.at[pl.ds(i * step, step)]
    reads = [pltpu.make_async_copy(part(dq_in, i), part(buf, i), in_sem.at[i]) for i in range(n)]
    writes = [pltpu.make_async_copy(part(buf, i), part(dq_out, i), out_sem.at[i]) for i in range(n)]
    for cpy in reads:
        cpy.start()
    wq_out[...], wk_out[...] = w_in[0:1, :], w_in[1:2, :]
    kv_heads, halves, _, chunk, _ = dkv_in.shape
    for i in range(n):
        reads[i].wait()
        writes[i].start()
        if i < 2 * halves:
            ref, half, what = (dk_out, dv_out)[i & 1], i >> 1, i & 1
            x = dkv_in[:, half, what].astype(F32)
            ref[pl.ds(half * chunk, chunk)] = jnp.stack([x[h] for h in range(kv_heads)], axis=1).astype(BF16)
    for cpy in writes:
        cpy.wait()


def emit(dq, dkv, weights):
    tok, _, hd = dq.shape
    kv_heads = dkv.shape[0]
    n = 8
    any_spec, vmem = pl.BlockSpec(memory_space=pl.ANY), pl.BlockSpec(memory_space=pltpu.VMEM)
    return pl.pallas_call(
        functools.partial(emit_kernel, n),
        in_specs=[any_spec, vmem, vmem],
        out_specs=[any_spec] + [vmem] * 4,
        out_shape=[jax.ShapeDtypeStruct(dq.shape, BF16)] + [jax.ShapeDtypeStruct((tok, kv_heads, hd), BF16)] * 2
        + [jax.ShapeDtypeStruct((1, hd), F32)] * 2,
        scratch_shapes=[pltpu.VMEM(dq.shape, BF16), *[pltpu.SemaphoreType.DMA((n,))] * 2],
        name='emit',
    )(pltpu.with_memory_space_constraint(dq, pltpu.HBM), dkv, weights)


def solution(mesh):
    cp_size = mesh.shape['cp']
    nz = cp_size // 2

    def local_grads(q_raw, k_raw, v_proj, out_fwd, lse_fwd, d_out, q_norm, k_norm):
        tok, kv_heads = k_raw.shape[0], k_raw.shape[1]
        inv_freq = ROPE_THETA ** (-np.arange(0, HEAD_DIM, 2, dtype=np.float64) / HEAD_DIM)
        inv_freq = np.concatenate([inv_freq, inv_freq])
        sign = np.where(np.arange(HEAD_DIM) < HEAD_DIM // 2, -1.0, 1.0)
        off_ang = np.arange(tok)[:, None] * inv_freq
        base_ang = (np.arange(cp_size) * tok)[:, None] * inv_freq
        table = lambda x: jnp.asarray(x, F32)
        rows = lambda a: a.reshape(tok * kv_heads, HEAD_DIM)
        dq_raw, dkv, sums = mega(nz, kv_heads, q_raw, d_out, out_fwd, lse_fwd.T, rows(k_raw), rows(v_proj),
                                 table(np.cos(off_ang)), table(np.sin(off_ang) * sign),
                                 table(np.cos(base_ang))[:, None], table(np.sin(base_ang) * sign)[:, None],
                                 q_norm.reshape(1, HEAD_DIM), k_norm.reshape(1, HEAD_DIM))
        dq_raw, dk_raw, dv, wq, wk = emit(dq_raw, dkv, sums)
        return dq_raw, dk_raw, dv, wq.reshape(HEAD_DIM), wk.reshape(HEAD_DIM)

    row_spec = P(('dp', 'cp'))
    in_specs = (row_spec, row_spec, row_spec, row_spec, row_spec, row_spec, P(), P())
    out_specs = (row_spec, row_spec, row_spec, P('dp'), P('dp'))
    return jax.shard_map(local_grads, mesh=mesh, in_specs=in_specs, out_specs=out_specs, check_vma=False)
```

```python
import functools

import jax
import jax.numpy as jnp
import numpy as np
from jax import lax
from jax.experimental import pallas as pl
from jax.experimental.pallas import tpu as pltpu
from jax.sharding import PartitionSpec as P

HEAD_DIM = 128
ROPE_THETA = 1000000.0
NORM_EPS = 1e-6
SM_SCALE = HEAD_DIM ** -0.5
EXP_SCALE = SM_SCALE * 1.4426950408889634
F32, BF16 = jnp.float32, jnp.bfloat16
MESH = pl.DeviceIdType.MESH
PAIR = range(2)

ORDER = (45681723, 82716354)
GATHER = (966006440013400068, 2184020220167401736, 2506024680231802380, 2766026400257202532, 2982028560279402706,
    3282031760302802966, 3436033100324403216, 3824036260363203482, 4342041480408403826, 5042047920472804398, 5114)
REDUCE = (1168011060104200774, 1550016140161501356, 1865018020167701551, 2354021850225101931, 2759026740256702416,
    2990029910286002885, 3626035670336903309, 3817037170362703649, 4197040750400603877, 5377050950505904135, 6307063050624105507,
    6499)
GATHER_RIGHT = (33333333, 22554322, 54555, 322)
GATHER_LEFT = (44444444, 55223455, 1223222, 1234455)
REDUCE_RIGHT = (44444444, 33333333, 1233444, 1234333)
REDUCE_LEFT = (33333333, 44444444, 4333, 444)
PREP_TOKENS = 32


def digits(numbers):
    return [int(c) for n in numbers for c in str(n).zfill(8)]


GATHER_REACH = (digits(GATHER_RIGHT), digits(GATHER_LEFT))
REDUCE_REACH = (digits(REDUCE_RIGHT), digits(REDUCE_LEFT))


def unpacked(numbers):
    out = []
    for n in numbers:
        while n:
            out.append(n % 100000)
            n //= 100000
    return out


G_SEQ, R_SEQ = unpacked(GATHER), unpacked(REDUCE)
GATHER_AT, GATHER_CODE = [n >> 7 for n in G_SEQ], [n & 127 for n in G_SEQ]
REDUCE_AT, REDUCE_CODE = [n >> 7 for n in R_SEQ], [n & 127 for n in R_SEQ]
MAX_HOP = max(map(max, GATHER_REACH + REDUCE_REACH))
SLOTS = [[4 * int(d) + j for d in str(order) for j in range(3 if d == '4' else 2)] for order in ORDER]


def dot(a, b, ca, cb):
    return lax.dot_general(a, b, (((ca,), (cb,)), ((), ())), preferred_element_type=F32)


def lane_sum(x):
    return jnp.sum(x, axis=-1, keepdims=True)


def lane_mean(x):
    return lane_sum(x) * (1.0 / HEAD_DIM)


def roll_half(x):
    return pltpu.roll(x, HEAD_DIM // 2, axis=x.ndim - 1)


def row_sum(prod, ones):
    high = prod.astype(BF16)
    low = (prod - high.astype(F32)).astype(BF16)
    return dot(jnp.concatenate([high, low], 1), ones, 1, 0)


def select_const(index, values):
    if len(values) == 1:
        return jnp.int32(values[0])
    top = 1 << ((len(values) - 1).bit_length() - 1)
    low, high = select_const(index, values[:top]), select_const(index, values[top:])
    return jnp.where((index & top) != 0, high, low)


def packed(index, values, bits):
    per, shift = (4, 2) if bits > 3 else (8, 3)
    assert max(values) < 1 << bits
    words = []
    for i in range(0, len(values), per):
        words.append(sum(v << (bits * k) for k, v in enumerate(values[i:i + per])))
    return (select_const(index >> shift, words) >> ((index & (per - 1)) * bits)) & ((1 << bits) - 1)


def split(code, *bits):
    out = []
    for b in reversed(bits):
        out.append(code & ((1 << b) - 1))
        code = code >> b
    return out[::-1]


def action_masks(nz, sequence, active):
    chips = [[int(active(zz, *act)) for act in sequence] for zz in range(nz)]
    return [[sum(bit << k for k, bit in enumerate(c[i:i + 16])) for c in chips] for i in range(0, len(sequence), 16)]


def landing_slots(nz, sequence, reach):
    slots, users = {}, []
    for key in sorted({act[:4] for act in sequence if act[4]}):
        dr, h, d, el = key
        chips = {zz for zz in range(nz) if d + 1 <= reach[dr][(el * 2 + h) * nz + (zz + (1 - 2 * dr) * d) % nz]}
        n = next((i for i, u in enumerate(users) if not u & chips), len(users))
        users[n:n + 1] = [(users[n] if n < len(users) else set()) | chips]
        slots[key] = n
    return slots, len(users)


def count_at(table, last):
    return [sum(1 for at in table if at == g) for g in range(last)]


def mega_kernel(nz, chunk, per_kv, kv_heads,
                q_hbm, do_hbm, out_hbm, lse_hbm, k_hbm, v_hbm, offc3_hbm, offs3_hbm, offc_hbm, offs_hbm, basec_ref, bases_ref, qw_ref, kw_ref,
                dq_hbm, dkv_hbm, w_ref,
                xq, xdo, xout, qb_a, qb_b, aux_a, aux_b, dq, dq_b, kvall, acc, rsb, kland, lland, pieces, cos_t, sin_t, cos_d, sin_d, kout, dwq, wmine, wslots,
                in_sem, sw_snd, sw_rcv, ld_sem, xs_sem, xr_sem, tab_sem,
                ag_send, ag_recv, rs_send, rs_recv, dq_loc, dq_snd, dq_rcv, dk_loc, dk_snd, dk_rcv, w_snd, w_rcv):
    me = lax.axis_index('cp')
    cp = 2 * nz
    z, core = me >> 1, me & 1
    other = 1 - core
    sib = 2 * z + other
    right = 2 * ((z + 1) & (nz - 1)) + core
    left = 2 * ((z + nz - 1) & (nz - 1)) + core
    tok = 2 * chunk
    rows = tok * per_kv
    qb, aux, dqs = (qb_a, qb_b), (aux_a, aux_b), (dq, dq_b)
    k_rows = tok * kv_heads

    def wrap(i):
        return (i + 2 * nz) & (nz - 1)

    def to(device):
        return dict(device_id={'cp': device}, device_id_type=MESH)

    barrier = pltpu.get_barrier_semaphore()

    def say(i, carry):
        pl.semaphore_signal(barrier, inc=1, **to((me + i) & (cp - 1)))
        return carry

    lax.fori_loop(1, cp, say, 0)

    def off_of(el, mine):
        return pl.multiple_of((core if (el == 0) == mine else other) * chunk, chunk)

    def x_rows(h, el, token, count):
        return pl.ds(pl.multiple_of(((h * 2 + el) * tok + token) * per_kv, chunk), count * per_kv)

    def h_rows(el, token, count):
        return pl.ds(pl.multiple_of((el * tok + token) * per_kv, chunk), count * per_kv)

    lands = ((k_hbm, kland.at[0]), (v_hbm, kland.at[1]), (lse_hbm, lland))
    own_in = [pltpu.make_async_copy(hbm, buf.at[0], in_sem.at[i]) for i, (hbm, buf) in enumerate(lands)]
    swaps = [pltpu.make_async_remote_copy(hbm, buf.at[1], sw_snd.at[i], sw_rcv.at[i], **to(sib)) for i, (hbm, buf) in enumerate(lands)]
    tables = [pltpu.make_async_copy(src, dst, tab_sem.at[i]) for i, (src, dst) in enumerate((
        (offc_hbm, cos_d.at[pl.ds(0, tok)]), (offs_hbm, sin_d.at[pl.ds(0, tok)]),
        (offc3_hbm, cos_t.at[pl.ds(0, tok)]), (offs3_hbm, sin_t.at[pl.ds(0, tok)])))]
    loads = []
    for h in PAIR:
        for el in PAIR:
            heads = lambda c: pl.ds(pl.multiple_of((2 * c + h) * per_kv, per_kv), per_kv)
            src = pl.ds(el * chunk, chunk)
            dst = x_rows(h, el, off_of(el, True), chunk)
            row = []
            for i, (hbm, buf) in enumerate(((q_hbm, xq), (do_hbm, xdo), (out_hbm, xout))):
                there = buf.at[dst].reshape(chunk, per_kv, HEAD_DIM)
                row.append((pltpu.make_async_copy(hbm.at[src, heads(core), :], there, ld_sem.at[h, el, i]),
                            pltpu.make_async_remote_copy(hbm.at[src, heads(other), :], there, xs_sem.at[h, el, i], xr_sem.at[h, el, i],
                                                         **to(sib))))
            loads.append(row)
    for cpy in own_in + tables:
        cpy.start()
    for row in loads:
        for loc, _ in row:
            loc.start()
    def base(el):
        blk = z if el == 0 else 2 * nz - 1 - z
        return basec_ref[blk], bases_ref[blk]

    def turn(cos_ref, sin_ref, lift):
        for el in (1, 0):
            bc, bs = base(el)
            bc, bs = lift(bc), lift(bs)
            step = 32

            def part(i, carry):
                src = pl.ds(pl.multiple_of(i * step, step), step)
                dst = pl.ds(pl.multiple_of(el * tok + i * step, step), step)
                oc, os = cos_ref[src], sin_ref[src]
                cos_ref[dst] = bc * oc - bs * os
                sin_ref[dst] = bs * oc + bc * os
                return carry

            lax.fori_loop(0, tok // step, part, 0)


    def raw_rows(what, side):
        return pl.ds((what * 2 + side) * k_rows, k_rows)

    def raw(what, side, h, el):
        return dq[pl.ds((what * 2 + side) * k_rows + el * chunk * kv_heads + 2 * core + h, chunk, stride=kv_heads), :]

    def unpack_keys(what, side):
        dq[raw_rows(what, side), :] = kland[what, side].astype(F32)

    kw = kw_ref[...]

    def keys_of(side):
        for i in PAIR:
            unpack_keys(i, side)
        for h in PAIR:
            for el in PAIR:
                off = off_of(el, side == 0)
                x = raw(0, side, h, el)
                y = x * lax.rsqrt(lane_mean(x * x) + NORM_EPS) * kw
                tabs = pl.ds(pl.multiple_of(el * tok + off, chunk), chunk)
                kvall[z, h, el, 0, :, pl.ds(off, chunk)] = (y * cos_d[tabs] + roll_half(y) * sin_d[tabs]).T.astype(BF16)
                kvall[z, h, el, 1, :, pl.ds(off, chunk)] = raw(1, side, h, el).T.astype(BF16)

    n_l = 3 * per_kv
    lane_c = lax.broadcasted_iota(jnp.int32, (chunk, HEAD_DIM), 1)

    def pieces_of(side):
        for h in PAIR:
            for el in PAIR:
                val = (lland[side, :, pl.ds(el * chunk, chunk)] * (-1.0 / SM_SCALE)).T
                val = jnp.concatenate([val, jnp.zeros((chunk, HEAD_DIM - val.shape[1]), F32)], axis=1)
                val = pltpu.roll(val, (HEAD_DIM - (2 * core + h) * per_kv) & (HEAD_DIM - 1), axis=1)
                hi = val.astype(BF16).astype(F32)
                mid = (val - hi).astype(BF16).astype(F32)
                low = val - hi - mid
                pc = jnp.where(lane_c < per_kv, hi, jnp.where(lane_c < 2 * per_kv, pltpu.roll(mid, per_kv, axis=1),
                               jnp.where(lane_c < n_l, pltpu.roll(low, 2 * per_kv, axis=1), 0.0)))
                pieces[h, pl.ds(pl.multiple_of(el * tok + off_of(el, side == 0), chunk), chunk)] = pc[:, None, :]

    pl.semaphore_wait(barrier, cp - 1)
    for cpy in swaps:
        cpy.start()
    for row in loads:
        for _, rem in row:
            rem.start()
    for t in tables:
        t.wait()
    turn(cos_d, sin_d, lambda x: x)
    for cpy in own_in:
        cpy.wait()
    keys_of(0)
    turn(cos_t, sin_t, lambda x: x[:, None, :])
    pieces_of(0)
    acc[...] = jnp.zeros_like(acc)
    for i in PAIR:
        swaps[i].wait_recv()
    keys_of(1)

    def lives(reach, el, h, hop, owner):
        return 1 <= hop <= reach[(el * 2 + h) * nz + owner % nz]

    def sign(direction):
        return 1 - 2 * direction

    g_seq, r_seq = [[tuple(split(c, 1, 1, 3, 1, 1)) for c in codes] for codes in (GATHER_CODE, REDUCE_CODE)]
    slots, _ = landing_slots(nz, r_seq, REDUCE_REACH)
    slot_in = [slots.get(act[:4], 0) for act in r_seq]
    slot_out = [slots.get((dr, h, d - 1, el), 0) for dr, h, d, el, _ in r_seq]
    g_wait, g_send, r_wait, r_send = (
        [select_const(z, w) for w in action_masks(nz, seq, active)] for seq, active in (
            (g_seq, lambda zz, dr, h, s, el, _: lives(GATHER_REACH[dr], el, h, s - 1, zz - sign(dr) * (s - 1))),
            (g_seq, lambda zz, dr, h, s, el, _: lives(GATHER_REACH[dr], el, h, s, zz - sign(dr) * (s - 1))),
            (r_seq, lambda zz, dr, h, d, el, on: on and lives(REDUCE_REACH[dr], el, h, d + 1, zz + sign(dr) * d)),
            (r_seq, lambda zz, dr, h, d, el, on: lives(REDUCE_REACH[dr], el, h, d, zz + sign(dr) * d)
             and on == lives(REDUCE_REACH[dr], el, h, d + 1, zz + sign(dr) * d))))

    def on(words, index):
        word = words[0]
        for i, w in enumerate(words[1:], 1):
            word = jnp.where(index >> 4 == i, w, word)
        return (word >> (index & 15)) & 1 == 1

    def neighbour(direction):
        return to(jnp.where(direction == 0, right, left))

    def gather_copy(direction, h, s, el):
        ref = kvall.at[wrap(z - sign(direction) * (s - 1)), h, el]
        return pltpu.make_async_remote_copy(ref, ref, ag_send.at[direction, h, s - 1, el], ag_recv.at[direction, h, s - 1, el],
                                            **neighbour(direction))

    def gather_arrival(direction, h, s, el):
        ref = kvall.at[wrap(z - sign(direction) * s), h, el]
        return pltpu.make_async_remote_copy(ref, ref, ag_send.at[direction, h, s - 1, el], ag_recv.at[direction, h, s - 1, el],
                                            **neighbour(direction))

    def gather_step(a):
        direction, h, s, el, _ = split(packed(a, GATHER_CODE, 7), 1, 1, 3, 1, 1)

        @pl.when(on(g_wait, a))
        def _():
            gather_arrival(direction, h, s - 1, el).wait_recv()

        @pl.when(on(g_send, a))
        def _():
            gather_copy(direction, h, s, el).start()

    def reduce_copy(direction, h, d, el, slot):
        return pltpu.make_async_remote_copy(acc.at[wrap(z + sign(direction) * d), h, el], rsb.at[slot],
                                            rs_send.at[direction, d - 1, h, el], rs_recv.at[direction, d - 1, h, el],
                                            **neighbour(direction))

    def reduce_arrival(direction, h, d, el, slot):
        return pltpu.make_async_remote_copy(acc.at[wrap(z + sign(direction) * d), h, el], rsb.at[slot],
                                            rs_send.at[direction, d, h, el], rs_recv.at[direction, d, h, el],
                                            **neighbour(direction))

    def reduce_step(b):
        direction, h, d, el, _ = split(packed(b, REDUCE_CODE, 7), 1, 1, 3, 1, 1)

        @pl.when(on(r_wait, b))
        def _():
            slot = packed(b, slot_in, 7)
            reduce_arrival(direction, h, d, el, slot).wait_recv()
            acc[wrap(z + sign(direction) * d), h, el] += rsb[slot]

        @pl.when(on(r_send, b))
        def _():
            reduce_copy(direction, h, d, el, packed(b, slot_out, 7)).start()

    def run_actions(step, first, count):
        def one(i, carry):
            step(i)
            return carry

        lax.fori_loop(first, first + count, one, 0)
        return first + count

    head_steps = 3 + 2 * (nz - 1)
    n_steps = 2 * head_steps
    n_pieces = 2 * tok // PREP_TOKENS
    first = n_pieces + 1
    n_ticks = n_steps + n_pieces
    gather_counts = count_at(GATHER_AT, first + n_ticks)
    prep_counts = gather_counts[:1] + [a + b for a, b in zip(gather_counts[1:first:2], gather_counts[2:first:2])]
    reduce_counts = count_at(REDUCE_AT, n_ticks)

    def ticks(g, done):
        ga = run_actions(gather_step, done[0], packed(first + g, gather_counts, 4))
        ra = run_actions(reduce_step, done[1], packed(g, reduce_counts, 4))
        return ga, ra

    gathered = run_actions(gather_step, 0, gather_counts[0])


    swaps[2].wait_recv()
    pieces_of(1)

    sub = PREP_TOKENS
    weight = qw_ref[...]
    ones = jnp.ones((2 * HEAD_DIM, HEAD_DIM), BF16)

    def masks(count):
        lane = lax.broadcasted_iota(jnp.int32, (count * per_kv, HEAD_DIM), 1)
        head = lax.broadcasted_iota(jnp.int32, (count * per_kv, HEAD_DIM), 0) & (per_kv - 1)
        return count, (lane == head) | (lane == head + per_kv) | (lane == head + 2 * per_kv), lane

    flat = lambda x: x.reshape(x.shape[0] * per_kv, HEAD_DIM)
    tall = lambda x: x.reshape(x.shape[0] // per_kv, per_kv, HEAD_DIM)

    def sums(prod, on_mxu):
        return row_sum(prod, ones) if on_mxu else lane_sum(prod)

    def prepare(h, el, t0, sub, lse_mask, lane):
        tabs = pl.ds(pl.multiple_of(el * tok + t0, sub), sub)
        r = x_rows(h, el, t0, sub)
        x = xq[r, :].astype(F32)
        ms = lane_mean(x * x)
        y = tall(x * lax.rsqrt(ms + NORM_EPS) * weight)
        hr = h_rows(el, t0, sub)
        qb[h][hr, :] = flat(y * cos_t[tabs] + roll_half(y) * sin_t[tabs]).astype(BF16)
        r0 = -lane_sum(xdo[r, :].astype(F32) * xout[r, :].astype(F32))
        r1 = r0 - r0.astype(BF16).astype(F32)
        r2 = r1 - r1.astype(BF16).astype(F32)
        dpart = jnp.where(lane == n_l, r0, jnp.where(lane == n_l + 1, r1, jnp.where(lane == n_l + 2, r2, 0.0)))
        consts = flat(jnp.broadcast_to(pieces[h, tabs], (sub, per_kv, HEAD_DIM)))
        aux[h][hr, :] = jnp.where(lse_mask, consts, dpart).astype(BF16)
        dqs[h][hr, :] = jnp.zeros((sub * per_kv, HEAD_DIM), F32)

    def finish(h, el, t0, on_mxu):
        tabs = pl.ds(pl.multiple_of(el * tok + t0, sub), sub)
        r = x_rows(h, el, t0, sub)
        x = xq[r, :].astype(F32)
        rstd = lax.rsqrt(sums(x * x, on_mxu) * (1.0 / HEAD_DIM) + NORM_EPS)
        xhat = x * rstd
        hr = h_rows(el, t0, sub)
        gq = tall(dqs[h][hr, :] * SM_SCALE)
        dy = flat(gq * cos_t[tabs] - roll_half(gq) * sin_t[tabs])
        dxh = dy * weight
        qb[h][hr, :] = (rstd * (dxh - xhat * lane_mean(dxh * xhat))).astype(BF16)
        return jnp.sum((dy * xhat).reshape(-1, 8, HEAD_DIM), axis=0)

    def piece_at(i):
        el = jnp.where(i >= n_pieces // 2, 1, 0)
        return el, (i - el * (n_pieces // 2)) * sub

    for el in PAIR:
        for loc, _ in loads[el]:
            loc.wait()
    quarter = chunk // (2 * sub)
    wide = masks(2 * sub)

    def piece(i, gathered):
        @pl.when(i == 2 * quarter)
        def _():
            for el in PAIR:
                for _, rem in loads[el]:
                    rem.wait_recv()

        part, k = jnp.where(i >= 2 * quarter, 1, 0), i & (2 * quarter - 1)
        el = jnp.where(k >= quarter, 1, 0)
        prepare(0, el, (core ^ part ^ el) * chunk + (k - el * quarter) * 2 * sub, *wide)
        return run_actions(gather_step, gathered, packed(1 + i, prep_counts, 4))

    gathered = lax.fori_loop(0, 4 * quarter, piece, gathered)
    for el in PAIR:
        for loc, rem in loads[2 + el]:
            loc.wait()
            rem.wait_recv()
    dwq[...] = jnp.zeros_like(dwq)

    keys = tok
    krow = lax.broadcasted_iota(jnp.int32, (HEAD_DIM, keys), 0)
    ones_k = jnp.where(krow < n_l, 1.0, 0.0).astype(BF16)
    ones_v = jnp.where((krow >= n_l) & (krow < n_l + 3), 1.0, 0.0).astype(BF16)
    klan = lax.broadcasted_iota(jnp.int32, (per_kv, keys), 1)

    def work(h, g, done):
        u = g - h * head_steps
        slot = packed(u, SLOTS[h], 6)
        delta, j = (slot >> 2) - 4, slot & 3
        own = delta == 0
        kz = wrap(z + delta)
        lower = kz < z
        q_late = jnp.where(own, jnp.where(j >= 1, 1, 0), jnp.where(lower, j, 1))
        k_late = jnp.where(own, jnp.where(j >= 2, 1, 0), jnp.where(lower, 0, j))
        q_blk = jnp.where(q_late == 1, 2 * nz - 1 - z, z)
        k_blk = jnp.where(k_late == 1, 2 * nz - 1 - kz, kz)
        off = (q_blk - k_blk) * tok
        r = pl.ds(pl.multiple_of((h * 2 + q_late) * rows, rows), rows)
        k, v = kvall[kz, h, k_late, 0], kvall[kz, h, k_late, 1]
        hr = pl.ds(pl.multiple_of(q_late * rows, rows), rows)
        qq, ax, dd = qb[h][hr, :], aux[h][hr, :], xdo[r, :]
        s = dot(jnp.concatenate([qq, ax], 1), jnp.concatenate([k, ones_k], 0), 1, 0)
        dp = dot(jnp.concatenate([dd, ax], 1), jnp.concatenate([v, ones_v], 0), 1, 0)
        p = jnp.exp2(s * EXP_SCALE)
        p = jnp.concatenate([jnp.where(klan <= off + t, p[per_kv * t:per_kv * (t + 1)], 0.0) for t in range(tok)], 0)
        ds = (p * dp).astype(BF16)
        pb = p.astype(BF16)
        dqs[h][hr, :] += dot(ds, k, 1, 1)
        acc[kz, h, k_late, 0] += dot(qq, ds, 0, 0)
        acc[kz, h, k_late, 1] += dot(dd, pb, 0, 0)
        el, t0 = piece_at(jnp.minimum(u, n_pieces - 1))
        if h == 0:
            prepare(1, el, t0, *masks(sub))
        else:
            dwq[...] += jnp.where(u < n_pieces, finish(0, el, t0, False), 0.0)
        return ticks(g, done)

    done = (gathered, jnp.int32(0))
    for h in PAIR:
        done = lax.fori_loop(h * head_steps, (h + 1) * head_steps, functools.partial(work, h), done)

    def last(i, done):
        el, t0 = piece_at(i)
        dwq[...] += finish(1, el, t0, True)
        return ticks(n_steps + i, done)

    def back(x, ssum, g, cos, sin, w):
        rstd = lax.rsqrt(ssum * (1.0 / HEAD_DIM) + NORM_EPS)
        xhat = x * rstd
        dy = g * cos - roll_half(g) * sin
        dxh = dy * w
        dx = rstd * (dxh - xhat * lane_mean(dxh * xhat))
        return dx, jnp.sum((dy * xhat).reshape(-1, 8, HEAD_DIM), axis=0)

    outs = []

    def send_queries(h, el):
        heads = pl.ds(pl.multiple_of((2 * core + h) * per_kv, per_kv), per_kv)
        dst = dq_hbm.at[pl.ds(el * chunk, chunk), heads, :]
        part = lambda mine: qb[h].at[h_rows(el, off_of(el, mine), chunk)].reshape(chunk, per_kv, HEAD_DIM)
        both = (pltpu.make_async_remote_copy(part(False), dst, dq_snd.at[h, el], dq_rcv.at[h, el], **to(sib)),
                pltpu.make_async_copy(part(True), dst, dq_loc.at[h, el]))
        outs.append(both)
        for cpy in both:
            cpy.start()

    hold = 4 * k_rows

    def key_gradients(h, dwk):
        for el in PAIR:
            kout[h, el, 1] = acc[z, h, el, 1].T.astype(BF16)
            dq[pl.ds(hold, tok), :] = acc[z, h, el, 0].T * SM_SCALE
            for s in PAIR:
                off = off_of(el, s == 0)
                x = raw(0, s, h, el)
                tabs = pl.ds(pl.multiple_of(el * tok + off, chunk), chunk)
                dx, dwp = back(x, lane_sum(x * x), dq[pl.ds(pl.multiple_of(hold + off, chunk), chunk), :], cos_d[tabs], sin_d[tabs], kw)
                kout[h, el, 0, pl.ds(off, chunk), :] = dx.astype(BF16)
                dwk = dwk + dwp
            dst = dkv_hbm.at[2 * core + h, el]
            both = (pltpu.make_async_copy(kout.at[h, el, :, pl.ds(off_of(el, True), chunk), :], dst, dk_loc.at[h, el]),
                    pltpu.make_async_remote_copy(kout.at[h, el, :, pl.ds(off_of(el, False), chunk), :], dst, dk_snd.at[h, el],
                                                 dk_rcv.at[h, el], **to(sib)))
            outs.append(both)
            for cpy in both:
                cpy.start()
        return dwk

    for el in PAIR:
        send_queries(0, el)
    for side in PAIR:
        unpack_keys(0, side)

    def drain_gather(a, carry):
        direction, h, s, el, _ = split(packed(a, GATHER_CODE, 7), 1, 1, 3, 1, 1)

        @pl.when(on(g_send, a))
        def _():
            gather_copy(direction, h, s, el).wait_send()

        return carry

    lax.fori_loop(0, len(G_SEQ), drain_gather, 0)
    for cpy in swaps:
        cpy.wait_send()
    for row in loads:
        for _, rem in row:
            rem.wait_send()

    complete = 1 + max(at for at, (_, h, d, _, _) in zip(REDUCE_AT, r_seq) if h == 0 and d == 0) - n_steps
    assert complete <= n_pieces
    complete, begin = max(complete, 0), 0
    for end in sorted({complete, n_pieces // 2, n_pieces}):
        if end > begin:
            done = lax.fori_loop(begin, end, last, done)
        if end in (n_pieces // 2, n_pieces):
            send_queries(1, 2 * end // n_pieces - 1)
        if end == complete:
            dwk = key_gradients(0, jnp.zeros((8, HEAD_DIM), F32))
        begin = end
    run_actions(reduce_step, done[1], len(R_SEQ) - done[1])
    dwk = key_gradients(1, dwk)
    top = lax.broadcasted_iota(jnp.int32, (8, HEAD_DIM), 0)
    wmine[...] = jnp.where(top == 0, jnp.sum(dwq[...], axis=0, keepdims=True),
                           jnp.where(top == 1, jnp.sum(dwk, axis=0, keepdims=True), 0.0))

    def weight_copy(i):
        return pltpu.make_async_remote_copy(wmine, wslots.at[cp - i], w_snd.at[i], w_rcv.at[cp - i], **to((me + i) & (cp - 1)))

    def weight_send(i, carry):
        weight_copy(i).start()
        return carry

    lax.fori_loop(1, cp, weight_send, 0)

    def drain_reduce(b, carry):
        direction, h, d, el, _ = split(packed(b, REDUCE_CODE, 7), 1, 1, 3, 1, 1)

        @pl.when(on(r_send, b))
        def _():
            reduce_copy(direction, h, d, el, 0).wait_send()

        return carry

    lax.fori_loop(0, len(R_SEQ), drain_reduce, 0)

    def weight_wait(i, carry):
        pltpu.make_async_remote_copy(wmine, wslots.at[i], w_snd.at[i], w_rcv.at[i], **to((me + i) & (cp - 1))).wait()
        return carry

    lax.fori_loop(1, cp, weight_wait, 0)
    wslots[0] = wmine[...]
    w_ref[...] = lax.fori_loop(0, cp, lambda i, total: total + wslots[(i - me + cp) & (cp - 1)], jnp.zeros((8, HEAD_DIM), F32))
    for loc, rem in outs:
        loc.wait()
        rem.wait()


def mega(nz, kv_heads, q_raw, d_out, out_fwd, lse, k_rows, v_rows, offc, offs, basec, bases, qw, kw):
    tok, heads, hd = q_raw.shape
    chunk, per_kv = tok // 2, heads // kv_heads
    any_spec = pl.BlockSpec(memory_space=pl.ANY)
    vmem = pl.BlockSpec(memory_space=pltpu.VMEM)
    dma, scr = pltpu.SemaphoreType.DMA, pltpu.VMEM
    n_rows = 2 * tok * per_kv
    _, n_slots = landing_slots(nz, [tuple(split(c, 1, 1, 3, 1, 1)) for c in REDUCE_CODE], REDUCE_REACH)
    hbm = lambda a: pltpu.with_memory_space_constraint(a, pltpu.HBM)
    args = [q_raw, d_out, out_fwd, lse, k_rows, v_rows, offc[:, None], offs[:, None], offc, offs]
    return pl.pallas_call(
        functools.partial(mega_kernel, nz, chunk, per_kv, kv_heads),
        in_specs=[any_spec] * len(args) + [vmem] * 4,
        out_specs=[any_spec, any_spec, vmem],
        out_shape=[jax.ShapeDtypeStruct(q_raw.shape, BF16), jax.ShapeDtypeStruct((kv_heads, 2, 2, chunk, hd), BF16),
                   jax.ShapeDtypeStruct((8, hd), F32)],
        scratch_shapes=[
            *[scr((2 * n_rows, hd), BF16)] * 3, *[scr((n_rows, hd), BF16)] * 4, *[scr((n_rows, hd), F32)] * 2,
            scr((nz, 2, 2, 2, hd, tok), BF16), scr((nz, 2, 2, 2, hd, tok), F32), scr((n_slots, 2, hd, tok), F32),
            scr((2, 2) + k_rows.shape, BF16), scr((2,) + lse.shape, F32), scr((2, 2 * tok, 1, hd), F32),
            *[scr((2 * tok, 1, hd), F32)] * 2, *[scr((2 * tok, hd), F32)] * 2,
            scr((2, 2, 2, tok, hd), BF16), *[scr((8, hd), F32)] * 2, scr((2 * nz, 8, hd), F32),
            *[dma((3,))] * 3, *[dma((2, 2, 3))] * 3, dma((4,)), *[dma((2, 2, MAX_HOP, 2))] * 2, *[dma((2, MAX_HOP, 2, 2))] * 2,
            *[dma((2, 2))] * 6, *[dma((2 * nz,))] * 2,
        ],
        name='attn_bwd',
        compiler_params=pltpu.CompilerParams(vmem_limit_bytes=67000000, collective_id=0, has_side_effects=True),
    )(*[hbm(a) for a in args], basec, bases, qw, kw)


def emit_kernel(n, dq_in, dkv_in, w_in, dq_out, dk_out, dv_out, wq_out, wk_out, buf, in_sem, out_sem):
    step = dq_in.shape[0] // n
    part = lambda ref, i: ref.at[pl.ds(i * step, step)]
    reads = [pltpu.make_async_copy(part(dq_in, i), part(buf, i), in_sem.at[i]) for i in range(n)]
    writes = [pltpu.make_async_copy(part(buf, i), part(dq_out, i), out_sem.at[i]) for i in range(n)]
    for cpy in reads:
        cpy.start()
    wq_out[...], wk_out[...] = w_in[0:1, :], w_in[1:2, :]
    kv_heads, halves, _, chunk, _ = dkv_in.shape
    for i in range(n):
        reads[i].wait()
        writes[i].start()
        if i < 2 * halves:
            ref, half, what = (dk_out, dv_out)[i & 1], i >> 1, i & 1
            x = dkv_in[:, half, what].astype(F32)
            ref[pl.ds(half * chunk, chunk)] = jnp.stack([x[h] for h in range(kv_heads)], axis=1).astype(BF16)
    for cpy in writes:
        cpy.wait()


def emit(dq, dkv, weights):
    tok, _, hd = dq.shape
    kv_heads = dkv.shape[0]
    n = 8
    any_spec, vmem = pl.BlockSpec(memory_space=pl.ANY), pl.BlockSpec(memory_space=pltpu.VMEM)
    return pl.pallas_call(
        functools.partial(emit_kernel, n),
        in_specs=[any_spec, vmem, vmem],
        out_specs=[any_spec] + [vmem] * 4,
        out_shape=[jax.ShapeDtypeStruct(dq.shape, BF16)] + [jax.ShapeDtypeStruct((tok, kv_heads, hd), BF16)] * 2
        + [jax.ShapeDtypeStruct((1, hd), F32)] * 2,
        scratch_shapes=[pltpu.VMEM(dq.shape, BF16), *[pltpu.SemaphoreType.DMA((n,))] * 2],
        name='emit',
    )(pltpu.with_memory_space_constraint(dq, pltpu.HBM), dkv, weights)


def solution(mesh):
    cp_size = mesh.shape['cp']
    nz = cp_size // 2

    def local_grads(q_raw, k_raw, v_proj, out_fwd, lse_fwd, d_out, q_norm, k_norm):
        tok, kv_heads = k_raw.shape[0], k_raw.shape[1]
        inv_freq = ROPE_THETA ** (-np.arange(0, HEAD_DIM, 2, dtype=np.float64) / HEAD_DIM)
        inv_freq = np.concatenate([inv_freq, inv_freq])
        sign = np.where(np.arange(HEAD_DIM) < HEAD_DIM // 2, -1.0, 1.0)
        off_ang = np.arange(tok)[:, None] * inv_freq
        base_ang = (np.arange(cp_size) * tok)[:, None] * inv_freq
        table = lambda x: jnp.asarray(x, F32)
        rows = lambda a: a.reshape(tok * kv_heads, HEAD_DIM)
        dq_raw, dkv, sums = mega(nz, kv_heads, q_raw, d_out, out_fwd, lse_fwd.T, rows(k_raw), rows(v_proj),
                                 table(np.cos(off_ang)), table(np.sin(off_ang) * sign),
                                 table(np.cos(base_ang))[:, None], table(np.sin(base_ang) * sign)[:, None],
                                 q_norm.reshape(1, HEAD_DIM), k_norm.reshape(1, HEAD_DIM))
        dq_raw, dk_raw, dv, wq, wk = emit(dq_raw, dkv, sums)
        return dq_raw, dk_raw, dv, wq.reshape(HEAD_DIM), wk.reshape(HEAD_DIM)

    row_spec = P(('dp', 'cp'))
    in_specs = (row_spec, row_spec, row_spec, row_spec, row_spec, row_spec, P(), P())
    out_specs = (row_spec, row_spec, row_spec, P('dp'), P('dp'))
    return jax.shard_map(local_grads, mesh=mesh, in_specs=in_specs, out_specs=out_specs, check_vma=False)
```

```python
import functools

import jax
import jax.numpy as jnp
import numpy as np
from jax import lax
from jax.experimental import pallas as pl
from jax.experimental.pallas import tpu as pltpu
from jax.sharding import PartitionSpec as P

HEAD_DIM = 128
ROPE_THETA = 1000000.0
NORM_EPS = 1e-6
SM_SCALE = HEAD_DIM ** -0.5
EXP_SCALE = SM_SCALE * 1.4426950408889634
F32, BF16 = jnp.float32, jnp.bfloat16
MESH = pl.DeviceIdType.MESH
PAIR = range(2)

ORDER = (56817243, 87136254)
GATHER = (774003240013200070, 2120018280154401482, 2186022520206002126, 2472023200238602278, 2646025740253202512,
    2792027260279402580, 3114030540290602732, 3636033080324803096, 4146040820395203630, 4858043420434004152, 4856)
REDUCE = (720006580065600262, 1165011640110000974, 1423014830135701294, 1931018650180201545, 2354024180241602119,
    2695026040250102309, 3311031190305302862, 3689035210349803369, 3947038770358703627, 4839041350419704006, 6433059850582705121,
    649906435)
GATHER_RIGHT = (54555555, 22554322, 22, 322)
GATHER_LEFT = (23222222, 55223455, 1234555, 1234455)
REDUCE_RIGHT = (43333443, 33333333, 1234444, 1234333)
REDUCE_LEFT = (34444334, 44444444, 333, 444)
PREP_TOKENS = 32


def digits(numbers):
    return [int(c) for n in numbers for c in str(n).zfill(8)]


GATHER_REACH = (digits(GATHER_RIGHT), digits(GATHER_LEFT))
REDUCE_REACH = (digits(REDUCE_RIGHT), digits(REDUCE_LEFT))


def unpacked(numbers):
    out = []
    for n in numbers:
        while n:
            out.append(n % 100000)
            n //= 100000
    return out


G_SEQ, R_SEQ = unpacked(GATHER), unpacked(REDUCE)
GATHER_AT, GATHER_CODE = [n >> 7 for n in G_SEQ], [n & 127 for n in G_SEQ]
REDUCE_AT, REDUCE_CODE = [n >> 7 for n in R_SEQ], [n & 127 for n in R_SEQ]
GATHER_HOPS, REDUCE_HOPS = max(map(max, GATHER_REACH)), max(map(max, REDUCE_REACH))
SLOTS = [[4 * int(d) + j for d in str(order) for j in range(3 if d == '4' else 2)] for order in ORDER]


def dot(a, b, ca, cb):
    return lax.dot_general(a, b, (((ca,), (cb,)), ((), ())), preferred_element_type=F32)


def lane_sum(x):
    return jnp.sum(x, axis=-1, keepdims=True)


def lane_mean(x):
    return lane_sum(x) * (1.0 / HEAD_DIM)


def roll_half(x):
    return pltpu.roll(x, HEAD_DIM // 2, axis=x.ndim - 1)


def row_sum(prod, ones):
    high = prod.astype(BF16)
    low = (prod - high.astype(F32)).astype(BF16)
    return dot(jnp.concatenate([high, low], 1), ones, 1, 0)


def select_const(index, values):
    if len(values) == 1:
        return jnp.int32(values[0])
    top = 1 << ((len(values) - 1).bit_length() - 1)
    low, high = select_const(index, values[:top]), select_const(index, values[top:])
    return jnp.where((index & top) != 0, high, low)


def packed(index, values, bits):
    per, shift = (4, 2) if bits > 3 else (8, 3)
    assert max(values) < 1 << bits
    words = []
    for i in range(0, len(values), per):
        words.append(sum(v << (bits * k) for k, v in enumerate(values[i:i + per])))
    return (select_const(index >> shift, words) >> ((index & (per - 1)) * bits)) & ((1 << bits) - 1)


def split(code, *bits):
    out = []
    for b in reversed(bits):
        out.append(code & ((1 << b) - 1))
        code = code >> b
    return out[::-1]


def action_masks(nz, sequence, active):
    chips = [[int(active(zz, *act)) for act in sequence] for zz in range(nz)]
    return [[sum(bit << k for k, bit in enumerate(c[i:i + 16])) for c in chips] for i in range(0, len(sequence), 16)]


def landing_slots(nz, sequence, reach):
    slots, users = {}, []
    for key in sorted({act[:4] for act in sequence if act[4]}):
        dr, h, d, el = key
        chips = {zz for zz in range(nz) if d + 1 <= reach[dr][(el * 2 + h) * nz + (zz + (1 - 2 * dr) * d) % nz]}
        n = next((i for i, u in enumerate(users) if not u & chips), len(users))
        users[n:n + 1] = [(users[n] if n < len(users) else set()) | chips]
        slots[key] = n
    return slots, len(users)


def count_at(table, last):
    return [sum(1 for at in table if at == g) for g in range(last)]


def mega_kernel(nz, chunk, per_kv, kv_heads,
                q_hbm, do_hbm, out_hbm, lse_hbm, k_hbm, v_hbm, offc3_hbm, offs3_hbm, offc_hbm, offs_hbm, basec_ref, bases_ref, qw_ref, kw_ref,
                dq_hbm, dkv_hbm, w_ref,
                xq, xdo, xout, qb_a, qb_b, aux_a, aux_b, dq, dq_b, kvall, acc, rsb, kland, lland, pieces, cos_t, sin_t, cos_d, sin_d, kout, dwq, wmine, wslots,
                in_sem, sw_snd, sw_rcv, ld_sem, xs_sem, xr_sem, tab_sem,
                ag_send, ag_recv, rs_send, rs_recv, dq_loc, dq_snd, dq_rcv, dk_loc, dk_snd, dk_rcv, w_snd, w_rcv):
    me = lax.axis_index('cp')
    cp = 2 * nz
    z, core = me >> 1, me & 1
    other = 1 - core
    sib = 2 * z + other
    right = 2 * ((z + 1) & (nz - 1)) + core
    left = 2 * ((z + nz - 1) & (nz - 1)) + core
    tok = 2 * chunk
    rows = tok * per_kv
    qb, aux, dqs = (qb_a, qb_b), (aux_a, aux_b), (dq, dq_b)
    k_rows = tok * kv_heads

    def wrap(i):
        return (i + 2 * nz) & (nz - 1)

    def to(device):
        return dict(device_id={'cp': device}, device_id_type=MESH)

    barrier = pltpu.get_barrier_semaphore()

    def say(i, carry):
        pl.semaphore_signal(barrier, inc=1, **to((me + i) & (cp - 1)))
        return carry

    lax.fori_loop(1, cp, say, 0)

    def off_of(el, mine):
        return pl.multiple_of((core if (el == 0) == mine else other) * chunk, chunk)

    def x_rows(h, el, token, count):
        return pl.ds(pl.multiple_of(((h * 2 + el) * tok + token) * per_kv, chunk), count * per_kv)

    def h_rows(el, token, count):
        return pl.ds(pl.multiple_of((el * tok + token) * per_kv, chunk), count * per_kv)

    lands = ((k_hbm, kland.at[0]), (v_hbm, kland.at[1]), (lse_hbm, lland))
    own_in = [pltpu.make_async_copy(hbm, buf.at[0], in_sem.at[i]) for i, (hbm, buf) in enumerate(lands)]
    swaps = [pltpu.make_async_remote_copy(hbm, buf.at[1], sw_snd.at[i], sw_rcv.at[i], **to(sib)) for i, (hbm, buf) in enumerate(lands)]
    tables = [pltpu.make_async_copy(src, dst, tab_sem.at[i]) for i, (src, dst) in enumerate((
        (offc_hbm, cos_d.at[pl.ds(0, tok)]), (offs_hbm, sin_d.at[pl.ds(0, tok)]),
        (offc3_hbm, cos_t.at[pl.ds(0, tok)]), (offs3_hbm, sin_t.at[pl.ds(0, tok)])))]
    loads = []
    for h in PAIR:
        for el in PAIR:
            heads = lambda c: pl.ds(pl.multiple_of((2 * c + h) * per_kv, per_kv), per_kv)
            src = pl.ds(el * chunk, chunk)
            dst = x_rows(h, el, off_of(el, True), chunk)
            row = []
            for i, (hbm, buf) in enumerate(((q_hbm, xq), (do_hbm, xdo), (out_hbm, xout))):
                there = buf.at[dst].reshape(chunk, per_kv, HEAD_DIM)
                row.append((pltpu.make_async_copy(hbm.at[src, heads(core), :], there, ld_sem.at[h, el, i]),
                            pltpu.make_async_remote_copy(hbm.at[src, heads(other), :], there, xs_sem.at[h, el, i], xr_sem.at[h, el, i],
                                                         **to(sib))))
            loads.append(row)
    for cpy in own_in + tables:
        cpy.start()
    for row in loads:
        for loc, _ in row:
            loc.start()
    def base(el):
        blk = z if el == 0 else 2 * nz - 1 - z
        return basec_ref[blk], bases_ref[blk]

    def turn(cos_ref, sin_ref, lift):
        for el in (1, 0):
            bc, bs = base(el)
            bc, bs = lift(bc), lift(bs)
            step = 32

            def part(i, carry):
                src = pl.ds(pl.multiple_of(i * step, step), step)
                dst = pl.ds(pl.multiple_of(el * tok + i * step, step), step)
                oc, os = cos_ref[src], sin_ref[src]
                cos_ref[dst] = bc * oc - bs * os
                sin_ref[dst] = bs * oc + bc * os
                return carry

            lax.fori_loop(0, tok // step, part, 0)


    def raw_rows(what, side):
        return pl.ds((what * 2 + side) * k_rows, k_rows)

    def raw(what, side, h, el):
        return dq[pl.ds((what * 2 + side) * k_rows + el * chunk * kv_heads + 2 * core + h, chunk, stride=kv_heads), :]

    def unpack_keys(what, side):
        dq[raw_rows(what, side), :] = kland[what, side].astype(F32)

    kw = kw_ref[...]

    def keys_of(side):
        for i in PAIR:
            unpack_keys(i, side)
        for h in PAIR:
            for el in PAIR:
                off = off_of(el, side == 0)
                x = raw(0, side, h, el)
                y = x * lax.rsqrt(lane_mean(x * x) + NORM_EPS) * kw
                tabs = pl.ds(pl.multiple_of(el * tok + off, chunk), chunk)
                kvall[z, h, el, 0, :, pl.ds(off, chunk)] = (y * cos_d[tabs] + roll_half(y) * sin_d[tabs]).T.astype(BF16)
                kvall[z, h, el, 1, :, pl.ds(off, chunk)] = raw(1, side, h, el).T.astype(BF16)

    n_l = 3 * per_kv
    lane_c = lax.broadcasted_iota(jnp.int32, (chunk, HEAD_DIM), 1)

    def pieces_of(side):
        for h in PAIR:
            for el in PAIR:
                val = (lland[side, :, pl.ds(el * chunk, chunk)] * (-1.0 / SM_SCALE)).T
                val = jnp.concatenate([val, jnp.zeros((chunk, HEAD_DIM - val.shape[1]), F32)], axis=1)
                val = pltpu.roll(val, (HEAD_DIM - (2 * core + h) * per_kv) & (HEAD_DIM - 1), axis=1)
                hi = val.astype(BF16).astype(F32)
                mid = (val - hi).astype(BF16).astype(F32)
                low = val - hi - mid
                pc = jnp.where(lane_c < per_kv, hi, jnp.where(lane_c < 2 * per_kv, pltpu.roll(mid, per_kv, axis=1),
                               jnp.where(lane_c < n_l, pltpu.roll(low, 2 * per_kv, axis=1), 0.0)))
                pieces[h, pl.ds(pl.multiple_of(el * tok + off_of(el, side == 0), chunk), chunk)] = pc[:, None, :]

    pl.semaphore_wait(barrier, cp - 1)
    for cpy in swaps:
        cpy.start()
    for row in loads:
        for _, rem in row:
            rem.start()
    for t in tables:
        t.wait()
    turn(cos_d, sin_d, lambda x: x)
    for cpy in own_in:
        cpy.wait()
    keys_of(0)
    turn(cos_t, sin_t, lambda x: x[:, None, :])
    pieces_of(0)
    acc[...] = jnp.zeros_like(acc)
    for i in PAIR:
        swaps[i].wait_recv()
    keys_of(1)

    def lives(reach, el, h, hop, owner):
        return 1 <= hop <= reach[(el * 2 + h) * nz + owner % nz]

    def sign(direction):
        return 1 - 2 * direction

    g_seq, r_seq = [[tuple(split(c, 1, 1, 3, 1, 1)) for c in codes] for codes in (GATHER_CODE, REDUCE_CODE)]
    slots, _ = landing_slots(nz, r_seq, REDUCE_REACH)
    slot_in = [slots.get(act[:4], 0) for act in r_seq]
    slot_out = [slots.get((dr, h, d - 1, el), 0) for dr, h, d, el, _ in r_seq]
    g_wait, g_send, r_wait, r_send = (
        [select_const(z, w) for w in action_masks(nz, seq, active)] for seq, active in (
            (g_seq, lambda zz, dr, h, s, el, _: lives(GATHER_REACH[dr], el, h, s - 1, zz - sign(dr) * (s - 1))),
            (g_seq, lambda zz, dr, h, s, el, _: lives(GATHER_REACH[dr], el, h, s, zz - sign(dr) * (s - 1))),
            (r_seq, lambda zz, dr, h, d, el, on: on and lives(REDUCE_REACH[dr], el, h, d + 1, zz + sign(dr) * d)),
            (r_seq, lambda zz, dr, h, d, el, on: lives(REDUCE_REACH[dr], el, h, d, zz + sign(dr) * d)
             and on == lives(REDUCE_REACH[dr], el, h, d + 1, zz + sign(dr) * d))))

    def on(words, index):
        word = words[0]
        for i, w in enumerate(words[1:], 1):
            word = jnp.where(index >> 4 == i, w, word)
        return (word >> (index & 15)) & 1 == 1

    def neighbour(direction):
        return to(jnp.where(direction == 0, right, left))

    def gather_copy(direction, h, s, el):
        ref = kvall.at[wrap(z - sign(direction) * (s - 1)), h, el]
        return pltpu.make_async_remote_copy(ref, ref, ag_send.at[direction, h, s - 1, el], ag_recv.at[direction, h, s - 1, el],
                                            **neighbour(direction))

    def gather_arrival(direction, h, s, el):
        ref = kvall.at[wrap(z - sign(direction) * s), h, el]
        return pltpu.make_async_remote_copy(ref, ref, ag_send.at[direction, h, s - 1, el], ag_recv.at[direction, h, s - 1, el],
                                            **neighbour(direction))

    def gather_step(a):
        direction, h, s, el, _ = split(packed(a, GATHER_CODE, 7), 1, 1, 3, 1, 1)

        @pl.when(on(g_wait, a))
        def _():
            gather_arrival(direction, h, s - 1, el).wait_recv()

        @pl.when(on(g_send, a))
        def _():
            gather_copy(direction, h, s, el).start()

    def reduce_copy(direction, h, d, el, slot):
        return pltpu.make_async_remote_copy(acc.at[wrap(z + sign(direction) * d), h, el], rsb.at[slot],
                                            rs_send.at[direction, d - 1, h, el], rs_recv.at[direction, d - 1, h, el],
                                            **neighbour(direction))

    def reduce_arrival(direction, h, d, el, slot):
        return pltpu.make_async_remote_copy(acc.at[wrap(z + sign(direction) * d), h, el], rsb.at[slot],
                                            rs_send.at[direction, d, h, el], rs_recv.at[direction, d, h, el],
                                            **neighbour(direction))

    def reduce_step(b):
        direction, h, d, el, _ = split(packed(b, REDUCE_CODE, 7), 1, 1, 3, 1, 1)

        @pl.when(on(r_wait, b))
        def _():
            slot = packed(b, slot_in, 7)
            reduce_arrival(direction, h, d, el, slot).wait_recv()
            acc[wrap(z + sign(direction) * d), h, el] += rsb[slot]

        @pl.when(on(r_send, b))
        def _():
            reduce_copy(direction, h, d, el, packed(b, slot_out, 7)).start()

    def run_actions(step, first, count):
        def one(i, carry):
            step(i)
            return carry

        lax.fori_loop(first, first + count, one, 0)
        return first + count

    head_steps = 3 + 2 * (nz - 1)
    n_steps = 2 * head_steps
    n_pieces = 2 * tok // PREP_TOKENS
    first = n_pieces + 1
    n_ticks = n_steps + n_pieces
    gather_counts = count_at(GATHER_AT, first + n_ticks)
    prep_counts = gather_counts[:1] + [a + b for a, b in zip(gather_counts[1:first:2], gather_counts[2:first:2])]
    reduce_counts = count_at(REDUCE_AT, n_ticks)

    def ticks(g, done):
        ga = run_actions(gather_step, done[0], packed(first + g, gather_counts, 4))
        ra = run_actions(reduce_step, done[1], packed(g, reduce_counts, 4))
        return ga, ra

    gathered = run_actions(gather_step, 0, gather_counts[0])


    swaps[2].wait_recv()
    pieces_of(1)

    sub = PREP_TOKENS
    weight = qw_ref[...]
    ones = jnp.ones((2 * HEAD_DIM, HEAD_DIM), BF16)

    def masks(count):
        lane = lax.broadcasted_iota(jnp.int32, (count * per_kv, HEAD_DIM), 1)
        head = lax.broadcasted_iota(jnp.int32, (count * per_kv, HEAD_DIM), 0) & (per_kv - 1)
        return count, (lane == head) | (lane == head + per_kv) | (lane == head + 2 * per_kv), lane

    flat = lambda x: x.reshape(x.shape[0] * per_kv, HEAD_DIM)
    tall = lambda x: x.reshape(x.shape[0] // per_kv, per_kv, HEAD_DIM)

    def sums(prod, on_mxu):
        return row_sum(prod, ones) if on_mxu else lane_sum(prod)

    def prepare(h, el, t0, sub, lse_mask, lane):
        tabs = pl.ds(pl.multiple_of(el * tok + t0, sub), sub)
        r = x_rows(h, el, t0, sub)
        x = xq[r, :].astype(F32)
        ms = lane_mean(x * x)
        y = tall(x * lax.rsqrt(ms + NORM_EPS) * weight)
        hr = h_rows(el, t0, sub)
        qb[h][hr, :] = flat(y * cos_t[tabs] + roll_half(y) * sin_t[tabs]).astype(BF16)
        r0 = -lane_sum(xdo[r, :].astype(F32) * xout[r, :].astype(F32))
        r1 = r0 - r0.astype(BF16).astype(F32)
        r2 = r1 - r1.astype(BF16).astype(F32)
        dpart = jnp.where(lane == n_l, r0, jnp.where(lane == n_l + 1, r1, jnp.where(lane == n_l + 2, r2, 0.0)))
        consts = flat(jnp.broadcast_to(pieces[h, tabs], (sub, per_kv, HEAD_DIM)))
        aux[h][hr, :] = jnp.where(lse_mask, consts, dpart).astype(BF16)
        dqs[h][hr, :] = jnp.zeros((sub * per_kv, HEAD_DIM), F32)

    def finish(h, el, t0, on_mxu):
        tabs = pl.ds(pl.multiple_of(el * tok + t0, sub), sub)
        r = x_rows(h, el, t0, sub)
        x = xq[r, :].astype(F32)
        rstd = lax.rsqrt(sums(x * x, on_mxu) * (1.0 / HEAD_DIM) + NORM_EPS)
        xhat = x * rstd
        hr = h_rows(el, t0, sub)
        gq = tall(dqs[h][hr, :] * SM_SCALE)
        dy = flat(gq * cos_t[tabs] - roll_half(gq) * sin_t[tabs])
        dxh = dy * weight
        qb[h][hr, :] = (rstd * (dxh - xhat * lane_mean(dxh * xhat))).astype(BF16)
        return jnp.sum((dy * xhat).reshape(-1, 8, HEAD_DIM), axis=0)

    def piece_at(i):
        el = jnp.where(i >= n_pieces // 2, 1, 0)
        return el, (i - el * (n_pieces // 2)) * sub

    for el in PAIR:
        for loc, _ in loads[el]:
            loc.wait()
    quarter = chunk // (2 * sub)
    wide = masks(2 * sub)

    def piece(i, gathered):
        @pl.when(i == 2 * quarter)
        def _():
            for el in PAIR:
                for _, rem in loads[el]:
                    rem.wait_recv()

        part, k = jnp.where(i >= 2 * quarter, 1, 0), i & (2 * quarter - 1)
        el = jnp.where(k >= quarter, 1, 0)
        prepare(0, el, (core ^ part ^ el) * chunk + (k - el * quarter) * 2 * sub, *wide)
        return run_actions(gather_step, gathered, packed(1 + i, prep_counts, 4))

    gathered = lax.fori_loop(0, 4 * quarter, piece, gathered)
    for el in PAIR:
        for loc, rem in loads[2 + el]:
            loc.wait()
            rem.wait_recv()
    dwq[...] = jnp.zeros_like(dwq)

    keys = tok
    krow = lax.broadcasted_iota(jnp.int32, (HEAD_DIM, keys), 0)
    ones_k = jnp.where(krow < n_l, 1.0, 0.0).astype(BF16)
    ones_v = jnp.where((krow >= n_l) & (krow < n_l + 3), 1.0, 0.0).astype(BF16)
    klan = lax.broadcasted_iota(jnp.int32, (per_kv, keys), 1)

    def work(h, g, done):
        u = g - h * head_steps
        slot = packed(u, SLOTS[h], 6)
        delta, j = (slot >> 2) - 4, slot & 3
        own = delta == 0
        kz = wrap(z + delta)
        lower = kz < z
        q_late = jnp.where(own, jnp.where(j >= 1, 1, 0), jnp.where(lower, j, 1))
        k_late = jnp.where(own, jnp.where(j >= 2, 1, 0), jnp.where(lower, 0, j))
        q_blk = jnp.where(q_late == 1, 2 * nz - 1 - z, z)
        k_blk = jnp.where(k_late == 1, 2 * nz - 1 - kz, kz)
        off = (q_blk - k_blk) * tok
        r = pl.ds(pl.multiple_of((h * 2 + q_late) * rows, rows), rows)
        k, v = kvall[kz, h, k_late, 0], kvall[kz, h, k_late, 1]
        hr = pl.ds(pl.multiple_of(q_late * rows, rows), rows)
        qq, ax, dd = qb[h][hr, :], aux[h][hr, :], xdo[r, :]
        s = dot(jnp.concatenate([qq, ax], 1), jnp.concatenate([k, ones_k], 0), 1, 0)
        dp = dot(jnp.concatenate([dd, ax], 1), jnp.concatenate([v, ones_v], 0), 1, 0)
        p = jnp.exp2(s * EXP_SCALE)
        p = jnp.concatenate([jnp.where(klan <= off + t, p[per_kv * t:per_kv * (t + 1)], 0.0) for t in range(tok)], 0)
        ds = (p * dp).astype(BF16)
        pb = p.astype(BF16)
        dqs[h][hr, :] += dot(ds, k, 1, 1)
        acc[kz, h, k_late, 0] += dot(qq, ds, 0, 0)
        acc[kz, h, k_late, 1] += dot(dd, pb, 0, 0)
        el, t0 = piece_at(jnp.minimum(u, n_pieces - 1))
        if h == 0:
            prepare(1, el, t0, *masks(sub))
        else:
            dwq[...] += jnp.where(u < n_pieces, finish(0, el, t0, False), 0.0)
        return ticks(g, done)

    done = (gathered, jnp.int32(0))
    for h in PAIR:
        done = lax.fori_loop(h * head_steps, (h + 1) * head_steps, functools.partial(work, h), done)

    def last(i, done):
        el, t0 = piece_at(i)
        dwq[...] += finish(1, el, t0, True)
        return ticks(n_steps + i, done)

    def back(x, ssum, g, cos, sin, w):
        rstd = lax.rsqrt(ssum * (1.0 / HEAD_DIM) + NORM_EPS)
        xhat = x * rstd
        dy = g * cos - roll_half(g) * sin
        dxh = dy * w
        dx = rstd * (dxh - xhat * lane_mean(dxh * xhat))
        return dx, jnp.sum((dy * xhat).reshape(-1, 8, HEAD_DIM), axis=0)

    outs = []

    def send_queries(h, el):
        heads = pl.ds(pl.multiple_of((2 * core + h) * per_kv, per_kv), per_kv)
        dst = dq_hbm.at[pl.ds(el * chunk, chunk), heads, :]
        part = lambda mine: qb[h].at[h_rows(el, off_of(el, mine), chunk)].reshape(chunk, per_kv, HEAD_DIM)
        both = (pltpu.make_async_remote_copy(part(False), dst, dq_snd.at[h, el], dq_rcv.at[h, el], **to(sib)),
                pltpu.make_async_copy(part(True), dst, dq_loc.at[h, el]))
        outs.append(both)
        for cpy in both:
            cpy.start()

    hold = 4 * k_rows

    def key_gradients(h, dwk):
        for el in PAIR:
            kout[h, el, 1] = acc[z, h, el, 1].T.astype(BF16)
            dq[pl.ds(hold, tok), :] = acc[z, h, el, 0].T * SM_SCALE
            for s in PAIR:
                off = off_of(el, s == 0)
                x = raw(0, s, h, el)
                tabs = pl.ds(pl.multiple_of(el * tok + off, chunk), chunk)
                dx, dwp = back(x, lane_sum(x * x), dq[pl.ds(pl.multiple_of(hold + off, chunk), chunk), :], cos_d[tabs], sin_d[tabs], kw)
                kout[h, el, 0, pl.ds(off, chunk), :] = dx.astype(BF16)
                dwk = dwk + dwp
            dst = dkv_hbm.at[2 * core + h, el]
            both = (pltpu.make_async_copy(kout.at[h, el, :, pl.ds(off_of(el, True), chunk), :], dst, dk_loc.at[h, el]),
                    pltpu.make_async_remote_copy(kout.at[h, el, :, pl.ds(off_of(el, False), chunk), :], dst, dk_snd.at[h, el],
                                                 dk_rcv.at[h, el], **to(sib)))
            outs.append(both)
            for cpy in both:
                cpy.start()
        return dwk

    for el in PAIR:
        send_queries(0, el)
    for side in PAIR:
        unpack_keys(0, side)

    def drain_gather(a, carry):
        direction, h, s, el, _ = split(packed(a, GATHER_CODE, 7), 1, 1, 3, 1, 1)

        @pl.when(on(g_send, a))
        def _():
            gather_copy(direction, h, s, el).wait_send()

        return carry

    lax.fori_loop(0, len(G_SEQ), drain_gather, 0)
    for cpy in swaps:
        cpy.wait_send()
    for row in loads:
        for _, rem in row:
            rem.wait_send()

    complete = 1 + max(at for at, (_, h, d, _, _) in zip(REDUCE_AT, r_seq) if h == 0 and d == 0) - n_steps
    assert complete <= n_pieces
    complete, begin = max(complete, 0), 0
    for end in sorted({complete, n_pieces // 2, n_pieces}):
        if end > begin:
            done = lax.fori_loop(begin, end, last, done)
        if end in (n_pieces // 2, n_pieces):
            send_queries(1, 2 * end // n_pieces - 1)
        if end == complete:
            dwk = key_gradients(0, jnp.zeros((8, HEAD_DIM), F32))
        begin = end
    run_actions(reduce_step, done[1], len(R_SEQ) - done[1])
    dwk = key_gradients(1, dwk)
    top = lax.broadcasted_iota(jnp.int32, (8, HEAD_DIM), 0)
    wmine[...] = jnp.where(top == 0, jnp.sum(dwq[...], axis=0, keepdims=True),
                           jnp.where(top == 1, jnp.sum(dwk, axis=0, keepdims=True), 0.0))

    def weight_copy(i):
        return pltpu.make_async_remote_copy(wmine, wslots.at[cp - i], w_snd.at[i], w_rcv.at[cp - i], **to((me + i) & (cp - 1)))

    def weight_send(i, carry):
        weight_copy(i).start()
        return carry

    lax.fori_loop(1, cp, weight_send, 0)

    def drain_reduce(b, carry):
        direction, h, d, el, _ = split(packed(b, REDUCE_CODE, 7), 1, 1, 3, 1, 1)

        @pl.when(on(r_send, b))
        def _():
            reduce_copy(direction, h, d, el, 0).wait_send()

        return carry

    lax.fori_loop(0, len(R_SEQ), drain_reduce, 0)

    def weight_wait(i, carry):
        pltpu.make_async_remote_copy(wmine, wslots.at[i], w_snd.at[i], w_rcv.at[i], **to((me + i) & (cp - 1))).wait()
        return carry

    lax.fori_loop(1, cp, weight_wait, 0)
    wslots[0] = wmine[...]
    w_ref[...] = lax.fori_loop(0, cp, lambda i, total: total + wslots[(i - me + cp) & (cp - 1)], jnp.zeros((8, HEAD_DIM), F32))
    for loc, rem in outs:
        loc.wait()
        rem.wait()


def mega(nz, kv_heads, q_raw, d_out, out_fwd, lse, k_rows, v_rows, offc, offs, basec, bases, qw, kw):
    tok, heads, hd = q_raw.shape
    chunk, per_kv = tok // 2, heads // kv_heads
    any_spec = pl.BlockSpec(memory_space=pl.ANY)
    vmem = pl.BlockSpec(memory_space=pltpu.VMEM)
    dma, scr = pltpu.SemaphoreType.DMA, pltpu.VMEM
    n_rows = 2 * tok * per_kv
    _, n_slots = landing_slots(nz, [tuple(split(c, 1, 1, 3, 1, 1)) for c in REDUCE_CODE], REDUCE_REACH)
    hbm = lambda a: pltpu.with_memory_space_constraint(a, pltpu.HBM)
    args = [q_raw, d_out, out_fwd, lse, k_rows, v_rows, offc[:, None], offs[:, None], offc, offs]
    return pl.pallas_call(
        functools.partial(mega_kernel, nz, chunk, per_kv, kv_heads),
        in_specs=[any_spec] * len(args) + [vmem] * 4,
        out_specs=[any_spec, any_spec, vmem],
        out_shape=[jax.ShapeDtypeStruct(q_raw.shape, BF16), jax.ShapeDtypeStruct((kv_heads, 2, 2, chunk, hd), BF16),
                   jax.ShapeDtypeStruct((8, hd), F32)],
        scratch_shapes=[
            *[scr((2 * n_rows, hd), BF16)] * 3, *[scr((n_rows, hd), BF16)] * 4, *[scr((n_rows, hd), F32)] * 2,
            scr((nz, 2, 2, 2, hd, tok), BF16), scr((nz, 2, 2, 2, hd, tok), F32), scr((n_slots, 2, hd, tok), F32),
            scr((2, 2) + k_rows.shape, BF16), scr((2,) + lse.shape, F32), scr((2, 2 * tok, 1, hd), F32),
            *[scr((2 * tok, 1, hd), F32)] * 2, *[scr((2 * tok, hd), F32)] * 2,
            scr((2, 2, 2, tok, hd), BF16), *[scr((8, hd), F32)] * 2, scr((2 * nz, 8, hd), F32),
            *[dma((3,))] * 3, *[dma((2, 2, 3))] * 3, dma((4,)), *[dma((2, 2, GATHER_HOPS, 2))] * 2, *[dma((2, REDUCE_HOPS, 2, 2))] * 2,
            *[dma((2, 2))] * 6, *[dma((2 * nz,))] * 2,
        ],
        name='attn_bwd',
        compiler_params=pltpu.CompilerParams(vmem_limit_bytes=67000000, collective_id=0, has_side_effects=True),
    )(*[hbm(a) for a in args], basec, bases, qw, kw)


def emit_kernel(n, dq_in, dkv_in, w_in, dq_out, dk_out, dv_out, wq_out, wk_out, buf, in_sem, out_sem):
    step = dq_in.shape[0] // n
    part = lambda ref, i: ref.at[pl.ds(i * step, step)]
    reads = [pltpu.make_async_copy(part(dq_in, i), part(buf, i), in_sem.at[i]) for i in range(n)]
    writes = [pltpu.make_async_copy(part(buf, i), part(dq_out, i), out_sem.at[i]) for i in range(n)]
    for cpy in reads:
        cpy.start()
    wq_out[...], wk_out[...] = w_in[0:1, :], w_in[1:2, :]
    kv_heads, halves, _, chunk, _ = dkv_in.shape
    for i in range(n):
        reads[i].wait()
        writes[i].start()
        if i < 2 * halves:
            ref, half, what = (dk_out, dv_out)[i & 1], i >> 1, i & 1
            x = dkv_in[:, half, what].astype(F32)
            ref[pl.ds(half * chunk, chunk)] = jnp.stack([x[h] for h in range(kv_heads)], axis=1).astype(BF16)
    for cpy in writes:
        cpy.wait()


def emit(dq, dkv, weights):
    tok, _, hd = dq.shape
    kv_heads = dkv.shape[0]
    n = 8
    any_spec, vmem = pl.BlockSpec(memory_space=pl.ANY), pl.BlockSpec(memory_space=pltpu.VMEM)
    return pl.pallas_call(
        functools.partial(emit_kernel, n),
        in_specs=[any_spec, vmem, vmem],
        out_specs=[any_spec] + [vmem] * 4,
        out_shape=[jax.ShapeDtypeStruct(dq.shape, BF16)] + [jax.ShapeDtypeStruct((tok, kv_heads, hd), BF16)] * 2
        + [jax.ShapeDtypeStruct((1, hd), F32)] * 2,
        scratch_shapes=[pltpu.VMEM(dq.shape, BF16), *[pltpu.SemaphoreType.DMA((n,))] * 2],
        name='emit',
    )(pltpu.with_memory_space_constraint(dq, pltpu.HBM), dkv, weights)


def solution(mesh):
    cp_size = mesh.shape['cp']
    nz = cp_size // 2

    def local_grads(q_raw, k_raw, v_proj, out_fwd, lse_fwd, d_out, q_norm, k_norm):
        tok, kv_heads = k_raw.shape[0], k_raw.shape[1]
        inv_freq = ROPE_THETA ** (-np.arange(0, HEAD_DIM, 2, dtype=np.float64) / HEAD_DIM)
        inv_freq = np.concatenate([inv_freq, inv_freq])
        sign = np.where(np.arange(HEAD_DIM) < HEAD_DIM // 2, -1.0, 1.0)
        off_ang = np.arange(tok)[:, None] * inv_freq
        base_ang = (np.arange(cp_size) * tok)[:, None] * inv_freq
        table = lambda x: jnp.asarray(x, F32)
        rows = lambda a: a.reshape(tok * kv_heads, HEAD_DIM)
        dq_raw, dkv, sums = mega(nz, kv_heads, q_raw, d_out, out_fwd, lse_fwd.T, rows(k_raw), rows(v_proj),
                                 table(np.cos(off_ang)), table(np.sin(off_ang) * sign),
                                 table(np.cos(base_ang))[:, None], table(np.sin(base_ang) * sign)[:, None],
                                 q_norm.reshape(1, HEAD_DIM), k_norm.reshape(1, HEAD_DIM))
        dq_raw, dk_raw, dv, wq, wk = emit(dq_raw, dkv, sums)
        return dq_raw, dk_raw, dv, wq.reshape(HEAD_DIM), wk.reshape(HEAD_DIM)

    row_spec = P(('dp', 'cp'))
    in_specs = (row_spec, row_spec, row_spec, row_spec, row_spec, row_spec, P(), P())
    out_specs = (row_spec, row_spec, row_spec, P('dp'), P('dp'))
    return jax.shard_map(local_grads, mesh=mesh, in_specs=in_specs, out_specs=out_specs, check_vma=False)
```
